128 devices in a mesh: wide: 16 (over z, y), deep: 8 (over x, core).
Axes of the slice: x: 4, y: 4, z: 4, core: 2. Of those that a mesh axis runs over, the one named last changes fastest.
Arguments:
- coarse_density: float32 [128, 8, 960], P('wide', None, 'deep'), may hold values from 0.8 to 1.6
- coarse_velocity: float32 [3, 128, 8, 960], P(None, 'wide', None, 'deep'), may hold values from -0.4 to 0.4
- coarse_pressure: float32 [128, 8, 960], P('wide', None, 'deep'), may hold values from 0.8 to 1.6
- fine_density: float32 [8, 64, 16, 256], P('deep', 'wide'), may hold values from 0.8 to 1.6
- fine_velocity: float32 [8, 64, 3, 16, 256], P('deep', 'wide'), may hold values from -0.4 to 0.4
- fine_pressure: float32 [8, 64, 16, 256], P('deep', 'wide'), may hold values from 0.8 to 1.6
- patch_count: int32 [8, 16], P('deep'), may hold values from 1 to 4, 32 in all within a row
- region_start: int32 [8], P('deep'), may hold values from 0 to 207
Outputs:
- coarse_state: float32 [5, 128, 8, 960], P(None, 'wide', None, 'deep')
- fine_state: float32 [8, 64, 5, 16, 256], P('deep', 'wide')
The draws below stay inside these ranges and needn't reach their ends.
Inputs may be any that keep to these rules, and one draw needn't show every extreme that they name: `patch_count`: each deep row's counts sum to 32, and some device of every row holds 4 patches.
All inputs are finite; a program needn't handle non-finite values.
Results may differ from the reference program's by a relative error of at most 0.0003.
Values sent between devices are 32-bit elements; how exact they have to be, the bound alone decides.
No kernel may reach another device: no remote copies, remote signals or barrier semaphores. Data moves between devices by JAX's collectives and lax.ppermute only.
A program may use at most 192 MiB of HBM per device.

```python
import math
import jax
import jax.numpy as jnp
import numpy as np
from jax import lax

PATCH = 16
SLOTS = 4
CZ = 120
BLOCK = 8
PLACES = 13
NX = 128
NY = 8
NZ = 960
NPATCH = 512
TOT_ROW = 32
N_WIDE = 16
N_DEEP = 8


def touch_ends(values, own_key, least, top_value):
    shape = values.shape
    index_at = [jax.random.randint(jax.random.fold_in(own_key, axis), (), 0, shape[axis]) for axis in range(len(shape))]
    values = values.at[tuple(index_at)].set(least)
    longest = shape.index(max(shape))
    index_at[longest] = (index_at[longest] + 1) % shape[longest]
    return values.at[tuple(index_at)].set(top_value)


def block_scale(stream_key, extent, cuts, smallest, top_value):
    gain, own = 1.0, jax.random.fold_in(stream_key, 6)
    for position, shards_of in cuts:
        heights = jnp.exp(jax.random.uniform(jax.random.fold_in(own, position), (shards_of,), jnp.float32, smallest / len(cuts), top_value / len(cuts)))
        gain = gain * jnp.repeat(heights, extent[position] // shards_of).reshape([-1 if axis == position else 1 for axis in range(len(extent))])
    return gain


def length_profile(amount, total, limit, skew):
    portions = [(1 << 20) // math.isqrt(standing ** skew) + 1 for standing in range(2, amount + 1)]
    rest, given = total - limit - (amount - 1), [1] * (amount - 1)
    while rest > 0:
        movable = [i for i in range(amount - 1) if given[i] < limit]
        pool, left = sum([portions[i] for i in movable]), rest
        for i in movable:
            extra = min(limit - given[i], max(1, left * portions[i] // pool), rest)
            given[i] = given[i] + extra
            rest = rest - extra
    return np.array([limit] + given)


def uneven(rng, count, total, reach, slope):
    if count == 2:
        one = jax.random.randint(rng, (), max(1, total - reach), min(reach, total - 1) + 1)
        return jnp.stack([one, total - one])
    tallies = jnp.asarray(length_profile(count, total, reach, slope), jnp.int32)
    twos = (count - 1) // 2
    source_of, receiver = tallies[1:1 + 2 * twos:2], tallies[2:2 + 2 * twos:2]
    margin = jnp.minimum(source_of - 1, reach - receiver)
    moved = jax.random.randint(jax.random.fold_in(rng, 1), (twos,), 0, 1 << 20) % (margin + 1)
    tallies = tallies.at[1:1 + 2 * twos:2].set(source_of - moved).at[2:2 + 2 * twos:2].set(receiver + moved)
    return tallies[jax.random.permutation(jax.random.fold_in(rng, 2), count)]


def setup_inputs(seed: int = 0) -> dict:
    splits = jax.random.split(jax.random.key(seed), 9)
    coarse_density = jnp.clip(jnp.exp(math.log(1.6) - 0.6931472 * jax.random.uniform(splits[0], (NX, NY, NZ), jnp.float32) ** block_scale(splits[0], (NX, NY, NZ), ((0, 16), (2, 8)), -0.2, 0.2)), 0.8, 1.6)
    coarse_velocity = jnp.clip(jax.random.uniform(splits[1], (3, NX, NY, NZ), jnp.float32, -0.4, 0.4) * block_scale(splits[1], (3, NX, NY, NZ), ((1, 16), (3, 8)), -0.4, 0.0), -0.4, 0.4)
    coarse_pressure = jnp.clip(jnp.exp(math.log(1.6) - 0.6931472 * jax.random.uniform(splits[2], (NX, NY, NZ), jnp.float32) ** block_scale(splits[2], (NX, NY, NZ), ((0, 16), (2, 8)), -0.2, 0.2)), 0.8, 1.6)
    fine_density = jnp.clip(jnp.exp(math.log(1.6) - 0.6931472 * jax.random.uniform(splits[3], (N_DEEP, N_WIDE * SLOTS, PATCH, PATCH * PATCH), jnp.float32) ** block_scale(splits[3], (N_DEEP, N_WIDE * SLOTS, PATCH, PATCH * PATCH), ((0, 8), (1, 16)), -0.2, 0.2)), 0.8, 1.6)
    fine_velocity = jnp.clip(jax.random.uniform(splits[4], (N_DEEP, N_WIDE * SLOTS, 3, PATCH, PATCH * PATCH), jnp.float32, -0.4, 0.4) * block_scale(splits[4], (N_DEEP, N_WIDE * SLOTS, 3, PATCH, PATCH * PATCH), ((0, 8), (1, 16)), -0.4, 0.0), -0.4, 0.4)
    fine_pressure = jnp.clip(jnp.exp(math.log(1.6) - 0.6931472 * jax.random.uniform(splits[5], (N_DEEP, N_WIDE * SLOTS, PATCH, PATCH * PATCH), jnp.float32) ** block_scale(splits[5], (N_DEEP, N_WIDE * SLOTS, PATCH, PATCH * PATCH), ((0, 8), (1, 16)), -0.2, 0.2)), 0.8, 1.6)
    patch_count = jax.vmap(lambda own: uneven(own, N_WIDE, TOT_ROW, SLOTS, 4))(jax.random.split(splits[6], N_DEEP)).reshape((N_DEEP, N_WIDE)).astype(jnp.int32)
    region_start = touch_ends(jax.random.randint(splits[7], (N_DEEP,), 0, N_WIDE * PLACES), jax.random.fold_in(splits[7], 1), 0, (N_WIDE * PLACES) - 1).astype(jnp.int32)
    return {"coarse_density": coarse_density, "coarse_velocity": coarse_velocity, "coarse_pressure": coarse_pressure, "fine_density": fine_density, "fine_velocity": fine_velocity, "fine_pressure": fine_pressure, "patch_count": patch_count, "region_start": region_start}


heat_ratio = 1.4
weno_floor = 1e-06
coarse_step = 0.2
fine_step = 0.1
fine_spacing = 0.5

def primitive(state):
    density = state[0]
    speed_x = state[1] / density
    speed_y = state[2] / density
    speed_z = state[3] / density
    kinetic = 0.5 * density * (speed_x * speed_x + speed_y * speed_y + speed_z * speed_z)
    pressure = (heat_ratio - 1.0) * (state[4] - kinetic)
    return jnp.stack([density, speed_x, speed_y, speed_z, pressure])

def conserved(prims):
    density = prims[0]
    kinetic = 0.5 * density * (prims[1] * prims[1] + prims[2] * prims[2] + prims[3] * prims[3])
    energy = prims[4] / (heat_ratio - 1.0) + kinetic
    return jnp.stack([density, density * prims[1], density * prims[2], density * prims[3], energy])

def weno_value(first, second, third, fourth, fifth):
    cand_one = (2.0 * first - 7.0 * second + 11.0 * third) / 6.0
    cand_two = (-second + 5.0 * third + 2.0 * fourth) / 6.0
    cand_three = (2.0 * third + 5.0 * fourth - fifth) / 6.0
    rough_one = 13.0 / 12.0 * (first - 2.0 * second + third) ** 2 + 0.25 * (first - 4.0 * second + 3.0 * third) ** 2
    rough_two = 13.0 / 12.0 * (second - 2.0 * third + fourth) ** 2 + 0.25 * (second - fourth) ** 2
    rough_three = 13.0 / 12.0 * (third - 2.0 * fourth + fifth) ** 2 + 0.25 * (3.0 * third - 4.0 * fourth + fifth) ** 2
    weight_one = 0.1 / (weno_floor + rough_one) ** 2
    weight_two = 0.6 / (weno_floor + rough_two) ** 2
    weight_three = 0.3 / (weno_floor + rough_three) ** 2
    total = weight_one + weight_two + weight_three
    return (weight_one * cand_one + weight_two * cand_two + weight_three * cand_three) / total

def wave_parts(dens, normal, side, other, press, wave, middle):
    energy = press / (heat_ratio - 1.0) + 0.5 * dens * (normal * normal + side * side + other * other)
    mass = dens * (wave - normal)
    state = jnp.stack([dens, dens * normal, dens * side, dens * other, energy])
    flux = jnp.stack([dens * normal, dens * normal * normal + press, dens * normal * side, dens * normal * other, normal * (energy + press)])
    factor = mass / (wave - middle)
    star = factor * jnp.stack([jnp.ones_like(dens), middle, side, other, energy / dens + (middle - normal) * (middle + press / mass)])
    return (flux, flux + wave * (star - state))

def hllc(left, right):
    sound_left = jnp.sqrt(heat_ratio * left[4] / left[0])
    sound_right = jnp.sqrt(heat_ratio * right[4] / right[0])
    slow = jnp.minimum(left[1] - sound_left, right[1] - sound_right)
    fast = jnp.maximum(left[1] + sound_left, right[1] + sound_right)
    mass_left = left[0] * (slow - left[1])
    mass_right = right[0] * (fast - right[1])
    middle = (right[4] - left[4] + mass_left * left[1] - mass_right * right[1]) / (mass_left - mass_right)
    flux_left, star_left = wave_parts(left[0], left[1], left[2], left[3], left[4], slow, middle)
    flux_right, star_right = wave_parts(right[0], right[1], right[2], right[3], right[4], fast, middle)
    return jnp.where(slow[None] >= 0.0, flux_left, jnp.where(middle[None] >= 0.0, star_left, jnp.where(fast[None] > 0.0, star_right, flux_right)))

def face_flux(padded, axis):
    prims = primitive(padded)
    count = padded.shape[axis] - 5
    pieces = [lax.slice_in_dim(prims, k, k + count, axis=axis) for k in range(6)]
    left = weno_value(pieces[0], pieces[1], pieces[2], pieces[3], pieces[4])
    right = weno_value(pieces[5], pieces[4], pieces[3], pieces[2], pieces[1])
    order = [0, axis] + [k for k in (1, 2, 3) if k != axis] + [4]
    inverse = [order.index(k) for k in range(5)]
    flux = hllc(left[np.array(order)], right[np.array(order)])
    return flux[np.array(inverse)]

def cell_rates(pad_x, pad_y, pad_z, spacing):
    flux_x = face_flux(pad_x, 1)
    flux_y = face_flux(pad_y, 2)
    flux_z = face_flux(pad_z, 3)
    change = flux_x[:, 1:] - flux_x[:, :-1] + (flux_y[:, :, 1:] - flux_y[:, :, :-1]) + (flux_z[:, :, :, 1:] - flux_z[:, :, :, :-1])
    return (-change / spacing, flux_x, flux_z)

def patch_rates(state, ghost_xl, ghost_xh, ghost_zl, ghost_zh):
    pad_x = jnp.concatenate([ghost_xl, state, ghost_xh], axis=1)
    pad_y = jnp.concatenate([state[:, :, -3:], state, state[:, :, :3]], axis=2)
    pad_z = jnp.concatenate([ghost_zl, state, ghost_zh], axis=3)
    rate, flux_x, flux_z = cell_rates(pad_x, pad_y, pad_z, fine_spacing)
    return (rate, flux_x[:, 0], flux_x[:, -1], flux_z[:, :, :, 0], flux_z[:, :, :, -1])

def coarse_ghosts(rim_x, rim_z):

    def spread(part, first_axis, second_axis):
        return jnp.repeat(jnp.repeat(part, 2, axis=first_axis), 2, axis=second_axis)
    low_x = spread(rim_x[:, np.array([0, 1, 1])], 2, 3)
    high_x = spread(rim_x[:, np.array([2, 2, 3])], 2, 3)
    low_z = spread(rim_z[..., np.array([0, 1, 1])], 1, 2)
    high_z = spread(rim_z[..., np.array([2, 2, 3])], 1, 2)
    return (low_x, high_x, low_z, high_z)

def coarsen(face):
    half = face.shape[-1] // 2
    return face.reshape(face.shape[:-2] + (half, 2, half, 2)).sum(axis=(-3, -1)) * 0.25

def average(state):
    half = state.shape[-1] // 2
    return state.reshape(state.shape[:-3] + (half, 2, half, 2, half, 2)).sum(axis=(-5, -3, -1)) * 0.125

def coarse_rates(state):
    padded_z = jnp.pad(state, ((0, 0), (0, 0), (0, 0), (3, 3)), mode='wrap')

    def one_row(row):
        slab = lax.dynamic_slice_in_dim(padded_z, row * CZ, CZ + 6, axis=3)
        centre = slab[:, :, :, 3:-3]
        pad_x = jnp.pad(centre, ((0, 0), (3, 3), (0, 0), (0, 0)), mode='wrap')
        pad_y = jnp.pad(centre, ((0, 0), (0, 0), (3, 3), (0, 0)), mode='wrap')
        return cell_rates(pad_x, pad_y, slab, 1.0)
    rate, flux_x, flux_z = lax.map(one_row, jnp.arange(N_DEEP, dtype=jnp.int32))
    rate = jnp.moveaxis(rate, 0, 3).reshape(5, NX, NY, NZ)
    return (rate, flux_x, flux_z)

def patch_rims(state, start_x, start_z):
    zero = jnp.zeros((), jnp.int32)
    size = state.shape[1]
    sides = [lax.dynamic_slice(state, (zero, ((start_x + shift) % size).astype(jnp.int32), zero, start_z.astype(jnp.int32)), (5, 1, BLOCK, BLOCK))[:, 0] for shift in (-2, -1, BLOCK, BLOCK + 1)]
    tops = [lax.dynamic_slice(state, (zero, start_x.astype(jnp.int32), zero, (start_z + shift).astype(jnp.int32)), (5, BLOCK, BLOCK, 1))[:, :, :, 0] for shift in (-2, -1, BLOCK, BLOCK + 1)]
    return (jnp.stack(sides, axis=1), jnp.stack(tops, axis=3))

def reference(coarse_density, coarse_velocity, coarse_pressure, fine_density, fine_velocity, fine_pressure, patch_count, region_start):
    coarse = conserved(jnp.stack([coarse_density, coarse_velocity[0], coarse_velocity[1], coarse_velocity[2], coarse_pressure]))
    rate_one, flux_xa, flux_za = coarse_rates(coarse)
    middle = coarse + coarse_step * rate_one
    rate_two, flux_xb, flux_zb = coarse_rates(middle)
    updated = 0.5 * (coarse + middle + coarse_step * rate_two)
    mean_x = 0.5 * (flux_xa + flux_xb)
    mean_z = 0.5 * (flux_za + flux_zb)
    density = jnp.swapaxes(fine_density.reshape(NPATCH, PATCH, PATCH, PATCH), 2, 3)
    velocity = jnp.swapaxes(fine_velocity.reshape(NPATCH, 3, PATCH, PATCH, PATCH), 3, 4)
    pressure = jnp.swapaxes(fine_pressure.reshape(NPATCH, PATCH, PATCH, PATCH), 2, 3)
    initial = jnp.moveaxis(conserved(jnp.stack([density, velocity[:, 0], velocity[:, 1], velocity[:, 2], pressure])), 0, 1)
    index = jnp.arange(NPATCH, dtype=jnp.int32)
    rows = index // (N_WIDE * SLOTS)
    owners = index // SLOTS % N_WIDE
    places = index % SLOTS
    ends = jnp.cumsum(patch_count, axis=1).astype(jnp.int32)
    begins = ends - patch_count
    totals = ends[:, -1]
    blocks_all = N_WIDE * PLACES
    anchor = region_start[rows]
    alive = places < patch_count[rows, owners]
    serial = begins[rows, owners] + places
    ident = (anchor + 3 * (serial // 2) + serial % 2) % blocks_all
    column = ident % N_WIDE
    height = ident // N_WIDE

    def locate(target):
        offset = (target - anchor) % blocks_all
        part = offset % 3
        rank = 2 * (offset // 3) + part
        live = (part < 2) & (rank < totals[rows])
        owner = jnp.minimum(lax.optimization_barrier(jnp.sum((rank[:, None] >= ends[rows]).astype(jnp.int32), axis=1)), N_WIDE - 1)
        place = jnp.clip(rank - begins[rows, owner], 0, SLOTS - 1)
        return (live, (rows * N_WIDE + owner) * SLOTS + place)
    live_xl, flat_xl = locate(height * N_WIDE + (column + N_WIDE - 1) % N_WIDE)
    live_xh, flat_xh = locate(height * N_WIDE + (column + 1) % N_WIDE)
    live_zl, flat_zl = locate(ident - N_WIDE)
    live_zl = live_zl & (height > 0)
    live_zh, flat_zh = locate(ident + N_WIDE)
    live_zh = live_zh & (height < PLACES - 1)
    start_x = (column * BLOCK).astype(jnp.int32)
    start_z = (rows * CZ + (height + 1) * BLOCK).astype(jnp.int32)
    old_x, old_z = jax.vmap(patch_rims, (None, 0, 0))(coarse, start_x, start_z)
    new_x, new_z = jax.vmap(patch_rims, (None, 0, 0))(updated, start_x, start_z)

    def mark(flag):
        return flag[:, None, None, None, None]

    def fine_rates(states, theta):
        rim_x = (1.0 - theta) * old_x + theta * new_x
        rim_z = (1.0 - theta) * old_z + theta * new_z
        cxl, cxh, czl, czh = jax.vmap(coarse_ghosts)(rim_x, rim_z)
        ghost_xl = jnp.where(mark(live_xl), states[:, :, -3:][flat_xl], cxl)
        ghost_xh = jnp.where(mark(live_xh), states[:, :, :3][flat_xh], cxh)
        ghost_zl = jnp.where(mark(live_zl), states[..., -3:][flat_zl], czl)
        ghost_zh = jnp.where(mark(live_zh), states[..., :3][flat_zh], czh)

        def one_patch(group):
            return patch_rates(group[0], group[1], group[2], group[3], group[4])
        return lax.map(one_patch, (states, ghost_xl, ghost_xh, ghost_zl, ghost_zh))

    def substep(states, theta_a, theta_b):
        early = fine_rates(states, theta_a)
        middle_f = states + fine_step * early[0]
        later = fine_rates(middle_f, theta_b)
        after = 0.5 * (states + middle_f + fine_step * later[0])
        faces = [fine_step * 0.5 * (a + b) for a, b in zip(early[1:], later[1:])]
        return (after, faces)
    halfway, faces_one = substep(initial, 0.0, 0.5)
    final_fine, faces_two = substep(halfway, 0.5, 1.0)
    registers = [coarsen(a + b) for a, b in zip(faces_one, faces_two)]
    averaged = average(final_fine)
    mask_xl = alive & ~live_xl
    mask_xh = alive & ~live_xh
    mask_zl = alive & ~live_zl
    mask_zh = alive & ~live_zh
    zero = jnp.zeros((), jnp.int32)

    def bump(field, piece, corner_x, corner_z):
        corner = (zero, corner_x.astype(jnp.int32), zero, corner_z.astype(jnp.int32))
        current = lax.dynamic_slice(field, corner, piece.shape)
        return lax.dynamic_update_slice(field, current + piece, corner)

    def add_one(patch, field):
        row = rows[patch]
        x_low = start_x[patch]
        local = ((height[patch] + 1) * BLOCK).astype(jnp.int32)
        z_low = start_z[patch]
        faces_x = lax.dynamic_index_in_dim(mean_x, row, 0, keepdims=False)
        faces_z = lax.dynamic_index_in_dim(mean_z, row, 0, keepdims=False)
        low = lax.dynamic_slice(faces_x, (zero, x_low, zero, local), (5, 1, BLOCK, BLOCK))
        delta = coarse_step * low - registers[0][patch][:, None]
        field = bump(field, jnp.where(mask_xl[patch], delta, 0.0), (x_low - 1) % NX, z_low)
        high = lax.dynamic_slice(faces_x, (zero, x_low + BLOCK, zero, local), (5, 1, BLOCK, BLOCK))
        delta = coarse_step * high - registers[1][patch][:, None]
        field = bump(field, jnp.where(mask_xh[patch], -delta, 0.0), (x_low + BLOCK) % NX, z_low)
        low = lax.dynamic_slice(faces_z, (zero, x_low, zero, local), (5, BLOCK, BLOCK, 1))
        delta = coarse_step * low - registers[2][patch][..., None]
        field = bump(field, jnp.where(mask_zl[patch], delta, 0.0), x_low, z_low - 1)
        high = lax.dynamic_slice(faces_z, (zero, x_low, zero, local + BLOCK), (5, BLOCK, BLOCK, 1))
        delta = coarse_step * high - registers[3][patch][..., None]
        field = bump(field, jnp.where(mask_zh[patch], -delta, 0.0), x_low, z_low + BLOCK)
        return field
    correction = lax.fori_loop(0, NPATCH, add_one, jnp.zeros_like(updated))
    combined = updated + correction

    def place_one(patch, field):
        corner = (zero, start_x[patch], zero, start_z[patch])
        current = lax.dynamic_slice(field, corner, (5, BLOCK, BLOCK, BLOCK))
        return lax.dynamic_update_slice(field, jnp.where(alive[patch], averaged[patch], current), corner)
    coarse_state = lax.fori_loop(0, NPATCH, place_one, combined)
    fine_final = jnp.where(mark(alive), final_fine, initial)
    fine_state = jnp.swapaxes(fine_final, 3, 4).reshape(N_DEEP, N_WIDE * SLOTS, 5, PATCH, PATCH * PATCH)
    return (coarse_state, fine_state)
```

```python
import jax
import jax.numpy as jnp
from jax import lax
from jax.experimental import pallas as pl
from jax.experimental.pallas import tpu as pltpu
from jax.sharding import PartitionSpec as P

f32 = jnp.float32
i32 = jnp.int32
HIGH = lax.Precision.HIGHEST
PLACES = 13
WIDE = 16
DEEP = 8
LIVE_Z = 120
FILL = (1.0, 0.0, 0.0, 0.0, 2.5)


def lanes():
    return lax.broadcasted_iota(i32, (8, 128), 1)


def subs():
    return lax.broadcasted_iota(i32, (8, 128), 0)


def roll(v, shift, axis):
    size = v.shape[axis]
    shift = shift % size
    return v if shift == 0 else pltpu.roll(v, shift, axis)


def y_shift(v, k):
    y = lanes() & 15
    if k > 0:
        return jnp.where(y < 16 - k, roll(v, -k, 1), roll(v, 16 - k, 1))
    return jnp.where(y >= -k, roll(v, -k, 1), roll(v, -k - 16, 1))


def sub_shift(v, k):
    return roll(v, -k, 0)


def lane_shift(v, k):
    return roll(v, -k, 1)


def prims_of(u):
    inv = 1.0 / u[0]
    vx, vy, vz = u[1] * inv, u[2] * inv, u[3] * inv
    kinetic = 0.5 * u[0] * (vx * vx + vy * vy + vz * vz)
    return [u[0], vx, vy, vz, 0.4 * (u[4] - kinetic)]


def cons_of(p):
    kinetic = 0.5 * p[0] * (p[1] * p[1] + p[2] * p[2] + p[3] * p[3])
    return [p[0], p[0] * p[1], p[0] * p[2], p[0] * p[3], p[4] / 0.4 + kinetic]


def recon(a, b, c, d, e):
    da, db, dc, dd = b - a, c - b, d - c, e - d
    ga, gb, gc = db - da, dc - db, dd - dc
    db2, dc2 = db + db, dc + dc
    ta, tb, tc = ga + db2, db + dc, gc - dc2
    k = 13.0 / 3.0
    sa = (k * ga) * ga + (ta * ta + 4e-6)
    sb = (k * gb) * gb + (tb * tb + 4e-6)
    sc = (k * gc) * gc + (tc * tc + 4e-6)
    pa, pb, pc = sa * sa, (sb * sb) * (1.0 / 6.0), sc * sc
    bc, ac, ab = pb * pc, pa * pc, pa * pb
    ab3, bc3 = 3.0 * ab, 3.0 * bc
    db4, dc4 = db2 + db2, dc2 + dc2
    left = bc * (db4 + db - (da + da)) + ac * (db + dc2) + ab3 * (dc4 - dd)
    right = ab * (dc4 + dc - (dd + dd)) + ac * (dc + db2) + bc3 * (db4 - da)
    left = left / (6.0 * (bc + ac + ab3))
    right = right / (6.0 * (ab + ac + bc3))
    return c + left, c - right


def hllc(lt, rt, n):
    o1, o2 = [k for k in (1, 2, 3) if k != n]
    dl, ul, pl_ = lt[0], lt[n], lt[4]
    dr, ur, pr = rt[0], rt[n], rt[4]
    il, ir = 1.0 / dl, 1.0 / dr
    cl = jnp.sqrt(1.4 * pl_ * il)
    cr = jnp.sqrt(1.4 * pr * ir)
    slow = jnp.minimum(ul - cl, ur - cr)
    fast = jnp.maximum(ul + cl, ur + cr)
    ml = dl * (slow - ul)
    mr = dr * (fast - ur)
    mid = (pr - pl_ + ml * ul - mr * ur) / (ml - mr)
    use = (slow >= 0.0) | (mid >= 0.0)
    d = jnp.where(use, dl, dr)
    u = jnp.where(use, ul, ur)
    t1 = jnp.where(use, lt[o1], rt[o1])
    t2 = jnp.where(use, lt[o2], rt[o2])
    p = jnp.where(use, pl_, pr)
    inv = jnp.where(use, il, ir)
    mass = jnp.where(use, ml, mr)
    wave = jnp.where(use, slow, fast)
    star = (use & (slow < 0.0)) | (jnp.logical_not(use) & (fast > 0.0))
    energy = 2.5 * p + 0.5 * d * (u * u + t1 * t1 + t2 * t2)
    du = d * u
    factor = mass / (wave - mid)
    e_star = energy * inv + (mid - u) * (mid + p / mass)
    out = [None] * 5
    flux = {0: du, n: du * u + p, o1: du * t1, o2: du * t2, 4: u * (energy + p)}
    state = {0: d, n: du, o1: d * t1, o2: d * t2, 4: energy}
    goal = {0: factor, n: factor * mid, o1: factor * t1, o2: factor * t2, 4: factor * e_star}
    for c in range(5):
        out[c] = jnp.where(star, flux[c] + wave * (goal[c] - state[c]), flux[c])
    return out


def major_pass(q, sl, sr, fx, n):
    def cells(m, carry):
        for c in range(5):
            l, r = recon(*[q[c, m + k] for k in range(5)])
            sl[c, m] = l
            sr[c, m] = r
        return carry

    lax.fori_loop(0, 10, cells, 0)

    def faces(g, carry):
        for j in range(3):
            f = g * 3 + j
            out = hllc([sl[c, f] for c in range(5)], [sr[c, f + 1] for c in range(5)], n)
            for c in range(5):
                fx[c, f] = out[c]
        return carry

    lax.fori_loop(0, 3, faces, 0)


def roll_pass(q, d, shift, n, keep=None):
    def cells(m, carry):
        left, right = [], []
        for c in range(5):
            v = q[c, m + 3]
            l, r = recon(shift(v, -2), shift(v, -1), v, shift(v, 1), shift(v, 2))
            left.append(shift(l, -1))
            right.append(r)
        out = hllc(left, right, n)
        for c in range(5):
            d[c, m] = d[c, m] + (shift(out[c], 1) - out[c])
            if keep is not None:
                keep[c, m] = out[c]
        return carry

    lax.fori_loop(0, 8, cells, 0)


def swap_groups(v):
    lane = lanes()
    for b in range(3):
        bit = ((lane >> (4 + b)) & 1) == 1
        step = 16 << b
        w = list(v)
        for m in range(8):
            if not (m >> b) & 1:
                lo, hi = v[m], v[m | (1 << b)]
                w[m] = jnp.where(bit, roll(hi, step, 1), lo)
                w[m | (1 << b)] = jnp.where(bit, hi, roll(lo, -step, 1))
        v = w
    return v


Z0, OWNER, COL, COUNT, ADJ, MATCH = 0, 2, 4, 8, 9, 10


def column_places(column, anchor):
    d = (column - anchor) & 15
    bad = 2 - lax.rem(d, 3)
    off_a = d + 16 * jnp.where(bad == 0, 1, 0)
    off_b = d + 16 * jnp.where(bad == 2, 1, 2)

    def ident(off):
        place = anchor + off
        return jnp.where(place >= WIDE * PLACES, place - WIDE * PLACES, place)

    swap = ident(off_b) < ident(off_a)
    first = jnp.where(swap, off_b, off_a)
    second = jnp.where(swap, off_a, off_b)
    heights = [ident(first) >> 4, ident(second) >> 4]
    ranks = [2 * lax.div(o, 3) + lax.rem(o, 3) for o in (first, second)]
    return heights, ranks


def info_kernel(counts, start, here, info):
    me = here[0]
    anchor = start[0]
    h, ranks = column_places(me, anchor)
    low, _ = column_places((me + 15) & 15, anchor)
    high, _ = column_places((me + 1) & 15, anchor)
    total = jnp.int32(0)
    begin = jnp.int32(0)
    mine = jnp.int32(0)
    owner = [jnp.int32(0), jnp.int32(0)]
    for w in range(WIDE):
        n = counts[0, w]
        begin = jnp.where(me == w, total, begin)
        mine = jnp.where(me == w, n, mine)
        total = total + n
        for p in range(2):
            owner[p] = owner[p] + jnp.where(ranks[p] >= total, 1, 0)
    for p in range(2):
        info[Z0 + p] = 8 * (h[p] + 1)
        info[OWNER + p] = jnp.minimum(owner[p], WIDE - 1)
        for side, other in enumerate((low, high)):
            info[MATCH + 2 * side + p] = jnp.where(
                other[0] == h[p], 0, jnp.where(other[1] == h[p], 1, 2)
            )
    for s in range(4):
        serial = begin + s
        place = anchor + 3 * (serial >> 1) + (serial & 1)
        info[COL + s] = place & 15
    info[COUNT] = mine
    info[ADJ] = jnp.where(h[1] == h[0] + 1, 1, 0)
    info[14] = 0
    info[15] = 0


def send_kernel(info, dens, vel, pres, out, sem):
    for s in range(4):

        @pl.when(s < info[COUNT])
        def _():
            copies = slot_copies(info, dens, vel, pres, out, sem, s)
            for cp in copies:
                cp.start()

    for s in range(4):

        @pl.when(s < info[COUNT])
        def _():
            for cp in slot_copies(info, dens, vel, pres, out, sem, s):
                cp.wait()


def slot_copies(info, dens, vel, pres, out, sem, s):
    to = info[COL + s]
    copies = []
    for xh in range(2):
        for zh in range(2):
            rows, cols = pl.ds(8 * xh, 8), pl.ds(128 * zh, 128)
            goal = pl.ds(16 * xh + 8 * zh, 8)
            k = 2 * xh + zh
            copies.append(
                pltpu.make_async_copy(
                    dens.at[0, s, rows, cols], out.at[to, 0, goal, :], sem.at[s, 3 * k]
                )
            )
            copies.append(
                pltpu.make_async_copy(
                    vel.at[0, s, :, rows, cols],
                    out.at[to, pl.ds(1, 3), goal, :],
                    sem.at[s, 3 * k + 1],
                )
            )
            copies.append(
                pltpu.make_async_copy(
                    pres.at[0, s, rows, cols], out.at[to, 4, goal, :], sem.at[s, 3 * k + 2]
                )
            )
    return copies


def patch_copies(info, far, near, sem, out):
    copies = []
    for p in range(2):
        for xh in range(2):
            there = far.at[info[OWNER + p], :, pl.ds(16 * xh, 16), :]
            here = near.at[:, pl.ds((4 * xh + 2 * p) * 8, 16), :]
            a, b = (here, there) if out else (there, here)
            copies.append(pltpu.make_async_copy(a, b, sem.at[2 * p + xh]))
    return copies


def take_kernel(info, far, s, lo, hi, near, sem):
    copies = patch_copies(info, far, near, sem, False)
    for cp in copies:
        cp.start()
    for cp in copies:
        cp.wait()
    for m in range(8):
        u = cons_of([near[c, pl.ds(m, 8, stride=8), :] for c in range(5)])
        for c in range(5):
            s[c, m] = u[c]
    lo[...] = s[:, 0:3, 0:4, :]
    hi[...] = s[:, 5:8, 4:8, :]


def give_kernel(info, s, far, near, sem):
    for m in range(8):
        for c in range(5):
            near[c, pl.ds(m, 8, stride=8), :] = s[c, m]
    copies = patch_copies(info, far, near, sem, True)
    for cp in copies:
        cp.start()
    for cp in copies:
        cp.wait()


def home_copies(info, far, out, sem, s):
    copies = []
    for xh in range(2):
        for zh in range(2):
            copies.append(
                pltpu.make_async_copy(
                    far.at[info[COL + s], :, pl.ds(16 * xh + 8 * zh, 8), :],
                    out.at[0, s, :, pl.ds(8 * xh, 8), pl.ds(128 * zh, 128)],
                    sem.at[s, 2 * xh + zh],
                )
            )
    return copies


def home_kernel(info, far, initial, out, sem):
    for s in range(4):

        @pl.when(s < info[COUNT])
        def _():
            for cp in home_copies(info, far, out, sem, s):
                cp.start()

    for s in range(4):

        @pl.when(s < info[COUNT])
        def _():
            for cp in home_copies(info, far, out, sem, s):
                cp.wait()


def pack_edge(u, first):
    lane = lanes()
    out = jnp.zeros((8, 128), f32)
    for c in range(5):
        for x in range(8):
            k = 3 * (8 * c + x)
            out = jnp.where((lane >= k) & (lane < k + 3), roll(u[c, x], k - first, 1), out)
    return out


def prep_kernel(dens, vel, pres, u, lo, hi, plo, phi):
    state = cons_of([dens[...], vel[0], vel[1], vel[2], pres[...]])
    for c in range(5):
        u[c] = jnp.full((8, 8, 128), FILL[c], f32)
        u[c, :, :, pl.ds(0, LIVE_Z)] = state[c]
    lo[...] = u[:, 0:3]
    hi[...] = u[:, 5:8]
    plo[...] = pack_edge(u, 0)
    phi[...] = pack_edge(u, LIVE_Z - 3)


def coarse_rates(u, xl, xh, zl, zh, q, sl, sr, fx, d, keep):
    lane = lanes()
    below, above = zl[...], zh[...]
    for m in range(8):
        state = []
        for c in range(5):
            k = 3 * (8 * c + m)
            v = jnp.where(lane >= 125, roll(below, 125 - k, 1), u[c, m])
            state.append(
                jnp.where((lane >= 120) & (lane < 123), roll(above, 120 - k, 1), v)
            )
        p = prims_of(state)
        for c in range(5):
            q[c, m + 3] = p[c]
    for g in range(3):
        for ref, at in ((xl, g), (xh, g + 11)):
            p = prims_of([ref[c, g] for c in range(5)])
            for c in range(5):
                q[c, at] = p[c]
    major_pass(q, sl, sr, fx, 1)
    for m in range(8):
        for c in range(5):
            d[c, m] = fx[c, m + 1] - fx[c, m]
    roll_pass(q, d, sub_shift, 2)
    roll_pass(q, d, lane_shift, 3, keep)


def coarse_one(u, xl, xh, zl, zh, mid, lo, hi, plo, phi, fa, fz, q, sl, sr, fx, d):
    coarse_rates(u, xl, xh, zl, zh, q, sl, sr, fx, d, fz)
    live = lanes() < LIVE_Z
    for c in range(5):
        fa[c, 0] = fx[c, 0]
        fa[c, 1] = fx[c, 8]
        for m in range(8):
            mid[c, m] = jnp.where(live, u[c, m] - 0.2 * d[c, m], FILL[c])
    lo[...] = mid[:, 0:3]
    hi[...] = mid[:, 5:8]
    plo[...] = pack_edge(mid, 0)
    phi[...] = pack_edge(mid, LIVE_Z - 3)


def coarse_two(u0, fa, fza, u, xl, xh, zl, zh, new, lo, hi, mx, mz, q, sl, sr, fx, d):
    coarse_rates(u, xl, xh, zl, zh, q, sl, sr, fx, d, mz)
    live = lanes() < LIVE_Z
    for c in range(5):
        mx[c, 0] = 0.5 * (fa[c, 0] + fx[c, 0])
        mx[c, 1] = 0.5 * (fa[c, 1] + fx[c, 8])
        for m in range(8):
            mz[c, m] = 0.5 * (fza[c, m] + mz[c, m])
            new[c, m] = jnp.where(
                live, 0.5 * (u0[c, m] + u[c, m]) - 0.1 * d[c, m], FILL[c]
            )
    lo[...] = new[:, 0:2]
    hi[...] = new[:, 6:8]


def dot(a, b):
    return jnp.dot(a, b, precision=HIGH, preferred_element_type=f32)


def dot_nt(a, b):
    return lax.dot_general(
        a, b, (((1,), (1,)), ((), ())), precision=HIGH, preferred_element_type=f32
    )


def iota2(shape, axis):
    return lax.broadcasted_iota(i32, shape, axis)


def pick(cond):
    return jnp.where(cond, 1.0, 0.0).astype(f32)


def rim_kernel(info, u, xl, xh, gx, gz, *, first):
    z = iota2((128, 128), 0)
    l = iota2((128, 128), 1)
    y8 = iota2((32, 128), 0) & 7
    ymask = pick(y8 == ((iota2((32, 128), 1) & 15) >> 1))
    layers = []
    for c in range(5):
        layers += [xl[c, first], xl[c, first + 1], xh[c, 0], xh[c, 1]]
    rows = jnp.concatenate(layers, axis=0)
    parts = []
    for pz in range(4):
        start = info[Z0 + pz // 2] + 4 * (pz % 2)
        parts.append(dot(rows, pick(z == start + (l >> 5))))
    r = iota2((24, 128), 0)
    k = iota2((24, 128), 1)
    g, s = r >> 3, r & 7
    layer = jnp.where(s < 4, jnp.where(g == 0, 0, 1), jnp.where(g == 2, 3, 2))
    left = pick(((s & 3) == (k >> 5)) & (layer == ((k >> 3) & 3)))
    for c in range(5):
        stack = jnp.concatenate([part[32 * c : 32 * c + 32] * ymask for part in parts], axis=0)
        gx[c] = dot(left, stack).reshape(3, 8, 128)
    pnum = (s >> 1) & 1
    start = jnp.where(pnum == 0, info[Z0], info[Z0 + 1])
    off = jnp.where((s & 1) == 0, jnp.where(g == 0, -2, -1), jnp.where(g == 2, 9, 8))
    choose = pick(k == start + off)
    er = iota2((64, 256), 0)
    ec = iota2((64, 256), 1)
    spread = pick(((er >> 3) == (ec >> 5)) & ((er & 7) == ((ec & 15) >> 1)))
    for c in range(5):
        cols = dot_nt(choose, u[c].reshape(64, 128))
        both = dot(cols, spread)
        gz[c] = jnp.where(s < 4, both[:, :128], both[:, 128:]).reshape(3, 8, 128)


def fine_kernel(*refs, stage):
    refs = list(refs)
    info, s, rl, rh = refs[:4]
    del refs[:4]
    theta = (0.0, 0.5, 0.5, 1.0)[stage]
    old = new = base = regs = None
    if theta < 1.0:
        old = refs[:2]
        del refs[:2]
    if theta > 0.0:
        new = refs[:2]
        del refs[:2]
    if stage % 2:
        base = refs.pop(0)
    if stage:
        regs = refs[:2]
        del refs[:2]
    out = refs.pop(0)
    if stage < 3:
        lo, hi = refs[:2]
        del refs[:2]
    rx, rz, q, sl, sr, fx, d, pr, near = refs

    sub = subs()
    upper_x = sub >= 4
    second = (sub & 2) != 0
    upper_z = (sub & 1) != 0

    def ghost(which, c, g):
        if theta == 0.0:
            return old[which][c, g]
        if theta == 1.0:
            return new[which][c, g]
        return 0.5 * old[which][c, g] + 0.5 * new[which][c, g]

    near[:, :, 0:4, :] = rl[...]
    near[:, :, 4:8, :] = rh[...]
    code = jnp.where(
        upper_x,
        jnp.where(second, info[MATCH + 3], info[MATCH + 2]),
        jnp.where(second, info[MATCH + 1], info[MATCH]),
    )
    none = code == 2
    same = code == jnp.where(second, 1, 0)

    for m in range(8):
        p = prims_of([s[c, m] for c in range(5)])
        for c in range(5):
            q[c, m + 3] = p[c]
            pr[c, m] = p[c]
    for g in range(3):
        state = []
        for c in range(5):
            v = near[c, g]
            other = jnp.where(second, roll(v, 2, 0), roll(v, -2, 0))
            state.append(
                jnp.where(none, ghost(0, c, g), jnp.where(same, v, other))
            )
        p = prims_of(state)
        for c in range(5):
            q[c, g] = jnp.where(upper_x, roll(pr[c, g + 5], 4, 0), p[c])
            q[c, g + 11] = jnp.where(upper_x, p[c], roll(pr[c, g], 4, 0))
    major_pass(q, sl, sr, fx, 1)
    for c in range(5):
        face = jnp.where(upper_x, fx[c, 8], fx[c, 0])
        rx[c] = face if regs is None else regs[0][c] + face
        for m in range(8):
            d[c, m] = fx[c, m + 1] - fx[c, m]
    roll_pass(q, d, y_shift, 2)

    adjacent = info[ADJ] == 1
    inner_low = upper_z | (second & adjacent)
    inner_high = jnp.logical_not(upper_z) | (jnp.logical_not(second) & adjacent)
    for c in range(5):
        t = swap_groups([pr[c, m] for m in range(8)])
        for m in range(8):
            q[c, m + 3] = t[m]
    for g in range(3):
        p = prims_of([ghost(1, c, g) for c in range(5)])
        for c in range(5):
            q[c, g] = jnp.where(inner_low, roll(q[c, g + 8], 1, 0), p[c])
            q[c, g + 11] = jnp.where(inner_high, roll(q[c, g + 3], -1, 0), p[c])
    major_pass(q, sl, sr, fx, 3)
    for c in range(5):
        face = jnp.where(upper_z, fx[c, 8], fx[c, 0])
        rz[c] = face if regs is None else regs[1][c] + face
        t = swap_groups([fx[c, m + 1] - fx[c, m] for m in range(8)])
        for m in range(8):
            change = d[c, m] + t[m]
            if base is None:
                out[c, m] = s[c, m] - 0.2 * change
            else:
                out[c, m] = 0.5 * (base[c, m] + s[c, m]) - 0.1 * change
    if stage < 3:
        lo[...] = out[:, 0:3, 0:4, :]
        hi[...] = out[:, 5:8, 4:8, :]


def sync_kernel(info, s, rx, rz, new, mx, mz, out, low, high):
    lane = lanes()
    y = pick(subs() == ((lane & 15) >> 1))
    z0 = [info[Z0], info[Z0 + 1]]
    lr = iota2((128, 128), 0)
    zc = iota2((128, 128), 1)
    spread = [pick(zc == z0[pz // 2] + 4 * (pz % 2) + (lr >> 5)) for pz in range(4)]
    mean = None
    for pz in range(4):
        rows = []
        for c in range(5):
            for x in range(8):
                m, at = 2 * (x % 4), 4 * (x // 4) + pz
                v = s[c, m] + s[c, m + 1]
                rows.append(jnp.broadcast_to(v[at : at + 1], (8, 128)) * y)
        term = dot(jnp.concatenate(rows, axis=0), spread[pz])
        mean = term if mean is None else mean + term
    edge = [[info[MATCH + 2 * side + p] == 2 for p in range(2)] for side in range(2)]
    inside = [(lane >= z0[p]) & (lane < z0[p] + 8) for p in range(2)]
    placed = None
    for pz in range(4):
        rows = []
        for side in range(2):
            for c in range(5):
                v = rx[c]
                at = 4 * side + pz
                rows.append(jnp.broadcast_to(v[at : at + 1], (8, 128)) * y)
        term = dot(jnp.concatenate(rows, axis=0), spread[pz])
        placed = term if placed is None else placed + term
    for side, goal in ((0, low), (1, high)):
        keep = (inside[0] & edge[side][0]) | (inside[1] & edge[side][1])
        for c in range(5):
            at = 8 * (5 * side + c)
            delta = 0.2 * mx[c, side] - 0.0125 * placed[at : at + 8]
            goal[c] = jnp.where(keep, delta if side == 0 else -delta, 0.0)
    adjacent = info[ADJ] == 1
    apart = jnp.logical_not(adjacent)
    at_low = (lane == z0[0] - 1) | ((lane == z0[1] - 1) & apart)
    at_high = (lane == z0[1] + 8) | ((lane == z0[0] + 8) & apart)
    sub = subs()
    is_second = (sub & 2) != 0
    is_high = (sub & 1) != 0
    where_z = jnp.where(is_second, z0[1], z0[0]) + jnp.where(is_high, 8, -1)
    gone = adjacent & (is_second != is_high)
    sign = jnp.where(is_high, 0.0125, -0.0125)
    put = jnp.where((lane == where_z) & jnp.logical_not(gone), sign, 0.0)
    er = iota2((64, 128), 0)
    el = iota2((64, 128), 1)
    group = [
        pick(((er >> 3) == 4 * xh + (el >> 5)) & ((er & 7) == ((el & 15) >> 1)))
        for xh in range(2)
    ]
    covered = inside[0] | inside[1]
    for c in range(5):
        v = rz[c]
        n = dot_nt(group[0], jnp.where(sub < 4, v, 0.0))
        n = n + dot_nt(group[1], jnp.where(sub < 4, 0.0, v))
        fix = dot(n, put)
        for x in range(8):
            f = 0.2 * mz[c, x]
            w = new[c, x] + fix[8 * x : 8 * x + 8]
            w = w + jnp.where(at_low, roll(f, -1, 1), 0.0)
            w = w - jnp.where(at_high, f, 0.0)
            at = 8 * (8 * c + x)
            out[c, x] = jnp.where(covered, 0.125 * mean[at : at + 8], w)


def last_kernel(info, w, left, right, out):
    lane = lanes()
    z0 = [info[Z0], info[Z0 + 1]]
    inside = [(lane >= z0[p]) & (lane < z0[p] + 8) for p in range(2)]
    covered = inside[0] | inside[1]
    for c in range(5):
        first = w[c, 0] + jnp.where(covered, 0.0, left[c])
        final = w[c, 7] + jnp.where(covered, 0.0, right[c])
        out[c, 0] = first[:, :LIVE_Z]
        out[c, 7] = final[:, :LIVE_Z]
        for x in range(1, 7):
            out[c, x] = w[c, x, :, pl.ds(0, LIVE_Z)]


VM = pl.BlockSpec(memory_space=pltpu.VMEM)
SM = pl.BlockSpec(memory_space=pltpu.SMEM)
ANY = pl.BlockSpec(memory_space=pl.ANY)


def call(kernel, name, ins, outs, scratch, args, alias=None):
    shapes = [jax.ShapeDtypeStruct(shape, dtype) for shape, dtype, _ in outs]
    return pl.pallas_call(
        kernel,
        name=name,
        in_specs=ins,
        out_specs=[spec for _, _, spec in outs],
        out_shape=shapes,
        scratch_shapes=scratch,
        input_output_aliases=alias or {},
    )(*args)


def vm(*shape):
    return (shape, f32, VM)


def buf(*shape):
    return pltpu.VMEM(shape, f32)


FIELD = (5, 8, 8, 128)
PASS = [buf(5, 14, 8, 128), buf(5, 10, 8, 128), buf(5, 10, 8, 128), buf(5, 9, 8, 128), buf(*FIELD)]


def ring(axis, up):
    count = DEEP if axis == "deep" else WIDE
    pairs = [(i, (i + 1) % count) for i in range(count)]
    return pairs if up else [(j, i) for i, j in pairs]


def swap(lo, hi, axis):
    return lax.ppermute(hi, axis, ring(axis, True)), lax.ppermute(lo, axis, ring(axis, False))


def local(dens, vel, pres, fdens, fvel, fpres, counts, start):
    here = lax.axis_index("wide").astype(i32).reshape(1)
    (info,) = call(
        info_kernel, "places", [SM] * 3, [((16,), i32, SM)], [], (counts, start, here)
    )
    dma = pltpu.SemaphoreType.DMA
    moved = (WIDE, 5, 32, 128)
    (sent,) = call(
        send_kernel,
        "send_patches",
        [SM, ANY, ANY, ANY],
        [(moved, f32, ANY)],
        [dma((4, 12))],
        (info, fdens, fvel, fpres),
    )
    came = lax.all_to_all(sent, "wide", split_axis=0, concat_axis=0, tiled=True)

    edge = vm(8, 128)
    side = vm(5, 3, 8, 128)
    u0, lo, hi, plo, phi = call(
        prep_kernel,
        "coarse_prep",
        [VM] * 3,
        [vm(*FIELD), side, side, edge, edge],
        [],
        (dens, vel, pres),
    )
    xl0, xh0 = swap(lo, hi, "wide")
    zl0, zh0 = swap(plo, phi, "deep")
    mid, lo, hi, plo, phi, fa, fza = call(
        coarse_one,
        "coarse_one",
        [VM] * 5,
        [vm(*FIELD), side, side, edge, edge, vm(5, 2, 8, 128), vm(*FIELD)],
        PASS,
        (u0, xl0, xh0, zl0, zh0),
    )
    xl1, xh1 = swap(lo, hi, "wide")
    zl1, zh1 = swap(plo, phi, "deep")
    pair = vm(5, 2, 8, 128)
    new, lo, hi, mx, mz = call(
        coarse_two,
        "coarse_two",
        [VM] * 8,
        [vm(*FIELD), pair, pair, pair, vm(*FIELD)],
        PASS,
        (u0, fa, fza, mid, xl1, xh1, zl1, zh1),
    )
    xl2, xh2 = swap(lo, hi, "wide")

    def rims(u, xl, xh, first, name):
        return call(
            lambda *refs: rim_kernel(*refs, first=first),
            name,
            [SM] + [VM] * 3,
            [side, side],
            [],
            (info, u, xl, xh),
        )

    old = rims(u0, xl0, xh0, 1, "rims_old")
    late = rims(new, xl2, xh2, 0, "rims_new")

    strip = vm(5, 3, 4, 128)
    near = buf(5, 64, 128)
    s, flo, fhi = call(
        take_kernel,
        "take_patches",
        [SM, ANY],
        [vm(*FIELD), strip, strip],
        [near, dma((4,))],
        (info, came),
    )
    scratch = PASS + [buf(*FIELD), buf(5, 3, 8, 128)]
    regs = None
    base = None
    for stage in range(4):
        rl, rh = swap(flo, fhi, "wide")
        args = [info, s, rl, rh]
        if stage < 3:
            args += list(old)
        if stage > 0:
            args += list(late)
        if stage % 2:
            args.append(base)
        else:
            base = s
        if stage:
            args += regs
        outs = [vm(*FIELD)] + ([strip, strip] if stage < 3 else [])
        outs += [vm(5, 8, 128), vm(5, 8, 128)]
        got = call(
            lambda *refs, stage=stage: fine_kernel(*refs, stage=stage),
            f"fine_{stage}",
            [SM] + [VM] * (len(args) - 1),
            outs,
            scratch,
            args,
        )
        s = got[0]
        if stage < 3:
            flo, fhi = got[1:3]
        regs = list(got[-2:])
    (gone,) = call(
        give_kernel,
        "give_patches",
        [SM, VM],
        [(moved, f32, ANY)],
        [near, dma((4,))],
        (info, s),
    )
    home = lax.all_to_all(gone, "wide", split_axis=0, concat_axis=0, tiled=True)
    plane = vm(5, 8, 128)
    w, low, high = call(
        sync_kernel,
        "sync",
        [SM] + [VM] * 6,
        [vm(*FIELD), plane, plane],
        [],
        (info, s, regs[0], regs[1], new, mx, mz),
    )
    from_left, from_right = swap(low, high, "wide")
    (coarse_out,) = call(
        last_kernel,
        "coarse_last",
        [SM] + [VM] * 3,
        [vm(5, 8, 8, LIVE_Z)],
        [],
        (info, w, from_left, from_right),
    )
    initial = jnp.stack(
        cons_of([fdens, fvel[:, :, 0], fvel[:, :, 1], fvel[:, :, 2], fpres]), axis=2
    )
    (fine_out,) = call(
        home_kernel,
        "home_patches",
        [SM, ANY, ANY],
        [(initial.shape, f32, ANY)],
        [dma((4, 4))],
        (info, home, initial),
        alias={2: 0},
    )
    return coarse_out, fine_out


def solution(mesh):
    return jax.shard_map(
        local,
        mesh=mesh,
        in_specs=(
            P("wide", None, "deep"),
            P(None, "wide", None, "deep"),
            P("wide", None, "deep"),
            P("deep", "wide", None, None),
            P("deep", "wide", None, None, None),
            P("deep", "wide", None, None),
            P("deep", None),
            P("deep"),
        ),
        out_specs=(P(None, "wide", None, "deep"), P("deep", "wide", None, None, None)),
        check_vma=False,
    )
```

```python
import jax
import jax.numpy as jnp
from jax import lax
from jax.experimental import pallas as pl
from jax.experimental.pallas import tpu as pltpu
from jax.sharding import PartitionSpec as P

f32 = jnp.float32
i32 = jnp.int32
HIGH = lax.Precision.HIGHEST
PLACES = 13
WIDE = 16
DEEP = 8
LIVE_Z = 120
FILL = (1.0, 0.0, 0.0, 0.0, 2.5)


def lanes():
    return lax.broadcasted_iota(i32, (8, 128), 1)


def subs():
    return lax.broadcasted_iota(i32, (8, 128), 0)


def roll(v, shift, axis):
    size = v.shape[axis]
    shift = shift % size
    return v if shift == 0 else pltpu.roll(v, shift, axis)


def y_shift(v, k):
    y = lanes() & 15
    if k > 0:
        return jnp.where(y < 16 - k, roll(v, -k, 1), roll(v, 16 - k, 1))
    return jnp.where(y >= -k, roll(v, -k, 1), roll(v, -k - 16, 1))


def sub_shift(v, k):
    return roll(v, -k, 0)


def lane_shift(v, k):
    return roll(v, -k, 1)


def prims_of(u):
    inv = 1.0 / u[0]
    vx, vy, vz = u[1] * inv, u[2] * inv, u[3] * inv
    kinetic = 0.5 * u[0] * (vx * vx + vy * vy + vz * vz)
    return [u[0], vx, vy, vz, 0.4 * (u[4] - kinetic)]


def cons_of(p):
    kinetic = 0.5 * p[0] * (p[1] * p[1] + p[2] * p[2] + p[3] * p[3])
    return [p[0], p[0] * p[1], p[0] * p[2], p[0] * p[3], p[4] / 0.4 + kinetic]


def recon(a, b, c, d, e):
    da, db, dc, dd = b - a, c - b, d - c, e - d
    ga, gb, gc = db - da, dc - db, dd - dc
    db2, dc2 = db + db, dc + dc
    ta, tb, tc = ga + db2, db + dc, gc - dc2
    k = 13.0 / 3.0
    sa = (k * ga) * ga + (ta * ta + 4e-6)
    sb = (k * gb) * gb + (tb * tb + 4e-6)
    sc = (k * gc) * gc + (tc * tc + 4e-6)
    pa, pb, pc = sa * sa, (sb * sb) * (1.0 / 6.0), sc * sc
    bc, ac, ab = pb * pc, pa * pc, pa * pb
    ab3, bc3 = 3.0 * ab, 3.0 * bc
    db4, dc4 = db2 + db2, dc2 + dc2
    left = bc * (db4 + db - (da + da)) + ac * (db + dc2) + ab3 * (dc4 - dd)
    right = ab * (dc4 + dc - (dd + dd)) + ac * (dc + db2) + bc3 * (db4 - da)
    left = left / (6.0 * (bc + ac + ab3))
    right = right / (6.0 * (ab + ac + bc3))
    return c + left, c - right


def hllc(lt, rt, n):
    o1, o2 = [k for k in (1, 2, 3) if k != n]
    dl, ul, pl_ = lt[0], lt[n], lt[4]
    dr, ur, pr = rt[0], rt[n], rt[4]
    il, ir = 1.0 / dl, 1.0 / dr
    cl = jnp.sqrt(1.4 * pl_ * il)
    cr = jnp.sqrt(1.4 * pr * ir)
    slow = jnp.minimum(ul - cl, ur - cr)
    fast = jnp.maximum(ul + cl, ur + cr)
    ml = dl * (slow - ul)
    mr = dr * (fast - ur)
    mid = (pr - pl_ + ml * ul - mr * ur) / (ml - mr)
    use = (slow >= 0.0) | (mid >= 0.0)
    d = jnp.where(use, dl, dr)
    u = jnp.where(use, ul, ur)
    t1 = jnp.where(use, lt[o1], rt[o1])
    t2 = jnp.where(use, lt[o2], rt[o2])
    p = jnp.where(use, pl_, pr)
    inv = jnp.where(use, il, ir)
    mass = jnp.where(use, ml, mr)
    wave = jnp.where(use, slow, fast)
    star = (use & (slow < 0.0)) | (jnp.logical_not(use) & (fast > 0.0))
    energy = 2.5 * p + 0.5 * d * (u * u + t1 * t1 + t2 * t2)
    du = d * u
    factor = mass / (wave - mid)
    e_star = energy * inv + (mid - u) * (mid + p / mass)
    out = [None] * 5
    flux = {0: du, n: du * u + p, o1: du * t1, o2: du * t2, 4: u * (energy + p)}
    state = {0: d, n: du, o1: d * t1, o2: d * t2, 4: energy}
    goal = {0: factor, n: factor * mid, o1: factor * t1, o2: factor * t2, 4: factor * e_star}
    for c in range(5):
        out[c] = jnp.where(star, flux[c] + wave * (goal[c] - state[c]), flux[c])
    return out


def major_pass(q, sl, sr, fx, n):
    def cells(m, carry):
        for c in range(5):
            l, r = recon(*[q[c, m + k] for k in range(5)])
            sl[c, m] = l
            sr[c, m] = r
        return carry

    lax.fori_loop(0, 10, cells, 0)

    def faces(g, carry):
        for j in range(3):
            f = g * 3 + j
            out = hllc([sl[c, f] for c in range(5)], [sr[c, f + 1] for c in range(5)], n)
            for c in range(5):
                fx[c, f] = out[c]
        return carry

    lax.fori_loop(0, 3, faces, 0)


def roll_pass(q, d, shift, n, keep=None):
    def cells(m, carry):
        left, right = [], []
        for c in range(5):
            v = q[c, m + 3]
            l, r = recon(shift(v, -2), shift(v, -1), v, shift(v, 1), shift(v, 2))
            left.append(shift(l, -1))
            right.append(r)
        out = hllc(left, right, n)
        for c in range(5):
            d[c, m] = d[c, m] + (shift(out[c], 1) - out[c])
            if keep is not None:
                keep[c, m] = out[c]
        return carry

    lax.fori_loop(0, 8, cells, 0)


def swap_groups(v):
    lane = lanes()
    for b in range(3):
        bit = ((lane >> (4 + b)) & 1) == 1
        step = 16 << b
        w = list(v)
        for m in range(8):
            if not (m >> b) & 1:
                lo, hi = v[m], v[m | (1 << b)]
                w[m] = jnp.where(bit, roll(hi, step, 1), lo)
                w[m | (1 << b)] = jnp.where(bit, hi, roll(lo, -step, 1))
        v = w
    return v


Z0, OWNER, COL, COUNT, ADJ, MATCH = 0, 2, 4, 8, 9, 10


def column_places(column, anchor):
    d = (column - anchor) & 15
    bad = 2 - lax.rem(d, 3)
    off_a = d + 16 * jnp.where(bad == 0, 1, 0)
    off_b = d + 16 * jnp.where(bad == 2, 1, 2)

    def ident(off):
        place = anchor + off
        return jnp.where(place >= WIDE * PLACES, place - WIDE * PLACES, place)

    swap = ident(off_b) < ident(off_a)
    first = jnp.where(swap, off_b, off_a)
    second = jnp.where(swap, off_a, off_b)
    heights = [ident(first) >> 4, ident(second) >> 4]
    ranks = [2 * lax.div(o, 3) + lax.rem(o, 3) for o in (first, second)]
    return heights, ranks


def info_kernel(counts, start, here, info):
    me = here[0]
    anchor = start[0]
    h, ranks = column_places(me, anchor)
    low, _ = column_places((me + 15) & 15, anchor)
    high, _ = column_places((me + 1) & 15, anchor)
    total = jnp.int32(0)
    begin = jnp.int32(0)
    mine = jnp.int32(0)
    owner = [jnp.int32(0), jnp.int32(0)]
    for w in range(WIDE):
        n = counts[0, w]
        begin = jnp.where(me == w, total, begin)
        mine = jnp.where(me == w, n, mine)
        total = total + n
        for p in range(2):
            owner[p] = owner[p] + jnp.where(ranks[p] >= total, 1, 0)
    for p in range(2):
        info[Z0 + p] = 8 * (h[p] + 1)
        info[OWNER + p] = jnp.minimum(owner[p], WIDE - 1)
        for side, other in enumerate((low, high)):
            info[MATCH + 2 * side + p] = jnp.where(
                other[0] == h[p], 0, jnp.where(other[1] == h[p], 1, 2)
            )
    for s in range(4):
        serial = begin + s
        place = anchor + 3 * (serial >> 1) + (serial & 1)
        info[COL + s] = place & 15
    info[COUNT] = mine
    info[ADJ] = jnp.where(h[1] == h[0] + 1, 1, 0)
    info[14] = 0
    info[15] = 0


def send_kernel(info, dens, vel, pres, out, sem):
    for s in range(4):

        @pl.when(s < info[COUNT])
        def _():
            copies = slot_copies(info, dens, vel, pres, out, sem, s)
            for cp in copies:
                cp.start()

    for s in range(4):

        @pl.when(s < info[COUNT])
        def _():
            for cp in slot_copies(info, dens, vel, pres, out, sem, s):
                cp.wait()


def slot_copies(info, dens, vel, pres, out, sem, s):
    to = info[COL + s]
    copies = []
    for xh in range(2):
        for zh in range(2):
            rows, cols = pl.ds(8 * xh, 8), pl.ds(128 * zh, 128)
            goal = pl.ds(16 * xh + 8 * zh, 8)
            k = 2 * xh + zh
            copies.append(
                pltpu.make_async_copy(
                    dens.at[0, s, rows, cols], out.at[to, 0, goal, :], sem.at[s, 3 * k]
                )
            )
            copies.append(
                pltpu.make_async_copy(
                    vel.at[0, s, :, rows, cols],
                    out.at[to, pl.ds(1, 3), goal, :],
                    sem.at[s, 3 * k + 1],
                )
            )
            copies.append(
                pltpu.make_async_copy(
                    pres.at[0, s, rows, cols], out.at[to, 4, goal, :], sem.at[s, 3 * k + 2]
                )
            )
    return copies


def patch_copies(info, far, near, sem, out):
    copies = []
    for p in range(2):
        for xh in range(2):
            there = far.at[info[OWNER + p], :, pl.ds(16 * xh, 16), :]
            here = near.at[:, pl.ds((4 * xh + 2 * p) * 8, 16), :]
            a, b = (here, there) if out else (there, here)
            copies.append(pltpu.make_async_copy(a, b, sem.at[2 * p + xh]))
    return copies


def take_kernel(info, far, s, lo, hi, near, sem):
    copies = patch_copies(info, far, near, sem, False)
    for cp in copies:
        cp.start()
    for cp in copies:
        cp.wait()
    for m in range(8):
        u = cons_of([near[c, pl.ds(m, 8, stride=8), :] for c in range(5)])
        for c in range(5):
            s[c, m] = u[c]
    lo[...] = s[:, 0:3, 0:4, :]
    hi[...] = s[:, 5:8, 4:8, :]


def give_kernel(info, s, far, near, sem):
    for m in range(8):
        for c in range(5):
            near[c, pl.ds(m, 8, stride=8), :] = s[c, m]
    copies = patch_copies(info, far, near, sem, True)
    for cp in copies:
        cp.start()
    for cp in copies:
        cp.wait()


def home_copies(info, far, out, sem, s):
    copies = []
    for xh in range(2):
        for zh in range(2):
            copies.append(
                pltpu.make_async_copy(
                    far.at[info[COL + s], :, pl.ds(16 * xh + 8 * zh, 8), :],
                    out.at[0, s, :, pl.ds(8 * xh, 8), pl.ds(128 * zh, 128)],
                    sem.at[s, 2 * xh + zh],
                )
            )
    return copies


def home_kernel(info, far, initial, out, sem):
    for s in range(4):

        @pl.when(s < info[COUNT])
        def _():
            for cp in home_copies(info, far, out, sem, s):
                cp.start()

    for s in range(4):

        @pl.when(s < info[COUNT])
        def _():
            for cp in home_copies(info, far, out, sem, s):
                cp.wait()


def pack_edge(u, first):
    lane = lanes()
    out = jnp.zeros((8, 128), f32)
    for c in range(5):
        for x in range(8):
            k = 3 * (8 * c + x)
            out = jnp.where((lane >= k) & (lane < k + 3), roll(u[c, x], k - first, 1), out)
    return out


def prep_kernel(dens, vel, pres, u, lo, hi, plo, phi):
    state = cons_of([dens[...], vel[0], vel[1], vel[2], pres[...]])
    for c in range(5):
        u[c] = jnp.full((8, 8, 128), FILL[c], f32)
        u[c, :, :, pl.ds(0, LIVE_Z)] = state[c]
    lo[...] = u[:, 0:3]
    hi[...] = u[:, 5:8]
    plo[...] = pack_edge(u, 0)
    phi[...] = pack_edge(u, LIVE_Z - 3)


def coarse_rates(u, xl, xh, zl, zh, q, sl, sr, fx, d, keep):
    lane = lanes()
    below, above = zl[...], zh[...]
    for m in range(8):
        state = []
        for c in range(5):
            k = 3 * (8 * c + m)
            v = jnp.where(lane >= 125, roll(below, 125 - k, 1), u[c, m])
            state.append(
                jnp.where((lane >= 120) & (lane < 123), roll(above, 120 - k, 1), v)
            )
        p = prims_of(state)
        for c in range(5):
            q[c, m + 3] = p[c]
    for g in range(3):
        for ref, at in ((xl, g), (xh, g + 11)):
            p = prims_of([ref[c, g] for c in range(5)])
            for c in range(5):
                q[c, at] = p[c]
    major_pass(q, sl, sr, fx, 1)
    for m in range(8):
        for c in range(5):
            d[c, m] = fx[c, m + 1] - fx[c, m]
    roll_pass(q, d, sub_shift, 2)
    roll_pass(q, d, lane_shift, 3, keep)


def coarse_one(u, xl, xh, zl, zh, mid, lo, hi, plo, phi, fa, fz, q, sl, sr, fx, d):
    coarse_rates(u, xl, xh, zl, zh, q, sl, sr, fx, d, fz)
    live = lanes() < LIVE_Z
    for c in range(5):
        fa[c, 0] = fx[c, 0]
        fa[c, 1] = fx[c, 8]
        for m in range(8):
            mid[c, m] = jnp.where(live, u[c, m] - 0.2 * d[c, m], FILL[c])
    lo[...] = mid[:, 0:3]
    hi[...] = mid[:, 5:8]
    plo[...] = pack_edge(mid, 0)
    phi[...] = pack_edge(mid, LIVE_Z - 3)


def coarse_two(u0, fa, fza, u, xl, xh, zl, zh, new, lo, hi, mx, mz, q, sl, sr, fx, d):
    coarse_rates(u, xl, xh, zl, zh, q, sl, sr, fx, d, mz)
    live = lanes() < LIVE_Z
    for c in range(5):
        mx[c, 0] = 0.5 * (fa[c, 0] + fx[c, 0])
        mx[c, 1] = 0.5 * (fa[c, 1] + fx[c, 8])
        for m in range(8):
            mz[c, m] = 0.5 * (fza[c, m] + mz[c, m])
            new[c, m] = jnp.where(
                live, 0.5 * (u0[c, m] + u[c, m]) - 0.1 * d[c, m], FILL[c]
            )
    lo[...] = new[:, 0:2]
    hi[...] = new[:, 6:8]


def dot(a, b):
    return jnp.dot(a, b, precision=HIGH, preferred_element_type=f32)


def dot_nt(a, b):
    return lax.dot_general(
        a, b, (((1,), (1,)), ((), ())), precision=HIGH, preferred_element_type=f32
    )


def iota2(shape, axis):
    return lax.broadcasted_iota(i32, shape, axis)


def pick(cond):
    return jnp.where(cond, 1.0, 0.0).astype(f32)


def rim_kernel(info, u, xl, xh, gx, gz, *, first):
    z = iota2((128, 128), 0)
    l = iota2((128, 128), 1)
    y8 = iota2((32, 128), 0) & 7
    ymask = pick(y8 == ((iota2((32, 128), 1) & 15) >> 1))
    layers = []
    for c in range(5):
        layers += [xl[c, first], xl[c, first + 1], xh[c, 0], xh[c, 1]]
    rows = jnp.concatenate(layers, axis=0)
    parts = []
    for pz in range(4):
        start = info[Z0 + pz // 2] + 4 * (pz % 2)
        parts.append(dot(rows, pick(z == start + (l >> 5))))
    r = iota2((24, 128), 0)
    k = iota2((24, 128), 1)
    g, s = r >> 3, r & 7
    layer = jnp.where(s < 4, jnp.where(g == 0, 0, 1), jnp.where(g == 2, 3, 2))
    left = pick(((s & 3) == (k >> 5)) & (layer == ((k >> 3) & 3)))
    for c in range(5):
        stack = jnp.concatenate([part[32 * c : 32 * c + 32] * ymask for part in parts], axis=0)
        gx[c] = dot(left, stack).reshape(3, 8, 128)
    pnum = (s >> 1) & 1
    start = jnp.where(pnum == 0, info[Z0], info[Z0 + 1])
    off = jnp.where((s & 1) == 0, jnp.where(g == 0, -2, -1), jnp.where(g == 2, 9, 8))
    choose = pick(k == start + off)
    er = iota2((64, 256), 0)
    ec = iota2((64, 256), 1)
    spread = pick(((er >> 3) == (ec >> 5)) & ((er & 7) == ((ec & 15) >> 1)))
    for c in range(5):
        cols = dot_nt(choose, u[c].reshape(64, 128))
        both = dot(cols, spread)
        gz[c] = jnp.where(s < 4, both[:, :128], both[:, 128:]).reshape(3, 8, 128)


def fine_kernel(*refs, stage):
    refs = list(refs)
    info, s, rl, rh = refs[:4]
    del refs[:4]
    theta = (0.0, 0.5, 0.5, 1.0)[stage]
    old = new = base = regs = None
    if theta < 1.0:
        old = refs[:2]
        del refs[:2]
    if theta > 0.0:
        new = refs[:2]
        del refs[:2]
    if stage % 2:
        base = refs.pop(0)
    if stage:
        regs = refs[:2]
        del refs[:2]
    out = refs.pop(0)
    if stage < 3:
        lo, hi = refs[:2]
        del refs[:2]
    rx, rz, q, sl, sr, fx, d, pr, near = refs

    sub = subs()
    upper_x = sub >= 4
    second = (sub & 2) != 0
    upper_z = (sub & 1) != 0

    def ghost(which, c, g):
        if theta == 0.0:
            return old[which][c, g]
        if theta == 1.0:
            return new[which][c, g]
        return 0.5 * old[which][c, g] + 0.5 * new[which][c, g]

    near[:, :, 0:4, :] = rl[...]
    near[:, :, 4:8, :] = rh[...]
    code = jnp.where(
        upper_x,
        jnp.where(second, info[MATCH + 3], info[MATCH + 2]),
        jnp.where(second, info[MATCH + 1], info[MATCH]),
    )
    none = code == 2
    same = code == jnp.where(second, 1, 0)

    for m in range(8):
        p = prims_of([s[c, m] for c in range(5)])
        for c in range(5):
            q[c, m + 3] = p[c]
            pr[c, m] = p[c]
    for g in range(3):
        state = []
        for c in range(5):
            v = near[c, g]
            other = jnp.where(second, roll(v, 2, 0), roll(v, -2, 0))
            state.append(
                jnp.where(none, ghost(0, c, g), jnp.where(same, v, other))
            )
        p = prims_of(state)
        for c in range(5):
            q[c, g] = jnp.where(upper_x, roll(pr[c, g + 5], 4, 0), p[c])
            q[c, g + 11] = jnp.where(upper_x, p[c], roll(pr[c, g], 4, 0))
    major_pass(q, sl, sr, fx, 1)
    for c in range(5):
        face = jnp.where(upper_x, fx[c, 8], fx[c, 0])
        rx[c] = face if regs is None else regs[0][c] + face
        for m in range(8):
            d[c, m] = fx[c, m + 1] - fx[c, m]
    roll_pass(q, d, y_shift, 2)

    adjacent = info[ADJ] == 1
    inner_low = upper_z | (second & adjacent)
    inner_high = jnp.logical_not(upper_z) | (jnp.logical_not(second) & adjacent)
    for c in range(5):
        t = swap_groups([pr[c, m] for m in range(8)])
        for m in range(8):
            q[c, m + 3] = t[m]
    for g in range(3):
        p = prims_of([ghost(1, c, g) for c in range(5)])
        for c in range(5):
            q[c, g] = jnp.where(inner_low, roll(q[c, g + 8], 1, 0), p[c])
            q[c, g + 11] = jnp.where(inner_high, roll(q[c, g + 3], -1, 0), p[c])
    major_pass(q, sl, sr, fx, 3)
    for c in range(5):
        face = jnp.where(upper_z, fx[c, 8], fx[c, 0])
        rz[c] = face if regs is None else regs[1][c] + face
        t = swap_groups([fx[c, m + 1] - fx[c, m] for m in range(8)])
        for m in range(8):
            change = d[c, m] + t[m]
            if base is None:
                out[c, m] = s[c, m] - 0.2 * change
            else:
                out[c, m] = 0.5 * (base[c, m] + s[c, m]) - 0.1 * change
    if stage < 3:
        lo[...] = out[:, 0:3, 0:4, :]
        hi[...] = out[:, 5:8, 4:8, :]


def sync_kernel(info, s, rx, rz, new, mx, mz, out, low, high):
    lane = lanes()
    y = pick(subs() == ((lane & 15) >> 1))
    z0 = [info[Z0], info[Z0 + 1]]
    lr = iota2((128, 128), 0)
    zc = iota2((128, 128), 1)
    spread = [pick(zc == z0[pz // 2] + 4 * (pz % 2) + (lr >> 5)) for pz in range(4)]
    mean = None
    for pz in range(4):
        rows = []
        for c in range(5):
            for x in range(8):
                m, at = 2 * (x % 4), 4 * (x // 4) + pz
                v = s[c, m] + s[c, m + 1]
                rows.append(jnp.broadcast_to(v[at : at + 1], (8, 128)) * y)
        term = dot(jnp.concatenate(rows, axis=0), spread[pz])
        mean = term if mean is None else mean + term
    edge = [[info[MATCH + 2 * side + p] == 2 for p in range(2)] for side in range(2)]
    inside = [(lane >= z0[p]) & (lane < z0[p] + 8) for p in range(2)]
    placed = None
    for pz in range(4):
        rows = []
        for side in range(2):
            for c in range(5):
                v = rx[c]
                at = 4 * side + pz
                rows.append(jnp.broadcast_to(v[at : at + 1], (8, 128)) * y)
        term = dot(jnp.concatenate(rows, axis=0), spread[pz])
        placed = term if placed is None else placed + term
    for side, goal in ((0, low), (1, high)):
        keep = (inside[0] & edge[side][0]) | (inside[1] & edge[side][1])
        for c in range(5):
            at = 8 * (5 * side + c)
            delta = 0.2 * mx[c, side] - 0.0125 * placed[at : at + 8]
            goal[c] = jnp.where(keep, delta if side == 0 else -delta, 0.0)
    adjacent = info[ADJ] == 1
    apart = jnp.logical_not(adjacent)
    at_low = (lane == z0[0] - 1) | ((lane == z0[1] - 1) & apart)
    at_high = (lane == z0[1] + 8) | ((lane == z0[0] + 8) & apart)
    sub = subs()
    is_second = (sub & 2) != 0
    is_high = (sub & 1) != 0
    where_z = jnp.where(is_second, z0[1], z0[0]) + jnp.where(is_high, 8, -1)
    gone = adjacent & (is_second != is_high)
    sign = jnp.where(is_high, 0.0125, -0.0125)
    put = jnp.where((lane == where_z) & jnp.logical_not(gone), sign, 0.0)
    er = iota2((64, 128), 0)
    el = iota2((64, 128), 1)
    group = [
        pick(((er >> 3) == 4 * xh + (el >> 5)) & ((er & 7) == ((el & 15) >> 1)))
        for xh in range(2)
    ]
    covered = inside[0] | inside[1]
    for c in range(5):
        v = rz[c]
        n = dot_nt(group[0], jnp.where(sub < 4, v, 0.0))
        n = n + dot_nt(group[1], jnp.where(sub < 4, 0.0, v))
        fix = dot(n, put)
        for x in range(8):
            f = 0.2 * mz[c, x]
            w = new[c, x] + fix[8 * x : 8 * x + 8]
            w = w + jnp.where(at_low, roll(f, -1, 1), 0.0)
            w = w - jnp.where(at_high, f, 0.0)
            at = 8 * (8 * c + x)
            out[c, x] = jnp.where(covered, 0.125 * mean[at : at + 8], w)


def last_kernel(info, w, left, right, out):
    lane = lanes()
    z0 = [info[Z0], info[Z0 + 1]]
    inside = [(lane >= z0[p]) & (lane < z0[p] + 8) for p in range(2)]
    covered = inside[0] | inside[1]
    for c in range(5):
        first = w[c, 0] + jnp.where(covered, 0.0, left[c])
        final = w[c, 7] + jnp.where(covered, 0.0, right[c])
        out[c, 0] = first[:, :LIVE_Z]
        out[c, 7] = final[:, :LIVE_Z]
        for x in range(1, 7):
            out[c, x] = w[c, x, :, pl.ds(0, LIVE_Z)]


VM = pl.BlockSpec(memory_space=pltpu.VMEM)
SM = pl.BlockSpec(memory_space=pltpu.SMEM)
LIMIT = 8 << 20
ANY = pl.BlockSpec(memory_space=pl.ANY)


def call(kernel, name, ins, outs, scratch, args, alias=None):
    shapes = [jax.ShapeDtypeStruct(shape, dtype) for shape, dtype, _ in outs]
    return pl.pallas_call(
        kernel,
        name=name,
        in_specs=ins,
        out_specs=[spec for _, _, spec in outs],
        out_shape=shapes,
        scratch_shapes=scratch,
        input_output_aliases=alias or {},
        compiler_params=pltpu.CompilerParams(vmem_limit_bytes=LIMIT),
    )(*args)


def vm(*shape):
    return (shape, f32, VM)


def buf(*shape):
    return pltpu.VMEM(shape, f32)


FIELD = (5, 8, 8, 128)
PASS = [buf(5, 14, 8, 128), buf(5, 10, 8, 128), buf(5, 10, 8, 128), buf(5, 9, 8, 128), buf(*FIELD)]


def ring(axis, up):
    count = DEEP if axis == "deep" else WIDE
    pairs = [(i, (i + 1) % count) for i in range(count)]
    return pairs if up else [(j, i) for i, j in pairs]


def swap(lo, hi, axis):
    return lax.ppermute(hi, axis, ring(axis, True)), lax.ppermute(lo, axis, ring(axis, False))


def local(dens, vel, pres, fdens, fvel, fpres, counts, start):
    here = lax.axis_index("wide").astype(i32).reshape(1)
    (info,) = call(
        info_kernel, "places", [SM] * 3, [((16,), i32, SM)], [], (counts, start, here)
    )
    dma = pltpu.SemaphoreType.DMA
    moved = (WIDE, 5, 32, 128)
    (sent,) = call(
        send_kernel,
        "send_patches",
        [SM, ANY, ANY, ANY],
        [(moved, f32, ANY)],
        [dma((4, 12))],
        (info, fdens, fvel, fpres),
    )
    came = lax.all_to_all(sent, "wide", split_axis=0, concat_axis=0, tiled=True)

    edge = vm(8, 128)
    side = vm(5, 3, 8, 128)
    u0, lo, hi, plo, phi = call(
        prep_kernel,
        "coarse_prep",
        [VM] * 3,
        [vm(*FIELD), side, side, edge, edge],
        [],
        (dens, vel, pres),
    )
    xl0, xh0 = swap(lo, hi, "wide")
    zl0, zh0 = swap(plo, phi, "deep")
    mid, lo, hi, plo, phi, fa, fza = call(
        coarse_one,
        "coarse_one",
        [VM] * 5,
        [vm(*FIELD), side, side, edge, edge, vm(5, 2, 8, 128), vm(*FIELD)],
        PASS,
        (u0, xl0, xh0, zl0, zh0),
    )
    xl1, xh1 = swap(lo, hi, "wide")
    zl1, zh1 = swap(plo, phi, "deep")
    pair = vm(5, 2, 8, 128)
    new, lo, hi, mx, mz = call(
        coarse_two,
        "coarse_two",
        [VM] * 8,
        [vm(*FIELD), pair, pair, pair, vm(*FIELD)],
        PASS,
        (u0, fa, fza, mid, xl1, xh1, zl1, zh1),
    )
    xl2, xh2 = swap(lo, hi, "wide")

    def rims(u, xl, xh, first, name):
        return call(
            lambda *refs: rim_kernel(*refs, first=first),
            name,
            [SM] + [VM] * 3,
            [side, side],
            [],
            (info, u, xl, xh),
        )

    old = rims(u0, xl0, xh0, 1, "rims_old")
    late = rims(new, xl2, xh2, 0, "rims_new")

    strip = vm(5, 3, 4, 128)
    near = buf(5, 64, 128)
    s, flo, fhi = call(
        take_kernel,
        "take_patches",
        [SM, ANY],
        [vm(*FIELD), strip, strip],
        [near, dma((4,))],
        (info, came),
    )
    scratch = PASS + [buf(*FIELD), buf(5, 3, 8, 128)]
    regs = None
    base = None
    for stage in range(4):
        rl, rh = swap(flo, fhi, "wide")
        args = [info, s, rl, rh]
        if stage < 3:
            args += list(old)
        if stage > 0:
            args += list(late)
        if stage % 2:
            args.append(base)
        else:
            base = s
        if stage:
            args += regs
        outs = [vm(*FIELD)] + ([strip, strip] if stage < 3 else [])
        outs += [vm(5, 8, 128), vm(5, 8, 128)]
        got = call(
            lambda *refs, stage=stage: fine_kernel(*refs, stage=stage),
            f"fine_{stage}",
            [SM] + [VM] * (len(args) - 1),
            outs,
            scratch,
            args,
        )
        s = got[0]
        if stage < 3:
            flo, fhi = got[1:3]
        regs = list(got[-2:])
    (gone,) = call(
        give_kernel,
        "give_patches",
        [SM, VM],
        [(moved, f32, ANY)],
        [near, dma((4,))],
        (info, s),
    )
    home = lax.all_to_all(gone, "wide", split_axis=0, concat_axis=0, tiled=True)
    plane = vm(5, 8, 128)
    w, low, high = call(
        sync_kernel,
        "sync",
        [SM] + [VM] * 6,
        [vm(*FIELD), plane, plane],
        [],
        (info, s, regs[0], regs[1], new, mx, mz),
    )
    from_left, from_right = swap(low, high, "wide")
    (coarse_out,) = call(
        last_kernel,
        "coarse_last",
        [SM] + [VM] * 3,
        [vm(5, 8, 8, LIVE_Z)],
        [],
        (info, w, from_left, from_right),
    )
    initial = jnp.stack(
        cons_of([fdens, fvel[:, :, 0], fvel[:, :, 1], fvel[:, :, 2], fpres]), axis=2
    )
    (fine_out,) = call(
        home_kernel,
        "home_patches",
        [SM, ANY, ANY],
        [(initial.shape, f32, ANY)],
        [dma((4, 4))],
        (info, home, initial),
        alias={2: 0},
    )
    return coarse_out, fine_out


def solution(mesh):
    return jax.shard_map(
        local,
        mesh=mesh,
        in_specs=(
            P("wide", None, "deep"),
            P(None, "wide", None, "deep"),
            P("wide", None, "deep"),
            P("deep", "wide", None, None),
            P("deep", "wide", None, None, None),
            P("deep", "wide", None, None),
            P("deep", None),
            P("deep"),
        ),
        out_specs=(P(None, "wide", None, "deep"), P("deep", "wide", None, None, None)),
        check_vma=False,
    )
```

```python
import jax
import jax.numpy as jnp
from jax import lax
from jax.experimental import pallas as pl
from jax.experimental.pallas import tpu as pltpu
from jax.sharding import PartitionSpec as P


f32 = jnp.float32
i32 = jnp.int32
HIGH = lax.Precision.HIGHEST
PLACES = 13
WIDE = 16
DEEP = 8
LIVE_Z = 120
FILL = (1.0, 0.0, 0.0, 0.0, 2.5)


def lanes():
    return lax.broadcasted_iota(i32, (8, 128), 1)


def subs():
    return lax.broadcasted_iota(i32, (8, 128), 0)


def roll(v, shift, axis):
    size = v.shape[axis]
    shift = shift % size
    return v if shift == 0 else pltpu.roll(v, shift, axis)


def y_shift(v, k):
    y = lanes() & 15
    if k > 0:
        return jnp.where(y < 16 - k, roll(v, -k, 1), roll(v, 16 - k, 1))
    return jnp.where(y >= -k, roll(v, -k, 1), roll(v, -k - 16, 1))


def sub_shift(v, k):
    return roll(v, -k, 0)


def lane_shift(v, k):
    return roll(v, -k, 1)


def prims_of(u):
    inv = 1.0 / u[0]
    vx, vy, vz = u[1] * inv, u[2] * inv, u[3] * inv
    kinetic = 0.5 * u[0] * (vx * vx + vy * vy + vz * vz)
    return [u[0], vx, vy, vz, 0.4 * (u[4] - kinetic)]


def cons_of(p):
    kinetic = 0.5 * p[0] * (p[1] * p[1] + p[2] * p[2] + p[3] * p[3])
    return [p[0], p[0] * p[1], p[0] * p[2], p[0] * p[3], p[4] / 0.4 + kinetic]


def recon(a, b, c, d, e):
    da, db, dc, dd = b - a, c - b, d - c, e - d
    ga, gb, gc = db - da, dc - db, dd - dc
    db2, dc2 = db + db, dc + dc
    ta, tb, tc = ga + db2, db + dc, gc - dc2
    k = 13.0 / 3.0
    sa = (k * ga) * ga + (ta * ta + 4e-6)
    sb = (k * gb) * gb + (tb * tb + 4e-6)
    sc = (k * gc) * gc + (tc * tc + 4e-6)
    pa, pb, pc = sa * sa, (sb * sb) * (1.0 / 6.0), sc * sc
    bc, ac, ab = pb * pc, pa * pc, pa * pb
    ab3, bc3 = 3.0 * ab, 3.0 * bc
    db4, dc4 = db2 + db2, dc2 + dc2
    left = bc * (db4 + db - (da + da)) + ac * (db + dc2) + ab3 * (dc4 - dd)
    right = ab * (dc4 + dc - (dd + dd)) + ac * (dc + db2) + bc3 * (db4 - da)
    left = left / (6.0 * (bc + ac + ab3))
    right = right / (6.0 * (ab + ac + bc3))
    return c + left, c - right


def hllc(lt, rt, n):
    o1, o2 = [k for k in (1, 2, 3) if k != n]
    dl, ul, pl_ = lt[0], lt[n], lt[4]
    dr, ur, pr = rt[0], rt[n], rt[4]
    il, ir = 1.0 / dl, 1.0 / dr
    cl = jnp.sqrt(1.4 * pl_ * il)
    cr = jnp.sqrt(1.4 * pr * ir)
    slow = jnp.minimum(ul - cl, ur - cr)
    fast = jnp.maximum(ul + cl, ur + cr)
    ml = dl * (slow - ul)
    mr = dr * (fast - ur)
    mid = (pr - pl_ + ml * ul - mr * ur) / (ml - mr)
    use = (slow >= 0.0) | (mid >= 0.0)
    d = jnp.where(use, dl, dr)
    u = jnp.where(use, ul, ur)
    t1 = jnp.where(use, lt[o1], rt[o1])
    t2 = jnp.where(use, lt[o2], rt[o2])
    p = jnp.where(use, pl_, pr)
    inv = jnp.where(use, il, ir)
    mass = jnp.where(use, ml, mr)
    wave = jnp.where(use, slow, fast)
    star = (use & (slow < 0.0)) | (jnp.logical_not(use) & (fast > 0.0))
    energy = 2.5 * p + 0.5 * d * (u * u + t1 * t1 + t2 * t2)
    du = d * u
    factor = mass / (wave - mid)
    e_star = energy * inv + (mid - u) * (mid + p / mass)
    out = [None] * 5
    flux = {0: du, n: du * u + p, o1: du * t1, o2: du * t2, 4: u * (energy + p)}
    state = {0: d, n: du, o1: d * t1, o2: d * t2, 4: energy}
    goal = {0: factor, n: factor * mid, o1: factor * t1, o2: factor * t2, 4: factor * e_star}
    for c in range(5):
        out[c] = jnp.where(star, flux[c] + wave * (goal[c] - state[c]), flux[c])
    return out


def repeat(count, unroll, body):
    turns = count // unroll

    def turn(t, carry):
        for j in range(unroll):
            body(t * unroll + j)
        return carry

    if turns > 0:
        lax.fori_loop(0, turns, turn, 0)
    for j in range(turns * unroll, count):
        body(j)


UNROLL_CELLS, UNROLL_FACES, UNROLL_ROLLS = 2, 9, 4


def major_pass(q, sl, sr, fx, n, count=10):
    def cells(m):
        for c in range(5):
            l, r = recon(*[q[c, m + k] for k in range(5)])
            sl[c, m] = l
            sr[c, m] = r

    repeat(count, UNROLL_CELLS, cells)

    def faces(f):
        out = hllc([sl[c, f] for c in range(5)], [sr[c, f + 1] for c in range(5)], n)
        for c in range(5):
            fx[c, f] = out[c]

    repeat(count - 1, UNROLL_FACES, faces)


def roll_pass(q, d, shift, n, count=8, keep=None, at=3):
    def cells(m):
        left, right = [], []
        for c in range(5):
            v = q[c, m + at]
            l, r = recon(shift(v, -2), shift(v, -1), v, shift(v, 1), shift(v, 2))
            left.append(shift(l, -1))
            right.append(r)
        out = hllc(left, right, n)
        for c in range(5):
            d[c, m] = d[c, m] + (shift(out[c], 1) - out[c])
            if keep is not None:
                keep[c, m] = out[c]

    repeat(count, UNROLL_ROLLS, cells)


def swap_groups(v):
    lane = lanes()
    for b in range(3):
        bit = ((lane >> (4 + b)) & 1) == 1
        step = 16 << b
        w = list(v)
        for m in range(8):
            if not (m >> b) & 1:
                lo, hi = v[m], v[m | (1 << b)]
                w[m] = jnp.where(bit, roll(hi, step, 1), lo)
                w[m | (1 << b)] = jnp.where(bit, hi, roll(lo, -step, 1))
        v = w
    return v


Z0, OWNER, COL, COUNT, ADJ, MATCH = 0, 2, 4, 8, 9, 10


def column_places(column, anchor):
    d = (column - anchor) & 15
    bad = 2 - lax.rem(d, 3)
    off_a = d + 16 * jnp.where(bad == 0, 1, 0)
    off_b = d + 16 * jnp.where(bad == 2, 1, 2)

    def ident(off):
        place = anchor + off
        return jnp.where(place >= WIDE * PLACES, place - WIDE * PLACES, place)

    swap = ident(off_b) < ident(off_a)
    first = jnp.where(swap, off_b, off_a)
    second = jnp.where(swap, off_a, off_b)
    heights = [ident(first) >> 4, ident(second) >> 4]
    ranks = [2 * lax.div(o, 3) + lax.rem(o, 3) for o in (first, second)]
    return heights, ranks


def info_kernel(counts, start, here, info):
    me = here[0]
    anchor = start[0]
    h, ranks = column_places(me, anchor)
    low, _ = column_places((me + 15) & 15, anchor)
    high, _ = column_places((me + 1) & 15, anchor)
    total = jnp.int32(0)
    begin = jnp.int32(0)
    mine = jnp.int32(0)
    owner = [jnp.int32(0), jnp.int32(0)]
    for w in range(WIDE):
        n = counts[0, w]
        begin = jnp.where(me == w, total, begin)
        mine = jnp.where(me == w, n, mine)
        total = total + n
        for p in range(2):
            owner[p] = owner[p] + jnp.where(ranks[p] >= total, 1, 0)
    for p in range(2):
        info[Z0 + p] = 8 * (h[p] + 1)
        info[OWNER + p] = jnp.minimum(owner[p], WIDE - 1)
        for side, other in enumerate((low, high)):
            info[MATCH + 2 * side + p] = jnp.where(
                other[0] == h[p], 0, jnp.where(other[1] == h[p], 1, 2)
            )
    for s in range(4):
        serial = begin + s
        place = anchor + 3 * (serial >> 1) + (serial & 1)
        info[COL + s] = place & 15
    info[COUNT] = mine
    info[ADJ] = jnp.where(h[1] == h[0] + 1, 1, 0)
    info[14] = 0
    info[15] = 0


def send_kernel(info, dens, vel, pres, out, sem):
    for s in range(4):

        @pl.when(s < info[COUNT])
        def _():
            copies = slot_copies(info, dens, vel, pres, out, sem, s)
            for cp in copies:
                cp.start()

    for s in range(4):

        @pl.when(s < info[COUNT])
        def _():
            for cp in slot_copies(info, dens, vel, pres, out, sem, s):
                cp.wait()


def slot_copies(info, dens, vel, pres, out, sem, s):
    to = info[COL + s]
    copies = []
    for xh in range(2):
        for zh in range(2):
            rows, cols = pl.ds(8 * xh, 8), pl.ds(128 * zh, 128)
            goal = pl.ds(16 * xh + 8 * zh, 8)
            k = 2 * xh + zh
            copies.append(
                pltpu.make_async_copy(
                    dens.at[0, s, rows, cols], out.at[to, 0, goal, :], sem.at[s, 3 * k]
                )
            )
            copies.append(
                pltpu.make_async_copy(
                    vel.at[0, s, :, rows, cols],
                    out.at[to, pl.ds(1, 3), goal, :],
                    sem.at[s, 3 * k + 1],
                )
            )
            copies.append(
                pltpu.make_async_copy(
                    pres.at[0, s, rows, cols], out.at[to, 4, goal, :], sem.at[s, 3 * k + 2]
                )
            )
    return copies


def patch_copies(info, far, near, sem, out):
    copies = []
    for p in range(2):
        for xh in range(2):
            there = far.at[info[OWNER + p], :, pl.ds(16 * xh, 16), :]
            here = near.at[:, pl.ds((4 * xh + 2 * p) * 8, 16), :]
            a, b = (here, there) if out else (there, here)
            copies.append(pltpu.make_async_copy(a, b, sem.at[2 * p + xh]))
    return copies


def take_kernel(info, far, s, lo, hi, near, sem):
    copies = patch_copies(info, far, near, sem, False)
    for cp in copies:
        cp.start()
    for cp in copies:
        cp.wait()
    for m in range(8):
        u = cons_of([near[c, pl.ds(m, 8, stride=8), :] for c in range(5)])
        for c in range(5):
            s[c, m] = u[c]
    lo[...] = s[:, 0:3, 0:4, :]
    hi[...] = s[:, 5:8, 4:8, :]


def give_kernel(info, s, far, near, sem):
    for m in range(8):
        for c in range(5):
            near[c, pl.ds(m, 8, stride=8), :] = s[c, m]
    copies = patch_copies(info, far, near, sem, True)
    for cp in copies:
        cp.start()
    for cp in copies:
        cp.wait()


def home_copies(info, far, out, sem, s):
    copies = []
    for xh in range(2):
        for zh in range(2):
            copies.append(
                pltpu.make_async_copy(
                    far.at[info[COL + s], :, pl.ds(16 * xh + 8 * zh, 8), :],
                    out.at[0, s, :, pl.ds(8 * xh, 8), pl.ds(128 * zh, 128)],
                    sem.at[s, 2 * xh + zh],
                )
            )
    return copies


def home_kernel(info, far, initial, out, sem):
    for s in range(4):

        @pl.when(s < info[COUNT])
        def _():
            for cp in home_copies(info, far, out, sem, s):
                cp.start()

    for s in range(4):

        @pl.when(s < info[COUNT])
        def _():
            for cp in home_copies(info, far, out, sem, s):
                cp.wait()


def pack_edge(u, first):
    lane = lanes()
    out = jnp.zeros((8, 128), f32)
    for c in range(5):
        for x in range(8):
            k = 3 * (8 * c + x)
            out = jnp.where((lane >= k) & (lane < k + 3), roll(u[c][x], k - first, 1), out)
    return out


def prep_kernel(dens_far, vel_far, pres_far, u, plo, phi, dens, vel, pres, sem):
    pairs = ((dens_far, dens), (vel_far, vel), (pres_far, pres))
    copies = [pltpu.make_async_copy(a, b, sem.at[k]) for k, (a, b) in enumerate(pairs)]
    for cp in copies:
        cp.start()
    for cp in copies:
        cp.wait()
    state = cons_of([dens[...], vel[0], vel[1], vel[2], pres[...]])
    for c in range(5):
        u[c] = jnp.full((8, 8, 128), FILL[c], f32)
        u[c, :, :, pl.ds(0, LIVE_Z)] = state[c]
    plo[...] = pack_edge([[u[c, x] for x in range(8)] for c in range(5)], 0)
    phi[...] = pack_edge([[u[c, x] for x in range(8)] for c in range(5)], LIVE_Z - 3)


def with_halo(v, below, above, k):
    lane = lanes()
    v = jnp.where(lane >= 125, roll(below, 125 - k, 1), v)
    return jnp.where((lane >= 120) & (lane < 123), roll(above, 120 - k, 1), v)


def halo_kernel(u, zl, zh, out):
    below, above = zl[...], zh[...]
    for c in range(5):
        for x in range(8):
            out[c, x] = with_halo(u[c, x], below, above, 3 * (8 * c + x))


def coarse_rates(layers, own, zl, zh, q, sl, sr, fx, d, keep):
    count = len(layers)
    for i, layer in enumerate(layers):
        state = [layer(c) for c in range(5)]
        if own is not None and 0 <= i - own < 8:
            state = [
                with_halo(state[c], zl[...], zh[...], 3 * (8 * c + i - own)) for c in range(5)
            ]
        p = prims_of(state)
        for c in range(5):
            q[c, i] = p[c]
    major_pass(q, sl, sr, fx, 1, count - 4)
    for c in range(5):
        for m in range(count - 6):
            d[c, m] = fx[c, m + 1] - fx[c, m]
    roll_pass(q, d, sub_shift, 2, count - 6)
    roll_pass(q, d, lane_shift, 3, count - 6, keep)


def take_layer(ref, x):
    return lambda c: ref[c, x]


def coarse_one(u, ul, ur, mid, plo, phi, fa, fz, q, sl, sr, fx, d, keep):
    refs = [take_layer(ref, x) for ref in (ul, u, ur) for x in range(8)]
    coarse_rates(refs, None, None, None, q, sl, sr, fx, d, keep)
    live = lanes() < LIVE_Z
    for c in range(5):
        fa[c, 0] = fx[c, 5]
        fa[c, 1] = fx[c, 13]
        for m in range(18):
            mid[c, m] = jnp.where(live, refs[m + 3](c) - 0.2 * d[c, m], FILL[c])
        for m in range(8):
            fz[c, m] = keep[c, m + 5]
    plo[...] = pack_edge([[mid[c, x + 5] for x in range(8)] for c in range(5)], 0)
    phi[...] = pack_edge([[mid[c, x + 5] for x in range(8)] for c in range(5)], LIVE_Z - 3)


def coarse_two(u0, ul, ur, fa, fza, u, zl, zh, new, mx, mz, q, sl, sr, fx, d, keep):
    refs = [take_layer(ref, x) for ref in (ul, u0, ur) for x in range(8)]
    coarse_rates([take_layer(u, m) for m in range(18)], 5, zl, zh, q, sl, sr, fx, d, keep)
    live = lanes() < LIVE_Z
    for c in range(5):
        mx[c, 0] = 0.5 * (fa[c, 0] + fx[c, 2])
        mx[c, 1] = 0.5 * (fa[c, 1] + fx[c, 10])
        for m in range(8):
            mz[c, m] = 0.5 * (fza[c, m] + keep[c, m + 2])
        for m in range(12):
            new[c, m] = jnp.where(
                live, 0.5 * (refs[m + 6](c) + u[c, m + 3]) - 0.1 * d[c, m], FILL[c]
            )


def dot(a, b):
    return jnp.dot(a, b, precision=HIGH, preferred_element_type=f32)


def dot_nt(a, b):
    return lax.dot_general(
        a, b, (((1,), (1,)), ((), ())), precision=HIGH, preferred_element_type=f32
    )


def iota2(shape, axis):
    return lax.broadcasted_iota(i32, shape, axis)


def pick(cond):
    return jnp.where(cond, 1.0, 0.0).astype(f32)


def rim_kernel(info, *refs, late):
    gx, gz = refs[-2:]
    if late:
        new = refs[0]
        low, high = [take_layer(new, 0), take_layer(new, 1)], [take_layer(new, 10), take_layer(new, 11)]
        own = lambda c: new[c, 2:10]
    else:
        u, ul, ur = refs[:3]
        low, high = [take_layer(ul, 6), take_layer(ul, 7)], [take_layer(ur, 0), take_layer(ur, 1)]
        own = lambda c: u[c]
    z = iota2((128, 128), 0)
    l = iota2((128, 128), 1)
    y8 = iota2((32, 128), 0) & 7
    ymask = pick(y8 == ((iota2((32, 128), 1) & 15) >> 1))
    layers = []
    for c in range(5):
        layers += [low[0](c), low[1](c), high[0](c), high[1](c)]
    rows = jnp.concatenate(layers, axis=0)
    parts = []
    for pz in range(4):
        start = info[Z0 + pz // 2] + 4 * (pz % 2)
        parts.append(dot(rows, pick(z == start + (l >> 5))))
    r = iota2((24, 128), 0)
    k = iota2((24, 128), 1)
    g, s = r >> 3, r & 7
    layer = jnp.where(s < 4, jnp.where(g == 0, 0, 1), jnp.where(g == 2, 3, 2))
    left = pick(((s & 3) == (k >> 5)) & (layer == ((k >> 3) & 3)))
    for c in range(5):
        stack = jnp.concatenate([part[32 * c : 32 * c + 32] * ymask for part in parts], axis=0)
        gx[c] = dot(left, stack).reshape(3, 8, 128)
    pnum = (s >> 1) & 1
    start = jnp.where(pnum == 0, info[Z0], info[Z0 + 1])
    off = jnp.where((s & 1) == 0, jnp.where(g == 0, -2, -1), jnp.where(g == 2, 9, 8))
    choose = pick(k == start + off)
    er = iota2((64, 256), 0)
    ec = iota2((64, 256), 1)
    spread = pick(((er >> 3) == (ec >> 5)) & ((er & 7) == ((ec & 15) >> 1)))
    for c in range(5):
        cols = dot_nt(choose, own(c).reshape(64, 128))
        both = dot(cols, spread)
        gz[c] = jnp.where(s < 4, both[:, :128], both[:, 128:]).reshape(3, 8, 128)


def blend(old, new, theta, c, g):
    if theta == 0.0:
        return old[c, g]
    if theta == 1.0:
        return new[c, g]
    return 0.5 * old[c, g] + 0.5 * new[c, g]


def split_refs(refs, flags):
    return [refs.pop(0) if flag else None for flag in flags]


def places_of_rows():
    sub = subs()
    return sub >= 4, (sub & 2) != 0, (sub & 1) != 0


THETA = (0.0, 0.5, 0.5, 1.0)


def yz_kernel(*refs, stage):
    theta = THETA[stage]
    refs = list(refs)
    info, s, old, new, reg = split_refs(refs, (1, 1, theta < 1.0, theta > 0.0, stage))
    pr, d, rz, q, sl, sr, fx = refs
    _, second, upper_z = places_of_rows()
    for m in range(8):
        p = prims_of([s[c, m] for c in range(5)])
        for c in range(5):
            pr[c, m] = p[c]
    adjacent = info[ADJ] == 1
    inner_low = upper_z | (second & adjacent)
    inner_high = jnp.logical_not(upper_z) | (jnp.logical_not(second) & adjacent)
    for c in range(5):
        t = swap_groups([pr[c, m] for m in range(8)])
        for m in range(8):
            q[c, m + 3] = t[m]
    for g in range(3):
        p = prims_of([blend(old, new, theta, c, g) for c in range(5)])
        for c in range(5):
            q[c, g] = jnp.where(inner_low, roll(q[c, g + 8], 1, 0), p[c])
            q[c, g + 11] = jnp.where(inner_high, roll(q[c, g + 3], -1, 0), p[c])
    major_pass(q, sl, sr, fx, 3)
    for c in range(5):
        face = jnp.where(upper_z, fx[c, 8], fx[c, 0])
        rz[c] = face if reg is None else reg[c] + face
        t = swap_groups([fx[c, m + 1] - fx[c, m] for m in range(8)])
        for m in range(8):
            d[c, m] = t[m]
    roll_pass(pr, d, y_shift, 2, at=0)


def x_kernel(*refs, stage):
    theta = THETA[stage]
    refs = list(refs)
    info, s, rl, rh, pr, d, old, new, base, reg = split_refs(
        refs, (1,) * 6 + (theta < 1.0, theta > 0.0, stage % 2, stage)
    )
    out, rx, lo, hi = split_refs(refs, (1, 1, stage < 3, stage < 3))
    q, sl, sr, fx, near = refs
    upper_x, second, _ = places_of_rows()
    near[:, :, 0:4, :] = rl[...]
    near[:, :, 4:8, :] = rh[...]
    code = jnp.where(
        upper_x,
        jnp.where(second, info[MATCH + 3], info[MATCH + 2]),
        jnp.where(second, info[MATCH + 1], info[MATCH]),
    )
    none = code == 2
    same = code == jnp.where(second, 1, 0)
    for c in range(5):
        for m in range(8):
            q[c, m + 3] = pr[c, m]
    for g in range(3):
        state = []
        for c in range(5):
            v = near[c, g]
            other = jnp.where(second, roll(v, 2, 0), roll(v, -2, 0))
            state.append(
                jnp.where(none, blend(old, new, theta, c, g), jnp.where(same, v, other))
            )
        p = prims_of(state)
        for c in range(5):
            q[c, g] = jnp.where(upper_x, roll(pr[c, g + 5], 4, 0), p[c])
            q[c, g + 11] = jnp.where(upper_x, p[c], roll(pr[c, g], 4, 0))
    major_pass(q, sl, sr, fx, 1)
    for c in range(5):
        face = jnp.where(upper_x, fx[c, 8], fx[c, 0])
        rx[c] = face if reg is None else reg[c] + face
        for m in range(8):
            change = d[c, m] + (fx[c, m + 1] - fx[c, m])
            if base is None:
                out[c, m] = s[c, m] - 0.2 * change
            else:
                out[c, m] = 0.5 * (base[c, m] + s[c, m]) - 0.1 * change
    if stage < 3:
        lo[...] = out[:, 0:3, 0:4, :]
        hi[...] = out[:, 5:8, 4:8, :]


def sync_kernel(info, s, rx, rz, new, mx, mz, out, low, high):
    lane = lanes()
    y = pick(subs() == ((lane & 15) >> 1))
    z0 = [info[Z0], info[Z0 + 1]]
    lr = iota2((128, 128), 0)
    zc = iota2((128, 128), 1)
    spread = [pick(zc == z0[pz // 2] + 4 * (pz % 2) + (lr >> 5)) for pz in range(4)]
    mean = None
    for pz in range(4):
        rows = []
        for c in range(5):
            for x in range(8):
                m, at = 2 * (x % 4), 4 * (x // 4) + pz
                v = s[c, m] + s[c, m + 1]
                rows.append(jnp.broadcast_to(v[at : at + 1], (8, 128)) * y)
        term = dot(jnp.concatenate(rows, axis=0), spread[pz])
        mean = term if mean is None else mean + term
    edge = [[info[MATCH + 2 * side + p] == 2 for p in range(2)] for side in range(2)]
    inside = [(lane >= z0[p]) & (lane < z0[p] + 8) for p in range(2)]
    placed = None
    for pz in range(4):
        rows = []
        for side in range(2):
            for c in range(5):
                v = rx[c]
                at = 4 * side + pz
                rows.append(jnp.broadcast_to(v[at : at + 1], (8, 128)) * y)
        term = dot(jnp.concatenate(rows, axis=0), spread[pz])
        placed = term if placed is None else placed + term
    for side, goal in ((0, low), (1, high)):
        keep = (inside[0] & edge[side][0]) | (inside[1] & edge[side][1])
        for c in range(5):
            at = 8 * (5 * side + c)
            delta = 0.2 * mx[c, side] - 0.0125 * placed[at : at + 8]
            goal[c] = jnp.where(keep, delta if side == 0 else -delta, 0.0)
    adjacent = info[ADJ] == 1
    apart = jnp.logical_not(adjacent)
    at_low = (lane == z0[0] - 1) | ((lane == z0[1] - 1) & apart)
    at_high = (lane == z0[1] + 8) | ((lane == z0[0] + 8) & apart)
    sub = subs()
    is_second = (sub & 2) != 0
    is_high = (sub & 1) != 0
    where_z = jnp.where(is_second, z0[1], z0[0]) + jnp.where(is_high, 8, -1)
    gone = adjacent & (is_second != is_high)
    sign = jnp.where(is_high, 0.0125, -0.0125)
    put = jnp.where((lane == where_z) & jnp.logical_not(gone), sign, 0.0)
    er = iota2((64, 128), 0)
    el = iota2((64, 128), 1)
    group = [
        pick(((er >> 3) == 4 * xh + (el >> 5)) & ((er & 7) == ((el & 15) >> 1)))
        for xh in range(2)
    ]
    covered = inside[0] | inside[1]
    for c in range(5):
        v = rz[c]
        n = dot_nt(group[0], jnp.where(sub < 4, v, 0.0))
        n = n + dot_nt(group[1], jnp.where(sub < 4, 0.0, v))
        fix = dot(n, put)
        for x in range(8):
            f = 0.2 * mz[c, x]
            w = new[c, x + 2] + fix[8 * x : 8 * x + 8]
            w = w + jnp.where(at_low, roll(f, -1, 1), 0.0)
            w = w - jnp.where(at_high, f, 0.0)
            at = 8 * (8 * c + x)
            out[c, x] = jnp.where(covered, 0.125 * mean[at : at + 8], w)


def last_kernel(info, w, left, right, out):
    lane = lanes()
    z0 = [info[Z0], info[Z0 + 1]]
    inside = [(lane >= z0[p]) & (lane < z0[p] + 8) for p in range(2)]
    covered = inside[0] | inside[1]
    for c in range(5):
        first = w[c, 0] + jnp.where(covered, 0.0, left[c])
        final = w[c, 7] + jnp.where(covered, 0.0, right[c])
        out[c, 0] = first[:, :LIVE_Z]
        out[c, 7] = final[:, :LIVE_Z]
        for x in range(1, 7):
            out[c, x] = w[c, x, :, pl.ds(0, LIVE_Z)]


VM = pl.BlockSpec(memory_space=pltpu.VMEM)
SM = pl.BlockSpec(memory_space=pltpu.SMEM)
LIMIT = 8 << 20
ANY = pl.BlockSpec(memory_space=pl.ANY)
HBM = pl.BlockSpec(memory_space=pltpu.HBM)


def call(kernel, ins, outs, scratch, args, alias=None):
    shapes = [jax.ShapeDtypeStruct(shape, dtype) for shape, dtype, _ in outs]
    return pl.pallas_call(
        kernel,
        in_specs=ins,
        out_specs=[spec for _, _, spec in outs],
        out_shape=shapes,
        scratch_shapes=scratch,
        input_output_aliases=alias or {},
        compiler_params=pltpu.CompilerParams(vmem_limit_bytes=LIMIT),
    )(*args)


def vm(*shape):
    return (shape, f32, VM)


def buf(*shape):
    return pltpu.VMEM(shape, f32)


FIELD = (5, 8, 8, 128)
WIDE_PASS = [buf(5, 24, 8, 128)] + [buf(5, 20, 8, 128)] * 2 + [buf(5, 19, 8, 128)] + [buf(5, 18, 8, 128)] * 2
PASS = [buf(5, 14, 8, 128), buf(5, 10, 8, 128), buf(5, 10, 8, 128), buf(5, 9, 8, 128)]


def ring(axis, up):
    count = DEEP if axis == "deep" else WIDE
    pairs = [(i, (i + 1) % count) for i in range(count)]
    return pairs if up else [(j, i) for i, j in pairs]


def swap(lo, hi, axis):
    below = lax.ppermute(hi, axis, ring(axis, True))
    return below, lax.ppermute(lo, axis, ring(axis, False))


def local(dens, vel, pres, fdens, fvel, fpres, counts, start):
    here = lax.axis_index("wide").astype(i32).reshape(1)
    (info,) = call(info_kernel, [SM] * 3, [((16,), i32, SM)], [], (counts, start, here))
    dma = pltpu.SemaphoreType.DMA
    moved = (WIDE, 5, 32, 128)
    (sent,) = call(
        send_kernel,
        [SM, ANY, ANY, ANY],
        [(moved, f32, ANY)],
        [dma((4, 12))],
        (info, fdens, fvel, fpres),
    )
    came = lax.all_to_all(sent, "wide", split_axis=0, concat_axis=0, tiled=True)

    edge = vm(8, 128)
    side = vm(5, 3, 8, 128)
    u0, plo, phi = call(
        prep_kernel,
        [HBM] * 3,
        [vm(*FIELD), edge, edge],
        [buf(8, 8, LIVE_Z), buf(3, 8, 8, LIVE_Z), buf(8, 8, LIVE_Z), dma((3,))],
        [pltpu.with_memory_space_constraint(x, pltpu.HBM) for x in (dens, vel, pres)],
    )
    zl0, zh0 = swap(plo, phi, "deep")
    (u0,) = call(halo_kernel, [VM] * 3, [vm(*FIELD)], [], (u0, zl0, zh0))
    ul, ur = swap(u0, u0, "wide")
    mid, plo, phi, fa, fza = call(
        coarse_one,
        [VM] * 3,
        [vm(5, 18, 8, 128), edge, edge, vm(5, 2, 8, 128), vm(*FIELD)],
        WIDE_PASS,
        (u0, ul, ur),
    )
    zl1, zh1 = swap(plo, phi, "deep")
    new, mx, mz = call(
        coarse_two,
        [VM] * 8,
        [vm(5, 12, 8, 128), vm(5, 2, 8, 128), vm(*FIELD)],
        WIDE_PASS,
        (u0, ul, ur, fa, fza, mid, zl1, zh1),
    )

    def rims(args, late):
        return call(
            lambda *refs: rim_kernel(*refs, late=late),
            [SM] + [VM] * len(args),
            [side, side],
            [],
            (info, *args),
        )

    old = rims((u0, ul, ur), False)
    late = rims((new,), True)

    strip = vm(5, 3, 4, 128)
    near = buf(5, 64, 128)
    s, flo, fhi = call(
        take_kernel, [SM, ANY], [vm(*FIELD), strip, strip], [near, dma((4,))], (info, came)
    )
    rx = rz = base = None
    for stage in range(4):
        theta = THETA[stage]
        rl, rh = swap(flo, fhi, "wide")
        gx = [old[0]] * (theta < 1.0) + [late[0]] * (theta > 0.0)
        gz = [old[1]] * (theta < 1.0) + [late[1]] * (theta > 0.0)
        args = [info, s] + gz + ([rz] if stage else [])
        pr, d, rz = call(
            lambda *refs, stage=stage: yz_kernel(*refs, stage=stage),
            [SM] + [VM] * (len(args) - 1),
            [vm(*FIELD), vm(*FIELD), vm(5, 8, 128)],
            PASS,
            args,
        )
        args = [info, s, rl, rh, pr, d] + gx
        args += ([base] if stage % 2 else []) + ([rx] if stage else [])
        if stage % 2 == 0:
            base = s
        got = call(
            lambda *refs, stage=stage: x_kernel(*refs, stage=stage),
            [SM] + [VM] * (len(args) - 1),
            [vm(*FIELD), vm(5, 8, 128)] + ([strip, strip] if stage < 3 else []),
            PASS + [buf(5, 3, 8, 128)],
            args,
        )
        s, rx = got[:2]
        if stage < 3:
            flo, fhi = got[2:]
    regs = (rx, rz)
    (gone,) = call(give_kernel, [SM, VM], [(moved, f32, ANY)], [near, dma((4,))], (info, s))
    home = lax.all_to_all(gone, "wide", split_axis=0, concat_axis=0, tiled=True)
    plane = vm(5, 8, 128)
    w, low, high = call(
        sync_kernel,
        [SM] + [VM] * 6,
        [vm(*FIELD), plane, plane],
        [],
        (info, s, regs[0], regs[1], new, mx, mz),
    )
    from_left, from_right = swap(low, high, "wide")
    (coarse_out,) = call(
        last_kernel, [SM] + [VM] * 3, [vm(5, 8, 8, LIVE_Z)], [], (info, w, from_left, from_right)
    )
    initial = jnp.stack(
        cons_of([fdens, fvel[:, :, 0], fvel[:, :, 1], fvel[:, :, 2], fpres]), axis=2
    )
    (fine_out,) = call(
        home_kernel,
        [SM, ANY, ANY],
        [(initial.shape, f32, ANY)],
        [dma((4, 4))],
        (info, home, initial),
        alias={2: 0},
    )
    return coarse_out, fine_out


def solution(mesh):
    return jax.shard_map(
        local,
        mesh=mesh,
        in_specs=(
            P("wide", None, "deep"),
            P(None, "wide", None, "deep"),
            P("wide", None, "deep"),
            P("deep", "wide", None, None),
            P("deep", "wide", None, None, None),
            P("deep", "wide", None, None),
            P("deep", None),
            P("deep"),
        ),
        out_specs=(P(None, "wide", None, "deep"), P("deep", "wide", None, None, None)),
        check_vma=False,
    )
```

```python
import jax
import jax.numpy as jnp
from jax import lax
from jax.experimental import pallas as pl
from jax.experimental.pallas import tpu as pltpu
from jax.sharding import PartitionSpec as P


f32 = jnp.float32
i32 = jnp.int32
HIGH = lax.Precision.HIGHEST
PLACES = 13
WIDE = 16
DEEP = 8
LIVE_Z = 120
FILL = (1.0, 0.0, 0.0, 0.0, 2.5)


def lanes():
    return lax.broadcasted_iota(i32, (8, 128), 1)


def subs():
    return lax.broadcasted_iota(i32, (8, 128), 0)


def roll(v, shift, axis):
    size = v.shape[axis]
    shift = shift % size
    return v if shift == 0 else pltpu.roll(v, shift, axis)


def y_shift(v, k):
    y = lanes() & 15
    if k > 0:
        return jnp.where(y < 16 - k, roll(v, -k, 1), roll(v, 16 - k, 1))
    return jnp.where(y >= -k, roll(v, -k, 1), roll(v, -k - 16, 1))


def sub_shift(v, k):
    return roll(v, -k, 0)


def lane_shift(v, k):
    return roll(v, -k, 1)


def prims_of(u):
    inv = 1.0 / u[0]
    vx, vy, vz = u[1] * inv, u[2] * inv, u[3] * inv
    kinetic = 0.5 * u[0] * (vx * vx + vy * vy + vz * vz)
    return [u[0], vx, vy, vz, 0.4 * (u[4] - kinetic)]


def cons_of(p):
    kinetic = 0.5 * p[0] * (p[1] * p[1] + p[2] * p[2] + p[3] * p[3])
    return [p[0], p[0] * p[1], p[0] * p[2], p[0] * p[3], p[4] / 0.4 + kinetic]


def recon(a, b, c, d, e):
    da, db, dc, dd = b - a, c - b, d - c, e - d
    ga, gb, gc = db - da, dc - db, dd - dc
    db2, dc2 = db + db, dc + dc
    ta, tb, tc = ga + db2, db + dc, gc - dc2
    k = 13.0 / 3.0
    sa = (k * ga) * ga + (ta * ta + 4e-6)
    sb = (k * gb) * gb + (tb * tb + 4e-6)
    sc = (k * gc) * gc + (tc * tc + 4e-6)
    pa, pb, pc = sa * sa, (sb * sb) * (1.0 / 6.0), sc * sc
    bc, ac, ab = pb * pc, pa * pc, pa * pb
    ab3, bc3 = 3.0 * ab, 3.0 * bc
    db4, dc4 = db2 + db2, dc2 + dc2
    left = bc * (db4 + db - (da + da)) + ac * (db + dc2) + ab3 * (dc4 - dd)
    right = ab * (dc4 + dc - (dd + dd)) + ac * (dc + db2) + bc3 * (db4 - da)
    left = left / (6.0 * (bc + ac + ab3))
    right = right / (6.0 * (ab + ac + bc3))
    return c + left, c - right


def hllc(lt, rt, n):
    o1, o2 = [k for k in (1, 2, 3) if k != n]
    dl, ul, pl_ = lt[0], lt[n], lt[4]
    dr, ur, pr = rt[0], rt[n], rt[4]
    il, ir = 1.0 / dl, 1.0 / dr
    cl = jnp.sqrt(1.4 * pl_ * il)
    cr = jnp.sqrt(1.4 * pr * ir)
    slow = jnp.minimum(ul - cl, ur - cr)
    fast = jnp.maximum(ul + cl, ur + cr)
    ml = dl * (slow - ul)
    mr = dr * (fast - ur)
    mid = (pr - pl_ + ml * ul - mr * ur) / (ml - mr)
    use = (slow >= 0.0) | (mid >= 0.0)
    d = jnp.where(use, dl, dr)
    u = jnp.where(use, ul, ur)
    t1 = jnp.where(use, lt[o1], rt[o1])
    t2 = jnp.where(use, lt[o2], rt[o2])
    p = jnp.where(use, pl_, pr)
    inv = jnp.where(use, il, ir)
    mass = jnp.where(use, ml, mr)
    wave = jnp.where(use, slow, fast)
    star = (use & (slow < 0.0)) | (jnp.logical_not(use) & (fast > 0.0))
    energy = 2.5 * p + 0.5 * d * (u * u + t1 * t1 + t2 * t2)
    du = d * u
    factor = mass / (wave - mid)
    e_star = energy * inv + (mid - u) * (mid + p / mass)
    out = [None] * 5
    flux = {0: du, n: du * u + p, o1: du * t1, o2: du * t2, 4: u * (energy + p)}
    state = {0: d, n: du, o1: d * t1, o2: d * t2, 4: energy}
    goal = {0: factor, n: factor * mid, o1: factor * t1, o2: factor * t2, 4: factor * e_star}
    for c in range(5):
        out[c] = jnp.where(star, flux[c] + wave * (goal[c] - state[c]), flux[c])
    return out


def repeat(count, unroll, body):
    turns = count // unroll

    def turn(t, carry):
        for j in range(unroll):
            body(t * unroll + j)
        return carry

    if turns > 0:
        lax.fori_loop(0, turns, turn, 0)
    for j in range(turns * unroll, count):
        body(j)


UNROLL_CELLS, UNROLL_FACES, UNROLL_ROLLS = 2, 9, 4


def major_pass(q, sl, sr, fx, n, count=10):
    def cells(m):
        for c in range(5):
            l, r = recon(*[q[c, m + k] for k in range(5)])
            sl[c, m] = l
            sr[c, m] = r

    repeat(count, UNROLL_CELLS, cells)

    def faces(f):
        out = hllc([sl[c, f] for c in range(5)], [sr[c, f + 1] for c in range(5)], n)
        for c in range(5):
            fx[c, f] = out[c]

    repeat(count - 1, UNROLL_FACES, faces)


def roll_pass(q, d, shift, n, count=8, keep=None, at=3):
    def cells(m):
        left, right = [], []
        for c in range(5):
            v = q[c, m + at]
            l, r = recon(shift(v, -2), shift(v, -1), v, shift(v, 1), shift(v, 2))
            left.append(shift(l, -1))
            right.append(r)
        out = hllc(left, right, n)
        for c in range(5):
            d[c, m] = d[c, m] + (shift(out[c], 1) - out[c])
            if keep is not None:
                keep[c, m] = out[c]

    repeat(count, UNROLL_ROLLS, cells)


def swap_groups(v):
    lane = lanes()
    for b in range(3):
        bit = ((lane >> (4 + b)) & 1) == 1
        step = 16 << b
        w = list(v)
        for m in range(8):
            if not (m >> b) & 1:
                lo, hi = v[m], v[m | (1 << b)]
                w[m] = jnp.where(bit, roll(hi, step, 1), lo)
                w[m | (1 << b)] = jnp.where(bit, hi, roll(lo, -step, 1))
        v = w
    return v


Z0, OWNER, COL, COUNT, ADJ, MATCH, PARITY = 0, 2, 4, 8, 9, 10, 14


def by_parity(info, first, second):
    odd = info[PARITY] == 1
    return jnp.where(odd, first, second), jnp.where(odd, second, first)


def column_places(column, anchor):
    d = (column - anchor) & 15
    bad = 2 - lax.rem(d, 3)
    off_a = d + 16 * jnp.where(bad == 0, 1, 0)
    off_b = d + 16 * jnp.where(bad == 2, 1, 2)

    def ident(off):
        place = anchor + off
        return jnp.where(place >= WIDE * PLACES, place - WIDE * PLACES, place)

    swap = ident(off_b) < ident(off_a)
    first = jnp.where(swap, off_b, off_a)
    second = jnp.where(swap, off_a, off_b)
    heights = [ident(first) >> 4, ident(second) >> 4]
    ranks = [2 * lax.div(o, 3) + lax.rem(o, 3) for o in (first, second)]
    return heights, ranks


def info_kernel(counts, start, here, info):
    me = here[0]
    anchor = start[0]
    h, ranks = column_places(me, anchor)
    low, _ = column_places((me + 15) & 15, anchor)
    high, _ = column_places((me + 1) & 15, anchor)
    total = jnp.int32(0)
    begin = jnp.int32(0)
    mine = jnp.int32(0)
    owner = [jnp.int32(0), jnp.int32(0)]
    for w in range(WIDE):
        n = counts[0, w]
        begin = jnp.where(me == w, total, begin)
        mine = jnp.where(me == w, n, mine)
        total = total + n
        for p in range(2):
            owner[p] = owner[p] + jnp.where(ranks[p] >= total, 1, 0)
    for p in range(2):
        info[Z0 + p] = 8 * (h[p] + 1)
        info[OWNER + p] = jnp.minimum(owner[p], WIDE - 1)
        for side, other in enumerate((low, high)):
            info[MATCH + 2 * side + p] = jnp.where(
                other[0] == h[p], 0, jnp.where(other[1] == h[p], 1, 2)
            )
    for s in range(4):
        serial = begin + s
        place = anchor + 3 * (serial >> 1) + (serial & 1)
        info[COL + s] = place & 15
    info[COUNT] = mine
    info[ADJ] = jnp.where(h[1] == h[0] + 1, 1, 0)
    info[PARITY] = me & 1
    info[15] = 0


def send_kernel(info, dens_far, vel_far, pres_far, out, dens, vel, pres, sem, load):
    pairs = ((dens_far, dens), (vel_far, vel), (pres_far, pres))
    loads = [pltpu.make_async_copy(a, b, load.at[k]) for k, (a, b) in enumerate(pairs)]
    for cp in loads:
        cp.start()
    for cp in loads:
        cp.wait()
    for s in range(4):

        @pl.when(s < info[COUNT])
        def _():
            for cp in slot_copies(info, dens, vel, pres, out, sem, s):
                cp.start()

    for s in range(4):

        @pl.when(s < info[COUNT])
        def _():
            for cp in slot_copies(info, dens, vel, pres, out, sem, s):
                cp.wait()


def slot_copies(info, dens, vel, pres, out, sem, s):
    to = info[COL + s]
    copies = []
    for xh in range(2):
        for zh in range(2):
            rows, cols = pl.ds(8 * xh, 8), pl.ds(128 * zh, 128)
            goal = pl.ds(16 * xh + 8 * zh, 8)
            k = 2 * xh + zh
            copies.append(
                pltpu.make_async_copy(
                    dens.at[0, s, rows, cols], out.at[to, 0, goal, :], sem.at[s, 3 * k]
                )
            )
            copies.append(
                pltpu.make_async_copy(
                    vel.at[0, s, :, rows, cols],
                    out.at[to, pl.ds(1, 3), goal, :],
                    sem.at[s, 3 * k + 1],
                )
            )
            copies.append(
                pltpu.make_async_copy(
                    pres.at[0, s, rows, cols], out.at[to, 4, goal, :], sem.at[s, 3 * k + 2]
                )
            )
    return copies


def patch_copies(info, far, near, sem, out):
    copies = []
    for p in range(2):
        for xh in range(2):
            there = far.at[info[OWNER + p], :, pl.ds(16 * xh, 16), :]
            here = near.at[:, pl.ds((4 * xh + 2 * p) * 8, 16), :]
            a, b = (here, there) if out else (there, here)
            copies.append(pltpu.make_async_copy(a, b, sem.at[2 * p + xh]))
    return copies


def take_kernel(info, far, s, near_side, far_side, near, sem):
    copies = patch_copies(info, far, near, sem, False)
    for cp in copies:
        cp.start()
    for cp in copies:
        cp.wait()
    for m in range(8):
        u = cons_of([near[c, pl.ds(m, 8, stride=8), :] for c in range(5)])
        for c in range(5):
            s[c, m] = u[c]
    sides(info, s, near_side, far_side)


def sides(info, s, near_side, far_side):
    for c in range(5):
        for g in range(3):
            near_side[c, g], far_side[c, g] = by_parity(info, s[c, g, 0:4, :], s[c, g + 5, 4:8, :])


def give_kernel(info, s, far, near, sem):
    for m in range(8):
        for c in range(5):
            near[c, pl.ds(m, 8, stride=8), :] = s[c, m]
    copies = patch_copies(info, far, near, sem, True)
    for cp in copies:
        cp.start()
    for cp in copies:
        cp.wait()


def home_copies(info, far, out, sem, s):
    copies = []
    for xh in range(2):
        for zh in range(2):
            copies.append(
                pltpu.make_async_copy(
                    far.at[info[COL + s], :, pl.ds(16 * xh + 8 * zh, 8), :],
                    out.at[0, s, :, pl.ds(8 * xh, 8), pl.ds(128 * zh, 128)],
                    sem.at[s, 2 * xh + zh],
                )
            )
    return copies


def pack_edge(u, first):
    lane = lanes()
    out = jnp.zeros((8, 128), f32)
    for c in range(5):
        for x in range(8):
            k = 3 * (8 * c + x)
            out = jnp.where((lane >= k) & (lane < k + 3), roll(u[c][x], k - first, 1), out)
    return out


def prep_kernel(dens_far, vel_far, pres_far, u, plo, phi, dens, vel, pres, sem):
    pairs = ((dens_far, dens), (vel_far, vel), (pres_far, pres))
    copies = [pltpu.make_async_copy(a, b, sem.at[k]) for k, (a, b) in enumerate(pairs)]
    for cp in copies:
        cp.start()
    for cp in copies:
        cp.wait()
    state = cons_of([dens[...], vel[0], vel[1], vel[2], pres[...]])
    for c in range(5):
        u[c] = jnp.full((8, 8, 128), FILL[c], f32)
        u[c, :, :, pl.ds(0, LIVE_Z)] = state[c]
    plo[...] = pack_edge([[u[c, x] for x in range(8)] for c in range(5)], 0)
    phi[...] = pack_edge([[u[c, x] for x in range(8)] for c in range(5)], LIVE_Z - 3)


def with_halo(v, below, above, k):
    lane = lanes()
    v = jnp.where(lane >= 125, roll(below, 125 - k, 1), v)
    return jnp.where((lane >= 120) & (lane < 123), roll(above, 120 - k, 1), v)


def halo_kernel(u, zl, zh, out):
    below, above = zl[...], zh[...]
    for c in range(5):
        for x in range(8):
            out[c, x] = with_halo(u[c, x], below, above, 3 * (8 * c + x))


def coarse_rates(layers, own, zl, zh, q, sl, sr, fx, d, keep):
    count = len(layers)
    for i, layer in enumerate(layers):
        state = [layer(c) for c in range(5)]
        if own is not None and 0 <= i - own < 8:
            state = [
                with_halo(state[c], zl[...], zh[...], 3 * (8 * c + i - own)) for c in range(5)
            ]
        p = prims_of(state)
        for c in range(5):
            q[c, i] = p[c]
    major_pass(q, sl, sr, fx, 1, count - 4)
    for c in range(5):
        for m in range(count - 6):
            d[c, m] = fx[c, m + 1] - fx[c, m]
    roll_pass(q, d, sub_shift, 2, count - 6)
    roll_pass(q, d, lane_shift, 3, count - 6, keep)


def take_layer(ref, x):
    return lambda c: ref[c, x]


def side_layers(info, ra, rb, side):
    def layer(x):
        return lambda c: by_parity(info, ra[c, x], rb[c, x])[side]

    return [layer(x) for x in range(8)]


def coarse_one(info, u, ra, rb, mid, plo, phi, fa, fz, q, sl, sr, fx, d, keep):
    refs = side_layers(info, ra, rb, 0) + [take_layer(u, x) for x in range(8)]
    refs += side_layers(info, ra, rb, 1)
    coarse_rates(refs, None, None, None, q, sl, sr, fx, d, keep)
    live = lanes() < LIVE_Z
    for c in range(5):
        fa[c, 0] = fx[c, 5]
        fa[c, 1] = fx[c, 13]
        for m in range(18):
            mid[c, m] = jnp.where(live, refs[m + 3](c) - 0.2 * d[c, m], FILL[c])
        for m in range(8):
            fz[c, m] = keep[c, m + 5]
    plo[...] = pack_edge([[mid[c, x + 5] for x in range(8)] for c in range(5)], 0)
    phi[...] = pack_edge([[mid[c, x + 5] for x in range(8)] for c in range(5)], LIVE_Z - 3)


def coarse_two(info, u0, ra, rb, fa, fza, u, zl, zh, new, mx, mz, q, sl, sr, fx, d, keep):
    refs = side_layers(info, ra, rb, 0) + [take_layer(u0, x) for x in range(8)]
    refs += side_layers(info, ra, rb, 1)
    coarse_rates([take_layer(u, m) for m in range(18)], 5, zl, zh, q, sl, sr, fx, d, keep)
    live = lanes() < LIVE_Z
    for c in range(5):
        mx[c, 0] = 0.5 * (fa[c, 0] + fx[c, 2])
        mx[c, 1] = 0.5 * (fa[c, 1] + fx[c, 10])
        for m in range(8):
            mz[c, m] = 0.5 * (fza[c, m] + keep[c, m + 2])
        for m in range(12):
            new[c, m] = jnp.where(
                live, 0.5 * (refs[m + 6](c) + u[c, m + 3]) - 0.1 * d[c, m], FILL[c]
            )


def dot(a, b):
    return jnp.dot(a, b, precision=HIGH, preferred_element_type=f32)


def dot_nt(a, b):
    return lax.dot_general(
        a, b, (((1,), (1,)), ((), ())), precision=HIGH, preferred_element_type=f32
    )


def iota2(shape, axis):
    return lax.broadcasted_iota(i32, shape, axis)


def pick(cond):
    return jnp.where(cond, 1.0, 0.0).astype(f32)


def rim_kernel(info, *refs, late):
    gx, gz = refs[-2:]
    if late:
        new = refs[0]
        low, high = [take_layer(new, 0), take_layer(new, 1)], [take_layer(new, 10), take_layer(new, 11)]
        own = lambda c: new[c, 2:10]
    else:
        u, ra, rb = refs[:3]
        low, high = side_layers(info, ra, rb, 0)[6:], side_layers(info, ra, rb, 1)[:2]
        own = lambda c: u[c]
    z = iota2((128, 128), 0)
    l = iota2((128, 128), 1)
    y8 = iota2((32, 128), 0) & 7
    ymask = pick(y8 == ((iota2((32, 128), 1) & 15) >> 1))
    layers = []
    for c in range(5):
        layers += [low[0](c), low[1](c), high[0](c), high[1](c)]
    rows = jnp.concatenate(layers, axis=0)
    parts = []
    for pz in range(4):
        start = info[Z0 + pz // 2] + 4 * (pz % 2)
        parts.append(dot(rows, pick(z == start + (l >> 5))))
    r = iota2((24, 128), 0)
    k = iota2((24, 128), 1)
    g, s = r >> 3, r & 7
    layer = jnp.where(s < 4, jnp.where(g == 0, 0, 1), jnp.where(g == 2, 3, 2))
    left = pick(((s & 3) == (k >> 5)) & (layer == ((k >> 3) & 3)))
    for c in range(5):
        stack = jnp.concatenate([part[32 * c : 32 * c + 32] * ymask for part in parts], axis=0)
        gx[c] = dot(left, stack).reshape(3, 8, 128)
    pnum = (s >> 1) & 1
    start = jnp.where(pnum == 0, info[Z0], info[Z0 + 1])
    off = jnp.where((s & 1) == 0, jnp.where(g == 0, -2, -1), jnp.where(g == 2, 9, 8))
    choose = pick(k == start + off)
    er = iota2((64, 256), 0)
    ec = iota2((64, 256), 1)
    spread = pick(((er >> 3) == (ec >> 5)) & ((er & 7) == ((ec & 15) >> 1)))
    for c in range(5):
        cols = dot_nt(choose, own(c).reshape(64, 128))
        both = dot(cols, spread)
        gz[c] = jnp.where(s < 4, both[:, :128], both[:, 128:]).reshape(3, 8, 128)


def blend(old, new, theta, c, g):
    if theta == 0.0:
        return old[c, g]
    if theta == 1.0:
        return new[c, g]
    return 0.5 * old[c, g] + 0.5 * new[c, g]


def split_refs(refs, flags):
    return [refs.pop(0) if flag else None for flag in flags]


def places_of_rows():
    sub = subs()
    return sub >= 4, (sub & 2) != 0, (sub & 1) != 0


THETA = (0.0, 0.5, 0.5, 1.0)


def yz_kernel(*refs, stage):
    theta = THETA[stage]
    refs = list(refs)
    info, s, old, new, reg = split_refs(refs, (1, 1, theta < 1.0, theta > 0.0, stage))
    pr, d, rz, q, sl, sr, fx = refs
    _, second, upper_z = places_of_rows()
    for m in range(8):
        p = prims_of([s[c, m] for c in range(5)])
        for c in range(5):
            pr[c, m] = p[c]
    adjacent = info[ADJ] == 1
    inner_low = upper_z | (second & adjacent)
    inner_high = jnp.logical_not(upper_z) | (jnp.logical_not(second) & adjacent)
    for c in range(5):
        t = swap_groups([pr[c, m] for m in range(8)])
        for m in range(8):
            q[c, m + 3] = t[m]
    for g in range(3):
        p = prims_of([blend(old, new, theta, c, g) for c in range(5)])
        for c in range(5):
            q[c, g] = jnp.where(inner_low, roll(q[c, g + 8], 1, 0), p[c])
            q[c, g + 11] = jnp.where(inner_high, roll(q[c, g + 3], -1, 0), p[c])
    major_pass(q, sl, sr, fx, 3)
    for c in range(5):
        face = jnp.where(upper_z, fx[c, 8], fx[c, 0])
        rz[c] = face if reg is None else reg[c] + face
        t = swap_groups([fx[c, m + 1] - fx[c, m] for m in range(8)])
        for m in range(8):
            d[c, m] = t[m]
    roll_pass(pr, d, y_shift, 2, at=0)


def x_kernel(*refs, stage):
    theta = THETA[stage]
    refs = list(refs)
    info, s, ra, rb, pr, d, old, new, base, reg = split_refs(
        refs, (1,) * 6 + (theta < 1.0, theta > 0.0, stage % 2, stage)
    )
    out, rx, near_side, far_side = split_refs(refs, (1, 1, stage < 3, stage < 3))
    q, sl, sr, fx, near = refs
    upper_x, second, _ = places_of_rows()
    for c in range(5):
        for g in range(3):
            near[c, g, 0:4, :], near[c, g, 4:8, :] = by_parity(info, ra[c, g], rb[c, g])
    code = jnp.where(
        upper_x,
        jnp.where(second, info[MATCH + 3], info[MATCH + 2]),
        jnp.where(second, info[MATCH + 1], info[MATCH]),
    )
    none = code == 2
    same = code == jnp.where(second, 1, 0)
    for c in range(5):
        for m in range(8):
            q[c, m + 3] = pr[c, m]
    for g in range(3):
        state = []
        for c in range(5):
            v = near[c, g]
            other = jnp.where(second, roll(v, 2, 0), roll(v, -2, 0))
            state.append(
                jnp.where(none, blend(old, new, theta, c, g), jnp.where(same, v, other))
            )
        p = prims_of(state)
        for c in range(5):
            q[c, g] = jnp.where(upper_x, roll(pr[c, g + 5], 4, 0), p[c])
            q[c, g + 11] = jnp.where(upper_x, p[c], roll(pr[c, g], 4, 0))
    major_pass(q, sl, sr, fx, 1)
    for c in range(5):
        face = jnp.where(upper_x, fx[c, 8], fx[c, 0])
        rx[c] = face if reg is None else reg[c] + face
        for m in range(8):
            change = d[c, m] + (fx[c, m + 1] - fx[c, m])
            if base is None:
                out[c, m] = s[c, m] - 0.2 * change
            else:
                out[c, m] = 0.5 * (base[c, m] + s[c, m]) - 0.1 * change
    if stage < 3:
        sides(info, out, near_side, far_side)


def sync_kernel(info, s, rx, rz, new, mx, mz, out, near_side, far_side):
    lane = lanes()
    y = pick(subs() == ((lane & 15) >> 1))
    z0 = [info[Z0], info[Z0 + 1]]
    lr = iota2((128, 128), 0)
    zc = iota2((128, 128), 1)
    spread = [pick(zc == z0[pz // 2] + 4 * (pz % 2) + (lr >> 5)) for pz in range(4)]
    mean = None
    for pz in range(4):
        rows = []
        for c in range(5):
            for x in range(8):
                m, at = 2 * (x % 4), 4 * (x // 4) + pz
                v = s[c, m] + s[c, m + 1]
                rows.append(jnp.broadcast_to(v[at : at + 1], (8, 128)) * y)
        term = dot(jnp.concatenate(rows, axis=0), spread[pz])
        mean = term if mean is None else mean + term
    edge = [[info[MATCH + 2 * side + p] == 2 for p in range(2)] for side in range(2)]
    inside = [(lane >= z0[p]) & (lane < z0[p] + 8) for p in range(2)]
    placed = None
    for pz in range(4):
        rows = []
        for side in range(2):
            for c in range(5):
                v = rx[c]
                at = 4 * side + pz
                rows.append(jnp.broadcast_to(v[at : at + 1], (8, 128)) * y)
        term = dot(jnp.concatenate(rows, axis=0), spread[pz])
        placed = term if placed is None else placed + term
    planes = []
    for side in range(2):
        keep = (inside[0] & edge[side][0]) | (inside[1] & edge[side][1])
        for c in range(5):
            at = 8 * (5 * side + c)
            delta = 0.2 * mx[c, side] - 0.0125 * placed[at : at + 8]
            planes.append(jnp.where(keep, delta if side == 0 else -delta, 0.0))
    for c in range(5):
        near_side[c], far_side[c] = by_parity(info, planes[c], planes[5 + c])
    adjacent = info[ADJ] == 1
    apart = jnp.logical_not(adjacent)
    at_low = (lane == z0[0] - 1) | ((lane == z0[1] - 1) & apart)
    at_high = (lane == z0[1] + 8) | ((lane == z0[0] + 8) & apart)
    sub = subs()
    is_second = (sub & 2) != 0
    is_high = (sub & 1) != 0
    where_z = jnp.where(is_second, z0[1], z0[0]) + jnp.where(is_high, 8, -1)
    gone = adjacent & (is_second != is_high)
    sign = jnp.where(is_high, 0.0125, -0.0125)
    put = jnp.where((lane == where_z) & jnp.logical_not(gone), sign, 0.0)
    er = iota2((64, 128), 0)
    el = iota2((64, 128), 1)
    group = [
        pick(((er >> 3) == 4 * xh + (el >> 5)) & ((er & 7) == ((el & 15) >> 1)))
        for xh in range(2)
    ]
    covered = inside[0] | inside[1]
    for c in range(5):
        v = rz[c]
        n = dot_nt(group[0], jnp.where(sub < 4, v, 0.0))
        n = n + dot_nt(group[1], jnp.where(sub < 4, 0.0, v))
        fix = dot(n, put)
        for x in range(8):
            f = 0.2 * mz[c, x]
            w = new[c, x + 2] + fix[8 * x : 8 * x + 8]
            w = w + jnp.where(at_low, roll(f, -1, 1), 0.0)
            w = w - jnp.where(at_high, f, 0.0)
            at = 8 * (8 * c + x)
            out[c, x] = jnp.where(covered, 0.125 * mean[at : at + 8], w)


def last_kernel(info, far, initial, w, ra, rb, coarse, fine, sem):
    for s in range(4):

        @pl.when(s < info[COUNT])
        def _():
            for cp in home_copies(info, far, fine, sem, s):
                cp.start()

    lane = lanes()
    z0 = [info[Z0], info[Z0 + 1]]
    inside = [(lane >= z0[p]) & (lane < z0[p] + 8) for p in range(2)]
    covered = inside[0] | inside[1]
    for c in range(5):
        left, right = by_parity(info, ra[c], rb[c])
        first = w[c, 0] + jnp.where(covered, 0.0, left)
        final = w[c, 7] + jnp.where(covered, 0.0, right)
        coarse[c, 0] = first[:, :LIVE_Z]
        coarse[c, 7] = final[:, :LIVE_Z]
        for x in range(1, 7):
            coarse[c, x] = w[c, x, :, pl.ds(0, LIVE_Z)]

    for s in range(4):

        @pl.when(s < info[COUNT])
        def _():
            for cp in home_copies(info, far, fine, sem, s):
                cp.wait()


VM = pl.BlockSpec(memory_space=pltpu.VMEM)
SM = pl.BlockSpec(memory_space=pltpu.SMEM)
LIMIT = 8 << 20
ANY = pl.BlockSpec(memory_space=pl.ANY)
HBM = pl.BlockSpec(memory_space=pltpu.HBM)


def call(kernel, ins, outs, scratch, args, alias=None):
    shapes = [jax.ShapeDtypeStruct(shape, dtype) for shape, dtype, _ in outs]
    return pl.pallas_call(
        kernel,
        in_specs=ins,
        out_specs=[spec for _, _, spec in outs],
        out_shape=shapes,
        scratch_shapes=scratch,
        input_output_aliases=alias or {},
        compiler_params=pltpu.CompilerParams(vmem_limit_bytes=LIMIT),
    )(*args)


def vm(*shape):
    return (shape, f32, VM)


def buf(*shape):
    return pltpu.VMEM(shape, f32)


FIELD = (5, 8, 8, 128)
WIDE_PASS = [buf(5, 24, 8, 128)] + [buf(5, 20, 8, 128)] * 2 + [buf(5, 19, 8, 128)] + [buf(5, 18, 8, 128)] * 2
PASS = [buf(5, 14, 8, 128), buf(5, 10, 8, 128), buf(5, 10, 8, 128), buf(5, 9, 8, 128)]


def ring(axis, up):
    count = DEEP if axis == "deep" else WIDE
    pairs = [(i, (i + 1) % count) for i in range(count)]
    return pairs if up else [(j, i) for i, j in pairs]


def swap(lo, hi, axis):
    below = lax.ppermute(hi, axis, ring(axis, True))
    return below, lax.ppermute(lo, axis, ring(axis, False))


def trade(near_side, far_side):
    far_pairs = [(i + 1, (i + 2) % WIDE) for i in range(0, WIDE, 2)]
    near_pairs = [(i, i + 1) for i in range(0, WIDE, 2)]
    got = []
    for value, pairs in ((far_side, far_pairs), (near_side, near_pairs)):
        got.append(lax.ppermute(value, "wide", pairs + [(j, i) for i, j in pairs]))
    return got[1], got[0]


def local(dens, vel, pres, fdens, fvel, fpres, counts, start):
    here = lax.axis_index("wide").astype(i32).reshape(1)
    (info,) = call(info_kernel, [SM] * 3, [((16,), i32, SM)], [], (counts, start, here))
    dma = pltpu.SemaphoreType.DMA
    moved = (WIDE, 5, 32, 128)
    (sent,) = call(
        send_kernel,
        [SM, HBM, HBM, HBM],
        [(moved, f32, ANY)],
        [buf(*x.shape) for x in (fdens, fvel, fpres)] + [dma((4, 12)), dma((3,))],
        [info] + [pltpu.with_memory_space_constraint(x, pltpu.HBM) for x in (fdens, fvel, fpres)],
    )
    came = lax.all_to_all(sent, "wide", split_axis=0, concat_axis=0, tiled=True)

    edge = vm(8, 128)
    side = vm(5, 3, 8, 128)
    u0, plo, phi = call(
        prep_kernel,
        [HBM] * 3,
        [vm(*FIELD), edge, edge],
        [buf(8, 8, LIVE_Z), buf(3, 8, 8, LIVE_Z), buf(8, 8, LIVE_Z), dma((3,))],
        [pltpu.with_memory_space_constraint(x, pltpu.HBM) for x in (dens, vel, pres)],
    )
    zl0, zh0 = swap(plo, phi, "deep")
    (u0,) = call(halo_kernel, [VM] * 3, [vm(*FIELD)], [], (u0, zl0, zh0))
    ra, rb = trade(u0, u0)
    mid, plo, phi, fa, fza = call(
        coarse_one,
        [SM] + [VM] * 3,
        [vm(5, 18, 8, 128), edge, edge, vm(5, 2, 8, 128), vm(*FIELD)],
        WIDE_PASS,
        (info, u0, ra, rb),
    )
    zl1, zh1 = swap(plo, phi, "deep")
    new, mx, mz = call(
        coarse_two,
        [SM] + [VM] * 8,
        [vm(5, 12, 8, 128), vm(5, 2, 8, 128), vm(*FIELD)],
        WIDE_PASS,
        (info, u0, ra, rb, fa, fza, mid, zl1, zh1),
    )

    def rims(args, late):
        return call(
            lambda *refs: rim_kernel(*refs, late=late),
            [SM] + [VM] * len(args),
            [side, side],
            [],
            (info, *args),
        )

    old = rims((u0, ra, rb), False)
    late = rims((new,), True)

    strip = vm(5, 3, 4, 128)
    near = buf(5, 64, 128)
    s, near_side, far_side = call(
        take_kernel, [SM, ANY], [vm(*FIELD), strip, strip], [near, dma((4,))], (info, came)
    )
    rx = rz = base = None
    for stage in range(4):
        theta = THETA[stage]
        ga, gb = trade(near_side, far_side)
        gx = [old[0]] * (theta < 1.0) + [late[0]] * (theta > 0.0)
        gz = [old[1]] * (theta < 1.0) + [late[1]] * (theta > 0.0)
        args = [info, s] + gz + ([rz] if stage else [])
        pr, d, rz = call(
            lambda *refs, stage=stage: yz_kernel(*refs, stage=stage),
            [SM] + [VM] * (len(args) - 1),
            [vm(*FIELD), vm(*FIELD), vm(5, 8, 128)],
            PASS,
            args,
        )
        args = [info, s, ga, gb, pr, d] + gx
        args += ([base] if stage % 2 else []) + ([rx] if stage else [])
        if stage % 2 == 0:
            base = s
        got = call(
            lambda *refs, stage=stage: x_kernel(*refs, stage=stage),
            [SM] + [VM] * (len(args) - 1),
            [vm(*FIELD), vm(5, 8, 128)] + ([strip, strip] if stage < 3 else []),
            PASS + [buf(5, 3, 8, 128)],
            args,
        )
        s, rx = got[:2]
        if stage < 3:
            near_side, far_side = got[2:]
    regs = (rx, rz)
    (gone,) = call(give_kernel, [SM, VM], [(moved, f32, ANY)], [near, dma((4,))], (info, s))
    home = lax.all_to_all(gone, "wide", split_axis=0, concat_axis=0, tiled=True)
    plane = vm(5, 8, 128)
    w, near_side, far_side = call(
        sync_kernel,
        [SM] + [VM] * 6,
        [vm(*FIELD), plane, plane],
        [],
        (info, s, regs[0], regs[1], new, mx, mz),
    )
    ra, rb = trade(near_side, far_side)
    initial = jnp.stack(
        cons_of([fdens, fvel[:, :, 0], fvel[:, :, 1], fvel[:, :, 2], fpres]), axis=2
    )
    coarse_out, fine_out = call(
        last_kernel,
        [SM, ANY, ANY] + [VM] * 3,
        [vm(5, 8, 8, LIVE_Z), (initial.shape, f32, ANY)],
        [dma((4, 4))],
        (info, home, initial, w, ra, rb),
        alias={2: 1},
    )
    return coarse_out, fine_out


def solution(mesh):
    return jax.shard_map(
        local,
        mesh=mesh,
        in_specs=(
            P("wide", None, "deep"),
            P(None, "wide", None, "deep"),
            P("wide", None, "deep"),
            P("deep", "wide", None, None),
            P("deep", "wide", None, None, None),
            P("deep", "wide", None, None),
            P("deep", None),
            P("deep"),
        ),
        out_specs=(P(None, "wide", None, "deep"), P("deep", "wide", None, None, None)),
        check_vma=False,
    )
```

```python
import jax
import jax.numpy as jnp
from jax import lax
from jax.experimental import pallas as pl
from jax.experimental.pallas import tpu as pltpu
from jax.sharding import PartitionSpec as P


f32 = jnp.float32
i32 = jnp.int32
HIGH = lax.Precision.HIGHEST
PLACES = 13
WIDE = 16
DEEP = 8
LIVE_Z = 120
FILL = (1.0, 0.0, 0.0, 0.0, 2.5)


def lanes():
    return lax.broadcasted_iota(i32, (8, 128), 1)


def subs():
    return lax.broadcasted_iota(i32, (8, 128), 0)


def roll(v, shift, axis):
    size = v.shape[axis]
    shift = shift % size
    return v if shift == 0 else pltpu.roll(v, shift, axis)


def y_shift(v, k):
    y = lanes() & 15
    if k > 0:
        return jnp.where(y < 16 - k, roll(v, -k, 1), roll(v, 16 - k, 1))
    return jnp.where(y >= -k, roll(v, -k, 1), roll(v, -k - 16, 1))


def sub_shift(v, k):
    return roll(v, -k, 0)


def lane_shift(v, k):
    return roll(v, -k, 1)


def prims_of(u):
    inv = 1.0 / u[0]
    vx, vy, vz = u[1] * inv, u[2] * inv, u[3] * inv
    kinetic = 0.5 * u[0] * (vx * vx + vy * vy + vz * vz)
    return [u[0], vx, vy, vz, 0.4 * (u[4] - kinetic)]


def cons_of(p):
    kinetic = 0.5 * p[0] * (p[1] * p[1] + p[2] * p[2] + p[3] * p[3])
    return [p[0], p[0] * p[1], p[0] * p[2], p[0] * p[3], p[4] / 0.4 + kinetic]


def recon(a, b, c, d, e):
    da, db, dc, dd = b - a, c - b, d - c, e - d
    ga, gb, gc = db - da, dc - db, dd - dc
    db2, dc2 = db + db, dc + dc
    ta, tb, tc = ga + db2, db + dc, gc - dc2
    k = 13.0 / 3.0
    sa = (k * ga) * ga + (ta * ta + 4e-6)
    sb = (k * gb) * gb + (tb * tb + 4e-6)
    sc = (k * gc) * gc + (tc * tc + 4e-6)
    pa, pb, pc = sa * sa, (sb * sb) * (1.0 / 6.0), sc * sc
    bc, ac, ab = pb * pc, pa * pc, pa * pb
    ab3, bc3 = 3.0 * ab, 3.0 * bc
    db4, dc4 = db2 + db2, dc2 + dc2
    left = bc * (db4 + db - (da + da)) + ac * (db + dc2) + ab3 * (dc4 - dd)
    right = ab * (dc4 + dc - (dd + dd)) + ac * (dc + db2) + bc3 * (db4 - da)
    left = left / (6.0 * (bc + ac + ab3))
    right = right / (6.0 * (ab + ac + bc3))
    return c + left, c - right


def hllc(lt, rt, n):
    o1, o2 = [k for k in (1, 2, 3) if k != n]
    dl, ul, pl_ = lt[0], lt[n], lt[4]
    dr, ur, pr = rt[0], rt[n], rt[4]
    il, ir = 1.0 / dl, 1.0 / dr
    cl = jnp.sqrt(1.4 * pl_ * il)
    cr = jnp.sqrt(1.4 * pr * ir)
    slow = jnp.minimum(ul - cl, ur - cr)
    fast = jnp.maximum(ul + cl, ur + cr)
    ml = dl * (slow - ul)
    mr = dr * (fast - ur)
    mid = (pr - pl_ + ml * ul - mr * ur) / (ml - mr)
    use = (slow >= 0.0) | (mid >= 0.0)
    d = jnp.where(use, dl, dr)
    u = jnp.where(use, ul, ur)
    t1 = jnp.where(use, lt[o1], rt[o1])
    t2 = jnp.where(use, lt[o2], rt[o2])
    p = jnp.where(use, pl_, pr)
    inv = jnp.where(use, il, ir)
    mass = jnp.where(use, ml, mr)
    wave = jnp.where(use, slow, fast)
    star = (use & (slow < 0.0)) | (jnp.logical_not(use) & (fast > 0.0))
    energy = 2.5 * p + 0.5 * d * (u * u + t1 * t1 + t2 * t2)
    du = d * u
    factor = mass / (wave - mid)
    e_star = energy * inv + (mid - u) * (mid + p / mass)
    out = [None] * 5
    flux = {0: du, n: du * u + p, o1: du * t1, o2: du * t2, 4: u * (energy + p)}
    state = {0: d, n: du, o1: d * t1, o2: d * t2, 4: energy}
    goal = {0: factor, n: factor * mid, o1: factor * t1, o2: factor * t2, 4: factor * e_star}
    for c in range(5):
        out[c] = jnp.where(star, flux[c] + wave * (goal[c] - state[c]), flux[c])
    return out


def repeat(count, unroll, body):
    turns = count // unroll

    def turn(t, carry):
        for j in range(unroll):
            body(t * unroll + j)
        return carry

    if turns > 0:
        lax.fori_loop(0, turns, turn, 0)
    for j in range(turns * unroll, count):
        body(j)


UNROLL_CELLS, UNROLL_FACES, UNROLL_ROLLS = 2, 9, 4


def major_cells(q, sl, sr, m):
    for c in range(5):
        l, r = recon(*[q[c, m + k] for k in range(5)])
        sl[c, m] = l
        sr[c, m] = r


def major_faces(sl, sr, fx, n, f):
    out = hllc([sl[c, f] for c in range(5)], [sr[c, f + 1] for c in range(5)], n)
    for c in range(5):
        fx[c, f] = out[c]


def major_pass(q, sl, sr, fx, n, count=10):
    repeat(count, UNROLL_CELLS, lambda m: major_cells(q, sl, sr, m))
    repeat(count - 1, UNROLL_FACES, lambda f: major_faces(sl, sr, fx, n, f))


def roll_pass(q, d, shift, n, count=8, keep=None, at=3):
    def cells(m):
        left, right = [], []
        for c in range(5):
            v = q[c, m + at]
            l, r = recon(shift(v, -2), shift(v, -1), v, shift(v, 1), shift(v, 2))
            left.append(shift(l, -1))
            right.append(r)
        out = hllc(left, right, n)
        for c in range(5):
            d[c, m] = d[c, m] + (shift(out[c], 1) - out[c])
            if keep is not None:
                keep[c, m] = out[c]

    repeat(count, UNROLL_ROLLS, cells)


def swap_groups(v):
    lane = lanes()
    for b in range(3):
        bit = ((lane >> (4 + b)) & 1) == 1
        step = 16 << b
        w = list(v)
        for m in range(8):
            if not (m >> b) & 1:
                lo, hi = v[m], v[m | (1 << b)]
                w[m] = jnp.where(bit, roll(hi, step, 1), lo)
                w[m | (1 << b)] = jnp.where(bit, hi, roll(lo, -step, 1))
        v = w
    return v


Z0, OWNER, COL, COUNT, ADJ, MATCH, PARITY = 0, 2, 4, 8, 9, 10, 14


def by_parity(info, first, second):
    odd = info[PARITY] == 1
    return jnp.where(odd, first, second), jnp.where(odd, second, first)


def column_places(column, anchor):
    d = (column - anchor) & 15
    bad = 2 - lax.rem(d, 3)
    off_a = d + 16 * jnp.where(bad == 0, 1, 0)
    off_b = d + 16 * jnp.where(bad == 2, 1, 2)

    def ident(off):
        place = anchor + off
        return jnp.where(place >= WIDE * PLACES, place - WIDE * PLACES, place)

    swap = ident(off_b) < ident(off_a)
    first = jnp.where(swap, off_b, off_a)
    second = jnp.where(swap, off_a, off_b)
    heights = [ident(first) >> 4, ident(second) >> 4]
    ranks = [2 * lax.div(o, 3) + lax.rem(o, 3) for o in (first, second)]
    return heights, ranks


def info_kernel(counts, start, here, info):
    me = here[0]
    anchor = start[0]
    h, ranks = column_places(me, anchor)
    low, _ = column_places((me + 15) & 15, anchor)
    high, _ = column_places((me + 1) & 15, anchor)
    total = jnp.int32(0)
    begin = jnp.int32(0)
    mine = jnp.int32(0)
    owner = [jnp.int32(0), jnp.int32(0)]
    for w in range(WIDE):
        n = counts[0, w]
        begin = jnp.where(me == w, total, begin)
        mine = jnp.where(me == w, n, mine)
        total = total + n
        for p in range(2):
            owner[p] = owner[p] + jnp.where(ranks[p] >= total, 1, 0)
    for p in range(2):
        info[Z0 + p] = 8 * (h[p] + 1)
        info[OWNER + p] = jnp.minimum(owner[p], WIDE - 1)
        for side, other in enumerate((low, high)):
            info[MATCH + 2 * side + p] = jnp.where(
                other[0] == h[p], 0, jnp.where(other[1] == h[p], 1, 2)
            )
    for s in range(4):
        serial = begin + s
        place = anchor + 3 * (serial >> 1) + (serial & 1)
        info[COL + s] = place & 15
    info[COUNT] = mine
    info[ADJ] = jnp.where(h[1] == h[0] + 1, 1, 0)
    info[PARITY] = me & 1
    info[15] = 0


def send_kernel(info, dens_far, vel_far, pres_far, out, dens, vel, pres, sem, load):
    pairs = ((dens_far, dens), (vel_far, vel), (pres_far, pres))
    loads = [pltpu.make_async_copy(a, b, load.at[k]) for k, (a, b) in enumerate(pairs)]
    for cp in loads:
        cp.start()
    for cp in loads:
        cp.wait()
    for s in range(4):

        @pl.when(s < info[COUNT])
        def _():
            for cp in slot_copies(info, dens, vel, pres, out, sem, s):
                cp.start()

    for s in range(4):

        @pl.when(s < info[COUNT])
        def _():
            for cp in slot_copies(info, dens, vel, pres, out, sem, s):
                cp.wait()


def slot_copies(info, dens, vel, pres, out, sem, s):
    to = info[COL + s]
    copies = []
    for xh in range(2):
        for zh in range(2):
            rows, cols = pl.ds(8 * xh, 8), pl.ds(128 * zh, 128)
            goal = pl.ds(16 * xh + 8 * zh, 8)
            k = 2 * xh + zh
            copies.append(
                pltpu.make_async_copy(
                    dens.at[0, s, rows, cols], out.at[to, 0, goal, :], sem.at[s, 3 * k]
                )
            )
            copies.append(
                pltpu.make_async_copy(
                    vel.at[0, s, :, rows, cols],
                    out.at[to, pl.ds(1, 3), goal, :],
                    sem.at[s, 3 * k + 1],
                )
            )
            copies.append(
                pltpu.make_async_copy(
                    pres.at[0, s, rows, cols], out.at[to, 4, goal, :], sem.at[s, 3 * k + 2]
                )
            )
    return copies


def patch_copies(info, far, near, sem, out):
    copies = []
    for p in range(2):
        for xh in range(2):
            there = far.at[info[OWNER + p], :, pl.ds(16 * xh, 16), :]
            here = near.at[:, pl.ds((4 * xh + 2 * p) * 8, 16), :]
            a, b = (here, there) if out else (there, here)
            copies.append(pltpu.make_async_copy(a, b, sem.at[2 * p + xh]))
    return copies


def take_kernel(info, far, s, near_side, far_side, near, sem):
    copies = patch_copies(info, far, near, sem, False)
    for cp in copies:
        cp.start()
    for cp in copies:
        cp.wait()
    for m in range(8):
        u = cons_of([near[c, pl.ds(m, 8, stride=8), :] for c in range(5)])
        for c in range(5):
            s[c, m] = u[c]
    sides(info, s, near_side, far_side)


def sides(info, s, near_side, far_side):
    for c in range(5):
        for g in range(3):
            near_side[c, g], far_side[c, g] = by_parity(info, s[c, g, 0:4, :], s[c, g + 5, 4:8, :])


def give(info, s, far, near, sem):
    for m in range(8):
        for c in range(5):
            near[c, pl.ds(m, 8, stride=8), :] = s[c, m]
    copies = patch_copies(info, far, near, sem, True)
    for cp in copies:
        cp.start()
    for cp in copies:
        cp.wait()


def home_copies(info, far, out, sem, s):
    copies = []
    for xh in range(2):
        for zh in range(2):
            copies.append(
                pltpu.make_async_copy(
                    far.at[info[COL + s], :, pl.ds(16 * xh + 8 * zh, 8), :],
                    out.at[0, s, :, pl.ds(8 * xh, 8), pl.ds(128 * zh, 128)],
                    sem.at[s, 2 * xh + zh],
                )
            )
    return copies


def pack_edge(u, first):
    lane = lanes()
    out = jnp.zeros((8, 128), f32)
    for c in range(5):
        for x in range(8):
            k = 3 * (8 * c + x)
            out = jnp.where((lane >= k) & (lane < k + 3), roll(u[c][x], k - first, 1), out)
    return out


def prep_kernel(dens_far, vel_far, pres_far, u, plo, phi, dens, vel, pres, sem):
    pairs = ((dens_far, dens), (vel_far, vel), (pres_far, pres))
    copies = [pltpu.make_async_copy(a, b, sem.at[k]) for k, (a, b) in enumerate(pairs)]
    for cp in copies:
        cp.start()
    for cp in copies:
        cp.wait()
    state = cons_of([dens[...], vel[0], vel[1], vel[2], pres[...]])
    for c in range(5):
        u[c] = jnp.full((8, 8, 128), FILL[c], f32)
        u[c, :, :, pl.ds(0, LIVE_Z)] = state[c]
    plo[...] = pack_edge([[u[c, x] for x in range(8)] for c in range(5)], 0)
    phi[...] = pack_edge([[u[c, x] for x in range(8)] for c in range(5)], LIVE_Z - 3)


def with_halo(v, below, above, k):
    lane = lanes()
    v = jnp.where(lane >= 125, roll(below, 125 - k, 1), v)
    return jnp.where((lane >= 120) & (lane < 123), roll(above, 120 - k, 1), v)


def halo_kernel(u, zl, zh, out):
    below, above = zl[...], zh[...]
    for c in range(5):
        for x in range(8):
            out[c, x] = with_halo(u[c, x], below, above, 3 * (8 * c + x))


def coarse_rates(layers, own, zl, zh, q, sl, sr, fx, d, keep):
    count = len(layers)
    for i, layer in enumerate(layers):
        state = [layer(c) for c in range(5)]
        if own is not None and 0 <= i - own < 8:
            state = [
                with_halo(state[c], zl[...], zh[...], 3 * (8 * c + i - own)) for c in range(5)
            ]
        p = prims_of(state)
        for c in range(5):
            q[c, i] = p[c]
    major_pass(q, sl, sr, fx, 1, count - 4)
    for c in range(5):
        for m in range(count - 6):
            d[c, m] = fx[c, m + 1] - fx[c, m]
    roll_pass(q, d, sub_shift, 2, count - 6)
    roll_pass(q, d, lane_shift, 3, count - 6, keep)


def take_layer(ref, x):
    return lambda c: ref[c, x]


def side_layers(info, ra, rb, side):
    def layer(x):
        return lambda c: by_parity(info, ra[c, x], rb[c, x])[side]

    return [layer(x) for x in range(8)]


def coarse_one(info, u, ra, rb, mid, plo, phi, fa, fz, q, sl, sr, fx, d, keep):
    refs = side_layers(info, ra, rb, 0) + [take_layer(u, x) for x in range(8)]
    refs += side_layers(info, ra, rb, 1)
    coarse_rates(refs, None, None, None, q, sl, sr, fx, d, keep)
    live = lanes() < LIVE_Z
    for c in range(5):
        fa[c, 0] = fx[c, 5]
        fa[c, 1] = fx[c, 13]
        for m in range(18):
            mid[c, m] = jnp.where(live, refs[m + 3](c) - 0.2 * d[c, m], FILL[c])
        for m in range(8):
            fz[c, m] = keep[c, m + 5]
    plo[...] = pack_edge([[mid[c, x + 5] for x in range(8)] for c in range(5)], 0)
    phi[...] = pack_edge([[mid[c, x + 5] for x in range(8)] for c in range(5)], LIVE_Z - 3)


def coarse_two(info, u0, ra, rb, fa, fza, u, zl, zh, new, mx, mz, q, sl, sr, fx, d, keep):
    refs = side_layers(info, ra, rb, 0) + [take_layer(u0, x) for x in range(8)]
    refs += side_layers(info, ra, rb, 1)
    coarse_rates([take_layer(u, m) for m in range(18)], 5, zl, zh, q, sl, sr, fx, d, keep)
    live = lanes() < LIVE_Z
    for c in range(5):
        mx[c, 0] = 0.5 * (fa[c, 0] + fx[c, 2])
        mx[c, 1] = 0.5 * (fa[c, 1] + fx[c, 10])
        for m in range(8):
            mz[c, m] = 0.5 * (fza[c, m] + keep[c, m + 2])
        for m in range(12):
            new[c, m] = jnp.where(
                live, 0.5 * (refs[m + 6](c) + u[c, m + 3]) - 0.1 * d[c, m], FILL[c]
            )


def dot(a, b):
    return jnp.dot(a, b, precision=HIGH, preferred_element_type=f32)


def dot_nt(a, b):
    return lax.dot_general(
        a, b, (((1,), (1,)), ((), ())), precision=HIGH, preferred_element_type=f32
    )


def iota2(shape, axis):
    return lax.broadcasted_iota(i32, shape, axis)


def pick(cond):
    return jnp.where(cond, 1.0, 0.0).astype(f32)


def rim_kernel(info, *refs, late):
    gx, gz = refs[-2:]
    if late:
        new = refs[0]
        low, high = [take_layer(new, 0), take_layer(new, 1)], [take_layer(new, 10), take_layer(new, 11)]
        own = lambda c: new[c, 2:10]
    else:
        u, ra, rb = refs[:3]
        low, high = side_layers(info, ra, rb, 0)[6:], side_layers(info, ra, rb, 1)[:2]
        own = lambda c: u[c]
    z = iota2((128, 128), 0)
    l = iota2((128, 128), 1)
    y8 = iota2((32, 128), 0) & 7
    ymask = pick(y8 == ((iota2((32, 128), 1) & 15) >> 1))
    layers = []
    for c in range(5):
        layers += [low[0](c), low[1](c), high[0](c), high[1](c)]
    rows = jnp.concatenate(layers, axis=0)
    parts = []
    for pz in range(4):
        start = info[Z0 + pz // 2] + 4 * (pz % 2)
        parts.append(dot(rows, pick(z == start + (l >> 5))))
    r = iota2((24, 128), 0)
    k = iota2((24, 128), 1)
    g, s = r >> 3, r & 7
    layer = jnp.where(s < 4, jnp.where(g == 0, 0, 1), jnp.where(g == 2, 3, 2))
    left = pick(((s & 3) == (k >> 5)) & (layer == ((k >> 3) & 3)))
    for c in range(5):
        stack = jnp.concatenate([part[32 * c : 32 * c + 32] * ymask for part in parts], axis=0)
        gx[c] = dot(left, stack).reshape(3, 8, 128)
    pnum = (s >> 1) & 1
    start = jnp.where(pnum == 0, info[Z0], info[Z0 + 1])
    off = jnp.where((s & 1) == 0, jnp.where(g == 0, -2, -1), jnp.where(g == 2, 9, 8))
    choose = pick(k == start + off)
    er = iota2((64, 256), 0)
    ec = iota2((64, 256), 1)
    spread = pick(((er >> 3) == (ec >> 5)) & ((er & 7) == ((ec & 15) >> 1)))
    for c in range(5):
        cols = dot_nt(choose, own(c).reshape(64, 128))
        both = dot(cols, spread)
        gz[c] = jnp.where(s < 4, both[:, :128], both[:, 128:]).reshape(3, 8, 128)


def blend(old, new, theta, c, g):
    if theta == 0.0:
        return old[c, g]
    if theta == 1.0:
        return new[c, g]
    return 0.5 * old[c, g] + 0.5 * new[c, g]


def split_refs(refs, flags):
    return [refs.pop(0) if flag else None for flag in flags]


def places_of_rows():
    sub = subs()
    return sub >= 4, (sub & 2) != 0, (sub & 1) != 0


THETA = (0.0, 0.5, 0.5, 1.0)


def yz_kernel(*refs, stage):
    theta = THETA[stage]
    refs = list(refs)
    info, s, old, new, reg = split_refs(refs, (1, 1, theta < 1.0, theta > 0.0, stage))
    pr, d, rz, inner, q, sl, sr, fx = refs
    _, second, upper_z = places_of_rows()
    for m in range(8):
        p = prims_of([s[c, m] for c in range(5)])
        for c in range(5):
            pr[c, m] = p[c]
    adjacent = info[ADJ] == 1
    inner_low = upper_z | (second & adjacent)
    inner_high = jnp.logical_not(upper_z) | (jnp.logical_not(second) & adjacent)
    for c in range(5):
        t = swap_groups([pr[c, m] for m in range(8)])
        for m in range(8):
            q[c, m + 3] = t[m]
    for g in range(3):
        p = prims_of([blend(old, new, theta, c, g) for c in range(5)])
        for c in range(5):
            q[c, g] = jnp.where(inner_low, roll(q[c, g + 8], 1, 0), p[c])
            q[c, g + 11] = jnp.where(inner_high, roll(q[c, g + 3], -1, 0), p[c])
    major_pass(q, sl, sr, fx, 3)
    for c in range(5):
        face = jnp.where(upper_z, fx[c, 8], fx[c, 0])
        rz[c] = face if reg is None else reg[c] + face
        t = swap_groups([fx[c, m + 1] - fx[c, m] for m in range(8)])
        for m in range(8):
            d[c, m] = t[m]
    roll_pass(pr, d, y_shift, 2, at=0)
    for c in range(5):
        for m in range(8):
            q[c, m + 3] = pr[c, m]
    repeat(4, 2, lambda m: major_cells(q, sl, sr, m + 3))
    for f in range(3, 6):
        major_faces(sl, sr, fx, 1, f)
    for c in range(5):
        for f in range(3):
            inner[c, f] = fx[c, f + 3]
        inner[c, 3] = sr[c, 3]
        inner[c, 4] = sl[c, 6]


def x_kernel(*refs, stage):
    theta = THETA[stage]
    refs = list(refs)
    info, s, ra, rb, pr, d, inner, old, new, base, reg = split_refs(
        refs, (1,) * 7 + (theta < 1.0, theta > 0.0, stage % 2, stage)
    )
    more = stage < 3
    out, rx, near_side, far_side, gone = split_refs(refs, (1, 1, more, more, not more))
    q, sl, sr, fx, near = refs[:5]
    upper_x, second, _ = places_of_rows()
    for c in range(5):
        for g in range(3):
            near[c, g, 0:4, :], near[c, g, 4:8, :] = by_parity(info, ra[c, g], rb[c, g])
    code = jnp.where(
        upper_x,
        jnp.where(second, info[MATCH + 3], info[MATCH + 2]),
        jnp.where(second, info[MATCH + 1], info[MATCH]),
    )
    none = code == 2
    same = code == jnp.where(second, 1, 0)
    for c in range(5):
        for m in range(8):
            q[c, m + 3] = pr[c, m]
    for g in range(3):
        state = []
        for c in range(5):
            v = near[c, g]
            other = jnp.where(second, roll(v, 2, 0), roll(v, -2, 0))
            state.append(
                jnp.where(none, blend(old, new, theta, c, g), jnp.where(same, v, other))
            )
        p = prims_of(state)
        for c in range(5):
            q[c, g] = jnp.where(upper_x, roll(pr[c, g + 5], 4, 0), p[c])
            q[c, g + 11] = jnp.where(upper_x, p[c], roll(pr[c, g], 4, 0))
    for c in range(5):
        for f in range(3):
            fx[c, f + 3] = inner[c, f]
        sr[c, 3] = inner[c, 3]
        sl[c, 6] = inner[c, 4]
    repeat(3, 3, lambda m: major_cells(q, sl, sr, m))
    repeat(3, 3, lambda m: major_cells(q, sl, sr, m + 7))
    for f in (0, 1, 2, 6, 7, 8):
        major_faces(sl, sr, fx, 1, f)
    for c in range(5):
        face = jnp.where(upper_x, fx[c, 8], fx[c, 0])
        rx[c] = face if reg is None else reg[c] + face
        for m in range(8):
            change = d[c, m] + (fx[c, m + 1] - fx[c, m])
            if base is None:
                out[c, m] = s[c, m] - 0.2 * change
            else:
                out[c, m] = 0.5 * (base[c, m] + s[c, m]) - 0.1 * change
    if more:
        sides(info, out, near_side, far_side)
    else:
        give(info, out, gone, *refs[5:])


def sync_kernel(info, s, rx, rz, new, mx, mz, out, near_side, far_side):
    lane = lanes()
    y = pick(subs() == ((lane & 15) >> 1))
    z0 = [info[Z0], info[Z0 + 1]]
    lr = iota2((128, 128), 0)
    zc = iota2((128, 128), 1)
    spread = [pick(zc == z0[pz // 2] + 4 * (pz % 2) + (lr >> 5)) for pz in range(4)]
    mean = None
    for pz in range(4):
        rows = []
        for c in range(5):
            for x in range(8):
                m, at = 2 * (x % 4), 4 * (x // 4) + pz
                v = s[c, m] + s[c, m + 1]
                rows.append(jnp.broadcast_to(v[at : at + 1], (8, 128)) * y)
        term = dot(jnp.concatenate(rows, axis=0), spread[pz])
        mean = term if mean is None else mean + term
    edge = [[info[MATCH + 2 * side + p] == 2 for p in range(2)] for side in range(2)]
    inside = [(lane >= z0[p]) & (lane < z0[p] + 8) for p in range(2)]
    placed = None
    for pz in range(4):
        rows = []
        for side in range(2):
            for c in range(5):
                v = rx[c]
                at = 4 * side + pz
                rows.append(jnp.broadcast_to(v[at : at + 1], (8, 128)) * y)
        term = dot(jnp.concatenate(rows, axis=0), spread[pz])
        placed = term if placed is None else placed + term
    planes = []
    for side in range(2):
        keep = (inside[0] & edge[side][0]) | (inside[1] & edge[side][1])
        for c in range(5):
            at = 8 * (5 * side + c)
            delta = 0.2 * mx[c, side] - 0.0125 * placed[at : at + 8]
            planes.append(jnp.where(keep, delta if side == 0 else -delta, 0.0))
    for c in range(5):
        near_side[c], far_side[c] = by_parity(info, planes[c], planes[5 + c])
    adjacent = info[ADJ] == 1
    apart = jnp.logical_not(adjacent)
    at_low = (lane == z0[0] - 1) | ((lane == z0[1] - 1) & apart)
    at_high = (lane == z0[1] + 8) | ((lane == z0[0] + 8) & apart)
    sub = subs()
    is_second = (sub & 2) != 0
    is_high = (sub & 1) != 0
    where_z = jnp.where(is_second, z0[1], z0[0]) + jnp.where(is_high, 8, -1)
    gone = adjacent & (is_second != is_high)
    sign = jnp.where(is_high, 0.0125, -0.0125)
    put = jnp.where((lane == where_z) & jnp.logical_not(gone), sign, 0.0)
    er = iota2((64, 128), 0)
    el = iota2((64, 128), 1)
    group = [
        pick(((er >> 3) == 4 * xh + (el >> 5)) & ((er & 7) == ((el & 15) >> 1)))
        for xh in range(2)
    ]
    covered = inside[0] | inside[1]
    for c in range(5):
        v = rz[c]
        n = dot_nt(group[0], jnp.where(sub < 4, v, 0.0))
        n = n + dot_nt(group[1], jnp.where(sub < 4, 0.0, v))
        fix = dot(n, put)
        for x in range(8):
            f = 0.2 * mz[c, x]
            w = new[c, x + 2] + fix[8 * x : 8 * x + 8]
            w = w + jnp.where(at_low, roll(f, -1, 1), 0.0)
            w = w - jnp.where(at_high, f, 0.0)
            at = 8 * (8 * c + x)
            out[c, x] = jnp.where(covered, 0.125 * mean[at : at + 8], w)


def last_kernel(info, far, initial, w, ra, rb, coarse, fine, sem):
    for s in range(4):

        @pl.when(s < info[COUNT])
        def _():
            for cp in home_copies(info, far, fine, sem, s):
                cp.start()

    lane = lanes()
    z0 = [info[Z0], info[Z0 + 1]]
    inside = [(lane >= z0[p]) & (lane < z0[p] + 8) for p in range(2)]
    covered = inside[0] | inside[1]
    for c in range(5):
        left, right = by_parity(info, ra[c], rb[c])
        first = w[c, 0] + jnp.where(covered, 0.0, left)
        final = w[c, 7] + jnp.where(covered, 0.0, right)
        coarse[c, 0] = first[:, :LIVE_Z]
        coarse[c, 7] = final[:, :LIVE_Z]
        for x in range(1, 7):
            coarse[c, x] = w[c, x, :, pl.ds(0, LIVE_Z)]

    for s in range(4):

        @pl.when(s < info[COUNT])
        def _():
            for cp in home_copies(info, far, fine, sem, s):
                cp.wait()


VM = pl.BlockSpec(memory_space=pltpu.VMEM)
SM = pl.BlockSpec(memory_space=pltpu.SMEM)
LIMIT = 8 << 20
ANY = pl.BlockSpec(memory_space=pl.ANY)
HBM = pl.BlockSpec(memory_space=pltpu.HBM)


def call(kernel, ins, outs, scratch, args, alias=None):
    shapes = [jax.ShapeDtypeStruct(shape, dtype) for shape, dtype, _ in outs]
    return pl.pallas_call(
        kernel,
        in_specs=ins,
        out_specs=[spec for _, _, spec in outs],
        out_shape=shapes,
        scratch_shapes=scratch,
        input_output_aliases=alias or {},
        compiler_params=pltpu.CompilerParams(vmem_limit_bytes=LIMIT),
    )(*args)


def vm(*shape):
    return (shape, f32, VM)


def buf(*shape):
    return pltpu.VMEM(shape, f32)


FIELD = (5, 8, 8, 128)
WIDE_PASS = [buf(5, 24, 8, 128)] + [buf(5, 20, 8, 128)] * 2 + [buf(5, 19, 8, 128)] + [buf(5, 18, 8, 128)] * 2
PASS = [buf(5, 14, 8, 128), buf(5, 10, 8, 128), buf(5, 10, 8, 128), buf(5, 9, 8, 128)]


def ring(axis, up):
    count = DEEP if axis == "deep" else WIDE
    pairs = [(i, (i + 1) % count) for i in range(count)]
    return pairs if up else [(j, i) for i, j in pairs]


def swap(lo, hi, axis):
    below = lax.ppermute(hi, axis, ring(axis, True))
    return below, lax.ppermute(lo, axis, ring(axis, False))


def trade(near_side, far_side):
    far_pairs = [(i + 1, (i + 2) % WIDE) for i in range(0, WIDE, 2)]
    near_pairs = [(i, i + 1) for i in range(0, WIDE, 2)]
    got = []
    for value, pairs in ((far_side, far_pairs), (near_side, near_pairs)):
        got.append(lax.ppermute(value, "wide", pairs + [(j, i) for i, j in pairs]))
    return got[1], got[0]


def local(dens, vel, pres, fdens, fvel, fpres, counts, start):
    here = lax.axis_index("wide").astype(i32).reshape(1)
    (info,) = call(info_kernel, [SM] * 3, [((16,), i32, SM)], [], (counts, start, here))
    dma = pltpu.SemaphoreType.DMA
    moved = (WIDE, 5, 32, 128)
    (sent,) = call(
        send_kernel,
        [SM, HBM, HBM, HBM],
        [(moved, f32, ANY)],
        [buf(*x.shape) for x in (fdens, fvel, fpres)] + [dma((4, 12)), dma((3,))],
        [info] + [pltpu.with_memory_space_constraint(x, pltpu.HBM) for x in (fdens, fvel, fpres)],
    )
    came = lax.all_to_all(sent, "wide", split_axis=0, concat_axis=0, tiled=True)

    edge = vm(8, 128)
    side = vm(5, 3, 8, 128)
    u0, plo, phi = call(
        prep_kernel,
        [HBM] * 3,
        [vm(*FIELD), edge, edge],
        [buf(8, 8, LIVE_Z), buf(3, 8, 8, LIVE_Z), buf(8, 8, LIVE_Z), dma((3,))],
        [pltpu.with_memory_space_constraint(x, pltpu.HBM) for x in (dens, vel, pres)],
    )
    zl0, zh0 = swap(plo, phi, "deep")
    (u0,) = call(halo_kernel, [VM] * 3, [vm(*FIELD)], [], (u0, zl0, zh0))
    ra, rb = trade(u0, u0)
    mid, plo, phi, fa, fza = call(
        coarse_one,
        [SM] + [VM] * 3,
        [vm(5, 18, 8, 128), edge, edge, vm(5, 2, 8, 128), vm(*FIELD)],
        WIDE_PASS,
        (info, u0, ra, rb),
    )
    zl1, zh1 = swap(plo, phi, "deep")
    new, mx, mz = call(
        coarse_two,
        [SM] + [VM] * 8,
        [vm(5, 12, 8, 128), vm(5, 2, 8, 128), vm(*FIELD)],
        WIDE_PASS,
        (info, u0, ra, rb, fa, fza, mid, zl1, zh1),
    )

    def rims(args, late):
        return call(
            lambda *refs: rim_kernel(*refs, late=late),
            [SM] + [VM] * len(args),
            [side, side],
            [],
            (info, *args),
        )

    old = rims((u0, ra, rb), False)
    late = rims((new,), True)

    strip = vm(5, 3, 4, 128)
    near = buf(5, 64, 128)
    s, near_side, far_side = call(
        take_kernel, [SM, ANY], [vm(*FIELD), strip, strip], [near, dma((4,))], (info, came)
    )
    rx = rz = base = None
    for stage in range(4):
        theta = THETA[stage]
        ga, gb = trade(near_side, far_side)
        gx = [old[0]] * (theta < 1.0) + [late[0]] * (theta > 0.0)
        gz = [old[1]] * (theta < 1.0) + [late[1]] * (theta > 0.0)
        args = [info, s] + gz + ([rz] if stage else [])
        pr, d, rz, inner = call(
            lambda *refs, stage=stage: yz_kernel(*refs, stage=stage),
            [SM] + [VM] * (len(args) - 1),
            [vm(*FIELD), vm(*FIELD), vm(5, 8, 128), vm(5, 5, 8, 128)],
            PASS,
            args,
        )
        args = [info, s, ga, gb, pr, d, inner] + gx
        args += ([base] if stage % 2 else []) + ([rx] if stage else [])
        if stage % 2 == 0:
            base = s
        got = call(
            lambda *refs, stage=stage: x_kernel(*refs, stage=stage),
            [SM] + [VM] * (len(args) - 1),
            [vm(*FIELD), vm(5, 8, 128)] + ([strip, strip] if stage < 3 else [(moved, f32, ANY)]),
            PASS + [buf(5, 3, 8, 128)] + ([] if stage < 3 else [near, dma((4,))]),
            args,
        )
        s, rx = got[:2]
        if stage < 3:
            near_side, far_side = got[2:]
    regs = (rx, rz)
    gone = got[2]
    home = lax.all_to_all(gone, "wide", split_axis=0, concat_axis=0, tiled=True)
    plane = vm(5, 8, 128)
    w, near_side, far_side = call(
        sync_kernel,
        [SM] + [VM] * 6,
        [vm(*FIELD), plane, plane],
        [],
        (info, s, regs[0], regs[1], new, mx, mz),
    )
    ra, rb = trade(near_side, far_side)
    initial = jnp.stack(
        cons_of([fdens, fvel[:, :, 0], fvel[:, :, 1], fvel[:, :, 2], fpres]), axis=2
    )
    coarse_out, fine_out = call(
        last_kernel,
        [SM, ANY, ANY] + [VM] * 3,
        [vm(5, 8, 8, LIVE_Z), (initial.shape, f32, ANY)],
        [dma((4, 4))],
        (info, home, initial, w, ra, rb),
        alias={2: 1},
    )
    return coarse_out, fine_out


def solution(mesh):
    return jax.shard_map(
        local,
        mesh=mesh,
        in_specs=(
            P("wide", None, "deep"),
            P(None, "wide", None, "deep"),
            P("wide", None, "deep"),
            P("deep", "wide", None, None),
            P("deep", "wide", None, None, None),
            P("deep", "wide", None, None),
            P("deep", None),
            P("deep"),
        ),
        out_specs=(P(None, "wide", None, "deep"), P("deep", "wide", None, None, None)),
        check_vma=False,
    )
```

```python
import jax
import jax.numpy as jnp
from jax import lax
from jax.experimental import pallas as pl
from jax.experimental.pallas import tpu as pltpu
from jax.sharding import PartitionSpec as P


f32 = jnp.float32
i32 = jnp.int32
HIGH = lax.Precision.HIGHEST
PLACES = 13
WIDE = 16
DEEP = 8
LIVE_Z = 120
FILL = (1.0, 0.0, 0.0, 0.0, 2.5)


def lanes():
    return lax.broadcasted_iota(i32, (8, 128), 1)


def subs():
    return lax.broadcasted_iota(i32, (8, 128), 0)


def roll(v, shift, axis):
    size = v.shape[axis]
    shift = shift % size
    return v if shift == 0 else pltpu.roll(v, shift, axis)


def y_shift(v, k):
    y = lanes() & 15
    if k > 0:
        return jnp.where(y < 16 - k, roll(v, -k, 1), roll(v, 16 - k, 1))
    return jnp.where(y >= -k, roll(v, -k, 1), roll(v, -k - 16, 1))


def sub_shift(v, k):
    return roll(v, -k, 0)


def lane_shift(v, k):
    return roll(v, -k, 1)


def prims_of(u):
    inv = 1.0 / u[0]
    vx, vy, vz = u[1] * inv, u[2] * inv, u[3] * inv
    kinetic = 0.5 * u[0] * (vx * vx + vy * vy + vz * vz)
    return [u[0], vx, vy, vz, 0.4 * (u[4] - kinetic)]


def cons_of(p):
    kinetic = 0.5 * p[0] * (p[1] * p[1] + p[2] * p[2] + p[3] * p[3])
    return [p[0], p[0] * p[1], p[0] * p[2], p[0] * p[3], p[4] / 0.4 + kinetic]


def recon(a, b, c, d, e):
    da, db, dc, dd = b - a, c - b, d - c, e - d
    ga, gb, gc = db - da, dc - db, dd - dc
    db2, dc2 = db + db, dc + dc
    ta, tb, tc = ga + db2, db + dc, gc - dc2
    k = 13.0 / 3.0
    sa = (k * ga) * ga + (ta * ta + 4e-6)
    sb = (k * gb) * gb + (tb * tb + 4e-6)
    sc = (k * gc) * gc + (tc * tc + 4e-6)
    pa, pb, pc = sa * sa, (sb * sb) * (1.0 / 6.0), sc * sc
    bc, ac, ab = pb * pc, pa * pc, pa * pb
    ab3, bc3 = 3.0 * ab, 3.0 * bc
    db4, dc4 = db2 + db2, dc2 + dc2
    left = bc * (db4 + db - (da + da)) + ac * (db + dc2) + ab3 * (dc4 - dd)
    right = ab * (dc4 + dc - (dd + dd)) + ac * (dc + db2) + bc3 * (db4 - da)
    left = left / (6.0 * (bc + ac + ab3))
    right = right / (6.0 * (ab + ac + bc3))
    return c + left, c - right


def hllc(lt, rt, n):
    o1, o2 = [k for k in (1, 2, 3) if k != n]
    dl, ul, pl_ = lt[0], lt[n], lt[4]
    dr, ur, pr = rt[0], rt[n], rt[4]
    il, ir = 1.0 / dl, 1.0 / dr
    cl = jnp.sqrt(1.4 * pl_ * il)
    cr = jnp.sqrt(1.4 * pr * ir)
    slow = jnp.minimum(ul - cl, ur - cr)
    fast = jnp.maximum(ul + cl, ur + cr)
    ml = dl * (slow - ul)
    mr = dr * (fast - ur)
    mid = (pr - pl_ + ml * ul - mr * ur) / (ml - mr)
    use = (slow >= 0.0) | (mid >= 0.0)
    d = jnp.where(use, dl, dr)
    u = jnp.where(use, ul, ur)
    t1 = jnp.where(use, lt[o1], rt[o1])
    t2 = jnp.where(use, lt[o2], rt[o2])
    p = jnp.where(use, pl_, pr)
    inv = jnp.where(use, il, ir)
    mass = jnp.where(use, ml, mr)
    wave = jnp.where(use, slow, fast)
    star = (use & (slow < 0.0)) | (jnp.logical_not(use) & (fast > 0.0))
    energy = 2.5 * p + 0.5 * d * (u * u + t1 * t1 + t2 * t2)
    du = d * u
    factor = mass / (wave - mid)
    e_star = energy * inv + (mid - u) * (mid + p / mass)
    out = [None] * 5
    flux = {0: du, n: du * u + p, o1: du * t1, o2: du * t2, 4: u * (energy + p)}
    state = {0: d, n: du, o1: d * t1, o2: d * t2, 4: energy}
    goal = {0: factor, n: factor * mid, o1: factor * t1, o2: factor * t2, 4: factor * e_star}
    for c in range(5):
        out[c] = jnp.where(star, flux[c] + wave * (goal[c] - state[c]), flux[c])
    return out


def repeat(count, unroll, body):
    turns = count // unroll

    def turn(t, carry):
        for j in range(unroll):
            body(t * unroll + j)
        return carry

    if turns > 0:
        lax.fori_loop(0, turns, turn, 0)
    for j in range(turns * unroll, count):
        body(j)


UNROLL_CELLS, UNROLL_FACES, UNROLL_ROLLS = 2, 9, 4


def major_cells(q, sl, sr, m):
    for c in range(5):
        l, r = recon(*[q[c, m + k] for k in range(5)])
        sl[c, m] = l
        sr[c, m] = r


def major_faces(sl, sr, fx, n, f):
    out = hllc([sl[c, f] for c in range(5)], [sr[c, f + 1] for c in range(5)], n)
    for c in range(5):
        fx[c, f] = out[c]


def major_pass(q, sl, sr, fx, n, count=10):
    repeat(count, UNROLL_CELLS, lambda m: major_cells(q, sl, sr, m))
    repeat(count - 1, UNROLL_FACES, lambda f: major_faces(sl, sr, fx, n, f))


def roll_pass(q, d, shift, n, count=8, keep=None, at=3):
    def cells(m):
        left, right = [], []
        for c in range(5):
            v = q[c, m + at]
            l, r = recon(shift(v, -2), shift(v, -1), v, shift(v, 1), shift(v, 2))
            left.append(shift(l, -1))
            right.append(r)
        out = hllc(left, right, n)
        for c in range(5):
            d[c, m] = d[c, m] + (shift(out[c], 1) - out[c])
            if keep is not None:
                keep[c, m] = out[c]

    repeat(count, UNROLL_ROLLS, cells)


def swap_groups(v):
    lane = lanes()
    for b in range(3):
        bit = ((lane >> (4 + b)) & 1) == 1
        step = 16 << b
        w = list(v)
        for m in range(8):
            if not (m >> b) & 1:
                lo, hi = v[m], v[m | (1 << b)]
                w[m] = jnp.where(bit, roll(hi, step, 1), lo)
                w[m | (1 << b)] = jnp.where(bit, hi, roll(lo, -step, 1))
        v = w
    return v


Z0, OWNER, COL, COUNT, ADJ, MATCH, PARITY = 0, 2, 4, 8, 9, 10, 14


def by_parity(info, first, second):
    odd = info[PARITY] == 1
    return jnp.where(odd, first, second), jnp.where(odd, second, first)


def column_places(column, anchor):
    d = (column - anchor) & 15
    bad = 2 - lax.rem(d, 3)
    off_a = d + 16 * jnp.where(bad == 0, 1, 0)
    off_b = d + 16 * jnp.where(bad == 2, 1, 2)

    def ident(off):
        place = anchor + off
        return jnp.where(place >= WIDE * PLACES, place - WIDE * PLACES, place)

    swap = ident(off_b) < ident(off_a)
    first = jnp.where(swap, off_b, off_a)
    second = jnp.where(swap, off_a, off_b)
    heights = [ident(first) >> 4, ident(second) >> 4]
    ranks = [2 * lax.div(o, 3) + lax.rem(o, 3) for o in (first, second)]
    return heights, ranks


def info_kernel(counts, start, here, info):
    me = here[0]
    anchor = start[0]
    h, ranks = column_places(me, anchor)
    low, _ = column_places((me + 15) & 15, anchor)
    high, _ = column_places((me + 1) & 15, anchor)
    total = jnp.int32(0)
    begin = jnp.int32(0)
    mine = jnp.int32(0)
    owner = [jnp.int32(0), jnp.int32(0)]
    for w in range(WIDE):
        n = counts[0, w]
        begin = jnp.where(me == w, total, begin)
        mine = jnp.where(me == w, n, mine)
        total = total + n
        for p in range(2):
            owner[p] = owner[p] + jnp.where(ranks[p] >= total, 1, 0)
    for p in range(2):
        info[Z0 + p] = 8 * (h[p] + 1)
        info[OWNER + p] = jnp.minimum(owner[p], WIDE - 1)
        for side, other in enumerate((low, high)):
            info[MATCH + 2 * side + p] = jnp.where(
                other[0] == h[p], 0, jnp.where(other[1] == h[p], 1, 2)
            )
    for s in range(4):
        serial = begin + s
        place = anchor + 3 * (serial >> 1) + (serial & 1)
        info[COL + s] = place & 15
    info[COUNT] = mine
    info[ADJ] = jnp.where(h[1] == h[0] + 1, 1, 0)
    info[PARITY] = me & 1
    info[15] = 0


def send_kernel(info, dens_far, vel_far, pres_far, out, dens, vel, pres, sem, load):
    pairs = ((dens_far, dens), (vel_far, vel), (pres_far, pres))
    loads = [pltpu.make_async_copy(a, b, load.at[k]) for k, (a, b) in enumerate(pairs)]
    for cp in loads:
        cp.start()
    for cp in loads:
        cp.wait()
    for s in range(4):

        @pl.when(s < info[COUNT])
        def _():
            for cp in slot_copies(info, dens, vel, pres, out, sem, s):
                cp.start()

    for s in range(4):

        @pl.when(s < info[COUNT])
        def _():
            for cp in slot_copies(info, dens, vel, pres, out, sem, s):
                cp.wait()


def slot_copies(info, dens, vel, pres, out, sem, s):
    to = info[COL + s]
    copies = []
    for xh in range(2):
        for zh in range(2):
            rows, cols = pl.ds(8 * xh, 8), pl.ds(128 * zh, 128)
            goal = pl.ds(16 * xh + 8 * zh, 8)
            k = 2 * xh + zh
            copies.append(
                pltpu.make_async_copy(
                    dens.at[0, s, rows, cols], out.at[to, 0, goal, :], sem.at[s, 3 * k]
                )
            )
            copies.append(
                pltpu.make_async_copy(
                    vel.at[0, s, :, rows, cols],
                    out.at[to, pl.ds(1, 3), goal, :],
                    sem.at[s, 3 * k + 1],
                )
            )
            copies.append(
                pltpu.make_async_copy(
                    pres.at[0, s, rows, cols], out.at[to, 4, goal, :], sem.at[s, 3 * k + 2]
                )
            )
    return copies


def patch_copies(info, far, near, sem, out):
    copies = []
    for p in range(2):
        for xh in range(2):
            there = far.at[info[OWNER + p], :, pl.ds(16 * xh, 16), :]
            here = near.at[:, pl.ds((4 * xh + 2 * p) * 8, 16), :]
            a, b = (here, there) if out else (there, here)
            copies.append(pltpu.make_async_copy(a, b, sem.at[2 * p + xh]))
    return copies


def take_kernel(info, far, s, near_side, far_side, near, sem):
    copies = patch_copies(info, far, near, sem, False)
    for cp in copies:
        cp.start()
    for cp in copies:
        cp.wait()
    for m in range(8):
        u = cons_of([near[c, pl.ds(m, 8, stride=8), :] for c in range(5)])
        for c in range(5):
            s[c, m] = u[c]
    sides(info, s, near_side, far_side)


def sides(info, s, near_side, far_side):
    for c in range(5):
        for g in range(3):
            near_side[c, g], far_side[c, g] = by_parity(info, s[c, g, 0:4, :], s[c, g + 5, 4:8, :])


def give(info, s, far, near, sem):
    for m in range(8):
        for c in range(5):
            near[c, pl.ds(m, 8, stride=8), :] = s[c, m]
    copies = patch_copies(info, far, near, sem, True)
    for cp in copies:
        cp.start()
    for cp in copies:
        cp.wait()


def home_copies(info, far, out, sem, s):
    copies = []
    for xh in range(2):
        for zh in range(2):
            copies.append(
                pltpu.make_async_copy(
                    far.at[info[COL + s], :, pl.ds(16 * xh + 8 * zh, 8), :],
                    out.at[0, s, :, pl.ds(8 * xh, 8), pl.ds(128 * zh, 128)],
                    sem.at[s, 2 * xh + zh],
                )
            )
    return copies


def pack_edge(u, first):
    lane = lanes()
    out = jnp.zeros((8, 128), f32)
    for c in range(5):
        for x in range(8):
            k = 3 * (8 * c + x)
            out = jnp.where((lane >= k) & (lane < k + 3), roll(u[c][x], k - first, 1), out)
    return out


def prep_kernel(dens_far, vel_far, pres_far, u, plo, phi, dens, vel, pres, sem):
    pairs = ((dens_far, dens), (vel_far, vel), (pres_far, pres))
    copies = [pltpu.make_async_copy(a, b, sem.at[k]) for k, (a, b) in enumerate(pairs)]
    for cp in copies:
        cp.start()
    for cp in copies:
        cp.wait()
    state = cons_of([dens[...], vel[0], vel[1], vel[2], pres[...]])
    for c in range(5):
        u[c] = jnp.full((8, 8, 128), FILL[c], f32)
        u[c, :, :, pl.ds(0, LIVE_Z)] = state[c]
    plo[...] = pack_edge([[u[c, x] for x in range(8)] for c in range(5)], 0)
    phi[...] = pack_edge([[u[c, x] for x in range(8)] for c in range(5)], LIVE_Z - 3)


def with_halo(v, below, above, k):
    lane = lanes()
    v = jnp.where(lane >= 125, roll(below, 125 - k, 1), v)
    return jnp.where((lane >= 120) & (lane < 123), roll(above, 120 - k, 1), v)


def halo_kernel(u, zl, zh, out):
    below, above = zl[...], zh[...]
    for c in range(5):
        for x in range(8):
            out[c, x] = with_halo(u[c, x], below, above, 3 * (8 * c + x))


def coarse_rates(layers, own, zl, zh, q, sl, sr, fx, d, keep):
    count = len(layers)
    for i, layer in enumerate(layers):
        state = [layer(c) for c in range(5)]
        if own is not None and 0 <= i - own < 8:
            state = [
                with_halo(state[c], zl[...], zh[...], 3 * (8 * c + i - own)) for c in range(5)
            ]
        p = prims_of(state)
        for c in range(5):
            q[c, i] = p[c]
    major_pass(q, sl, sr, fx, 1, count - 4)
    for c in range(5):
        for m in range(count - 6):
            d[c, m] = fx[c, m + 1] - fx[c, m]
    roll_pass(q, d, sub_shift, 2, count - 6)
    roll_pass(q, d, lane_shift, 3, count - 6, keep)


def take_layer(ref, x):
    return lambda c: ref[c, x]


def side_layers(info, ra, rb, side):
    def layer(x):
        return lambda c: by_parity(info, ra[c, x], rb[c, x])[side]

    return [layer(x) for x in range(8)]


def coarse_one(info, u, ra, rb, mid, plo, phi, fa, fz, q, sl, sr, fx, d, keep):
    refs = side_layers(info, ra, rb, 0) + [take_layer(u, x) for x in range(8)]
    refs += side_layers(info, ra, rb, 1)
    coarse_rates(refs, None, None, None, q, sl, sr, fx, d, keep)
    live = lanes() < LIVE_Z
    for c in range(5):
        fa[c, 0] = fx[c, 5]
        fa[c, 1] = fx[c, 13]
        for m in range(18):
            mid[c, m] = jnp.where(live, refs[m + 3](c) - 0.2 * d[c, m], FILL[c])
        for m in range(8):
            fz[c, m] = keep[c, m + 5]
    plo[...] = pack_edge([[mid[c, x + 5] for x in range(8)] for c in range(5)], 0)
    phi[...] = pack_edge([[mid[c, x + 5] for x in range(8)] for c in range(5)], LIVE_Z - 3)


def coarse_two(info, u0, ra, rb, fa, fza, u, zl, zh, new, mx, mz, q, sl, sr, fx, d, keep):
    refs = side_layers(info, ra, rb, 0) + [take_layer(u0, x) for x in range(8)]
    refs += side_layers(info, ra, rb, 1)
    coarse_rates([take_layer(u, m) for m in range(18)], 5, zl, zh, q, sl, sr, fx, d, keep)
    live = lanes() < LIVE_Z
    for c in range(5):
        mx[c, 0] = 0.5 * (fa[c, 0] + fx[c, 2])
        mx[c, 1] = 0.5 * (fa[c, 1] + fx[c, 10])
        for m in range(8):
            mz[c, m] = 0.5 * (fza[c, m] + keep[c, m + 2])
        for m in range(12):
            new[c, m] = jnp.where(
                live, 0.5 * (refs[m + 6](c) + u[c, m + 3]) - 0.1 * d[c, m], FILL[c]
            )


def dot(a, b):
    return jnp.dot(a, b, precision=HIGH, preferred_element_type=f32)


def dot_nt(a, b):
    return lax.dot_general(
        a, b, (((1,), (1,)), ((), ())), precision=HIGH, preferred_element_type=f32
    )


def iota2(shape, axis):
    return lax.broadcasted_iota(i32, shape, axis)


def pick(cond):
    return jnp.where(cond, 1.0, 0.0).astype(f32)


def rim_kernel(info, *refs, late):
    gx, gz = refs[-2:]
    if late:
        new = refs[0]
        low, high = [take_layer(new, 0), take_layer(new, 1)], [take_layer(new, 10), take_layer(new, 11)]
        own = lambda c: new[c, 2:10]
    else:
        u, ra, rb = refs[:3]
        low, high = side_layers(info, ra, rb, 0)[6:], side_layers(info, ra, rb, 1)[:2]
        own = lambda c: u[c]
    z = iota2((128, 128), 0)
    l = iota2((128, 128), 1)
    y8 = iota2((32, 128), 0) & 7
    ymask = pick(y8 == ((iota2((32, 128), 1) & 15) >> 1))
    layers = []
    for c in range(5):
        layers += [low[0](c), low[1](c), high[0](c), high[1](c)]
    rows = jnp.concatenate(layers, axis=0)
    parts = []
    for pz in range(4):
        start = info[Z0 + pz // 2] + 4 * (pz % 2)
        parts.append(dot(rows, pick(z == start + (l >> 5))))
    r = iota2((24, 128), 0)
    k = iota2((24, 128), 1)
    g, s = r >> 3, r & 7
    layer = jnp.where(s < 4, jnp.where(g == 0, 0, 1), jnp.where(g == 2, 3, 2))
    left = pick(((s & 3) == (k >> 5)) & (layer == ((k >> 3) & 3)))
    for c in range(5):
        stack = jnp.concatenate([part[32 * c : 32 * c + 32] * ymask for part in parts], axis=0)
        gx[c] = dot(left, stack).reshape(3, 8, 128)
    pnum = (s >> 1) & 1
    start = jnp.where(pnum == 0, info[Z0], info[Z0 + 1])
    off = jnp.where((s & 1) == 0, jnp.where(g == 0, -2, -1), jnp.where(g == 2, 9, 8))
    choose = pick(k == start + off)
    er = iota2((64, 256), 0)
    ec = iota2((64, 256), 1)
    spread = pick(((er >> 3) == (ec >> 5)) & ((er & 7) == ((ec & 15) >> 1)))
    for c in range(5):
        cols = dot_nt(choose, own(c).reshape(64, 128))
        both = dot(cols, spread)
        gz[c] = jnp.where(s < 4, both[:, :128], both[:, 128:]).reshape(3, 8, 128)


def blend(old, new, theta, c, g):
    if theta == 0.0:
        return old[c, g]
    if theta == 1.0:
        return new[c, g]
    return 0.5 * old[c, g] + 0.5 * new[c, g]


def split_refs(refs, flags):
    return [refs.pop(0) if flag else None for flag in flags]


def places_of_rows():
    sub = subs()
    return sub >= 4, (sub & 2) != 0, (sub & 1) != 0


THETA = (0.0, 0.5, 0.5, 1.0)


def yz_kernel(*refs, stage):
    theta = THETA[stage]
    refs = list(refs)
    info, s, old, new, reg = split_refs(refs, (1, 1, theta < 1.0, theta > 0.0, stage))
    pr, d, rz, inner, q, sl, sr, fx = refs
    _, second, upper_z = places_of_rows()
    for m in range(8):
        p = prims_of([s[c, m] for c in range(5)])
        for c in range(5):
            pr[c, m] = p[c]
    adjacent = info[ADJ] == 1
    inner_low = upper_z | (second & adjacent)
    inner_high = jnp.logical_not(upper_z) | (jnp.logical_not(second) & adjacent)
    for c in range(5):
        t = swap_groups([pr[c, m] for m in range(8)])
        for m in range(8):
            q[c, m + 3] = t[m]
    for g in range(3):
        p = prims_of([blend(old, new, theta, c, g) for c in range(5)])
        for c in range(5):
            q[c, g] = jnp.where(inner_low, roll(q[c, g + 8], 1, 0), p[c])
            q[c, g + 11] = jnp.where(inner_high, roll(q[c, g + 3], -1, 0), p[c])
    major_pass(q, sl, sr, fx, 3)
    for c in range(5):
        face = jnp.where(upper_z, fx[c, 8], fx[c, 0])
        rz[c] = face if reg is None else reg[c] + face
        t = swap_groups([fx[c, m + 1] - fx[c, m] for m in range(8)])
        for m in range(8):
            d[c, m] = t[m]
    roll_pass(pr, d, y_shift, 2, at=0)
    for c in range(5):
        for m in range(8):
            q[c, m + 3] = pr[c, m]
    repeat(4, 2, lambda m: major_cells(q, sl, sr, m + 3))
    for f in range(3, 6):
        major_faces(sl, sr, fx, 1, f)
    for c in range(5):
        for f in range(3):
            inner[c, f] = fx[c, f + 3]
        inner[c, 3] = sr[c, 3]
        inner[c, 4] = sl[c, 6]


def x_kernel(*refs, stage):
    theta = THETA[stage]
    refs = list(refs)
    info, s, ra, rb, pr, d, inner, old, new, base, reg = split_refs(
        refs, (1,) * 7 + (theta < 1.0, theta > 0.0, stage % 2, stage)
    )
    more = stage < 3
    out, rx, near_side, far_side, gone = split_refs(refs, (1, 1, more, more, not more))
    q, sl, sr, fx, near = refs[:5]
    upper_x, second, _ = places_of_rows()
    for c in range(5):
        for g in range(3):
            near[c, g, 0:4, :], near[c, g, 4:8, :] = by_parity(info, ra[c, g], rb[c, g])
    code = jnp.where(
        upper_x,
        jnp.where(second, info[MATCH + 3], info[MATCH + 2]),
        jnp.where(second, info[MATCH + 1], info[MATCH]),
    )
    none = code == 2
    same = code == jnp.where(second, 1, 0)
    for c in range(5):
        for m in range(8):
            q[c, m + 3] = pr[c, m]
    for g in range(3):
        state = []
        for c in range(5):
            v = near[c, g]
            other = jnp.where(second, roll(v, 2, 0), roll(v, -2, 0))
            state.append(
                jnp.where(none, blend(old, new, theta, c, g), jnp.where(same, v, other))
            )
        p = prims_of(state)
        for c in range(5):
            q[c, g] = jnp.where(upper_x, roll(pr[c, g + 5], 4, 0), p[c])
            q[c, g + 11] = jnp.where(upper_x, p[c], roll(pr[c, g], 4, 0))
    for c in range(5):
        for f in range(3):
            fx[c, f + 3] = inner[c, f]
        sr[c, 3] = inner[c, 3]
        sl[c, 6] = inner[c, 4]
    repeat(3, 3, lambda m: major_cells(q, sl, sr, m))
    repeat(3, 3, lambda m: major_cells(q, sl, sr, m + 7))
    for f in (0, 1, 2, 6, 7, 8):
        major_faces(sl, sr, fx, 1, f)
    for c in range(5):
        face = jnp.where(upper_x, fx[c, 8], fx[c, 0])
        rx[c] = face if reg is None else reg[c] + face
        for m in range(8):
            change = d[c, m] + (fx[c, m + 1] - fx[c, m])
            if base is None:
                out[c, m] = s[c, m] - 0.2 * change
            else:
                out[c, m] = 0.5 * (base[c, m] + s[c, m]) - 0.1 * change
    if more:
        sides(info, out, near_side, far_side)
    else:
        give(info, out, gone, *refs[5:])


def sync_kernel(info, s, rx, rz, new, mx, mz, out, near_side, far_side):
    lane = lanes()
    y = pick(subs() == ((lane & 15) >> 1))
    z0 = [info[Z0], info[Z0 + 1]]
    lr = iota2((128, 128), 0)
    zc = iota2((128, 128), 1)
    spread = [pick(zc == z0[pz // 2] + 4 * (pz % 2) + (lr >> 5)) for pz in range(4)]
    mean = None
    for pz in range(4):
        rows = []
        for c in range(5):
            for x in range(8):
                m, at = 2 * (x % 4), 4 * (x // 4) + pz
                v = s[c, m] + s[c, m + 1]
                rows.append(jnp.broadcast_to(v[at : at + 1], (8, 128)) * y)
        term = dot(jnp.concatenate(rows, axis=0), spread[pz])
        mean = term if mean is None else mean + term
    edge = [[info[MATCH + 2 * side + p] == 2 for p in range(2)] for side in range(2)]
    inside = [(lane >= z0[p]) & (lane < z0[p] + 8) for p in range(2)]
    placed = None
    for pz in range(4):
        rows = []
        for side in range(2):
            for c in range(5):
                v = rx[c]
                at = 4 * side + pz
                rows.append(jnp.broadcast_to(v[at : at + 1], (8, 128)) * y)
        term = dot(jnp.concatenate(rows, axis=0), spread[pz])
        placed = term if placed is None else placed + term
    planes = []
    for side in range(2):
        keep = (inside[0] & edge[side][0]) | (inside[1] & edge[side][1])
        for c in range(5):
            at = 8 * (5 * side + c)
            delta = 0.2 * mx[c, side] - 0.0125 * placed[at : at + 8]
            planes.append(jnp.where(keep, delta if side == 0 else -delta, 0.0))
    for c in range(5):
        near_side[c], far_side[c] = by_parity(info, planes[c], planes[5 + c])
    adjacent = info[ADJ] == 1
    apart = jnp.logical_not(adjacent)
    at_low = (lane == z0[0] - 1) | ((lane == z0[1] - 1) & apart)
    at_high = (lane == z0[1] + 8) | ((lane == z0[0] + 8) & apart)
    sub = subs()
    is_second = (sub & 2) != 0
    is_high = (sub & 1) != 0
    where_z = jnp.where(is_second, z0[1], z0[0]) + jnp.where(is_high, 8, -1)
    gone = adjacent & (is_second != is_high)
    sign = jnp.where(is_high, 0.0125, -0.0125)
    put = jnp.where((lane == where_z) & jnp.logical_not(gone), sign, 0.0)
    er = iota2((64, 128), 0)
    el = iota2((64, 128), 1)
    group = [
        pick(((er >> 3) == 4 * xh + (el >> 5)) & ((er & 7) == ((el & 15) >> 1)))
        for xh in range(2)
    ]
    covered = inside[0] | inside[1]
    for c in range(5):
        v = rz[c]
        n = dot_nt(group[0], jnp.where(sub < 4, v, 0.0))
        n = n + dot_nt(group[1], jnp.where(sub < 4, 0.0, v))
        fix = dot(n, put)
        for x in range(8):
            f = 0.2 * mz[c, x]
            w = new[c, x + 2] + fix[8 * x : 8 * x + 8]
            w = w + jnp.where(at_low, roll(f, -1, 1), 0.0)
            w = w - jnp.where(at_high, f, 0.0)
            at = 8 * (8 * c + x)
            out[c, x] = jnp.where(covered, 0.125 * mean[at : at + 8], w)


def home_kernel(info, far, initial, fine, sem):
    for s in range(4):

        @pl.when(s < info[COUNT])
        def _():
            for cp in home_copies(info, far, fine, sem, s):
                cp.start()

    for s in range(4):

        @pl.when(s < info[COUNT])
        def _():
            for cp in home_copies(info, far, fine, sem, s):
                cp.wait()


def last_kernel(info, w, ra, rb, coarse):
    lane = lanes()
    z0 = [info[Z0], info[Z0 + 1]]
    inside = [(lane >= z0[p]) & (lane < z0[p] + 8) for p in range(2)]
    covered = inside[0] | inside[1]
    for c in range(5):
        left, right = by_parity(info, ra[c], rb[c])
        first = w[c, 0] + jnp.where(covered, 0.0, left)
        final = w[c, 7] + jnp.where(covered, 0.0, right)
        coarse[c, 0] = first[:, :LIVE_Z]
        coarse[c, 7] = final[:, :LIVE_Z]
        for x in range(1, 7):
            coarse[c, x] = w[c, x, :, pl.ds(0, LIVE_Z)]


VM = pl.BlockSpec(memory_space=pltpu.VMEM)
SM = pl.BlockSpec(memory_space=pltpu.SMEM)
LIMIT = 8 << 20
ANY = pl.BlockSpec(memory_space=pl.ANY)
HBM = pl.BlockSpec(memory_space=pltpu.HBM)


def call(kernel, ins, outs, scratch, args, alias=None):
    shapes = [jax.ShapeDtypeStruct(shape, dtype) for shape, dtype, _ in outs]
    return pl.pallas_call(
        kernel,
        in_specs=ins,
        out_specs=[spec for _, _, spec in outs],
        out_shape=shapes,
        scratch_shapes=scratch,
        input_output_aliases=alias or {},
        compiler_params=pltpu.CompilerParams(vmem_limit_bytes=LIMIT),
    )(*args)


def vm(*shape):
    return (shape, f32, VM)


def buf(*shape):
    return pltpu.VMEM(shape, f32)


FIELD = (5, 8, 8, 128)
WIDE_PASS = [buf(5, 24, 8, 128)] + [buf(5, 20, 8, 128)] * 2 + [buf(5, 19, 8, 128)] + [buf(5, 18, 8, 128)] * 2
PASS = [buf(5, 14, 8, 128), buf(5, 10, 8, 128), buf(5, 10, 8, 128), buf(5, 9, 8, 128)]


def ring(axis, up):
    count = DEEP if axis == "deep" else WIDE
    pairs = [(i, (i + 1) % count) for i in range(count)]
    return pairs if up else [(j, i) for i, j in pairs]


def swap(lo, hi, axis):
    below = lax.ppermute(hi, axis, ring(axis, True))
    return below, lax.ppermute(lo, axis, ring(axis, False))


def trade(near_side, far_side):
    far_pairs = [(i + 1, (i + 2) % WIDE) for i in range(0, WIDE, 2)]
    near_pairs = [(i, i + 1) for i in range(0, WIDE, 2)]
    got = []
    for value, pairs in ((far_side, far_pairs), (near_side, near_pairs)):
        got.append(lax.ppermute(value, "wide", pairs + [(j, i) for i, j in pairs]))
    return got[1], got[0]


def local(dens, vel, pres, fdens, fvel, fpres, counts, start):
    here = lax.axis_index("wide").astype(i32).reshape(1)
    (info,) = call(info_kernel, [SM] * 3, [((16,), i32, SM)], [], (counts, start, here))
    dma = pltpu.SemaphoreType.DMA
    moved = (WIDE, 5, 32, 128)
    (sent,) = call(
        send_kernel,
        [SM, HBM, HBM, HBM],
        [(moved, f32, ANY)],
        [buf(*x.shape) for x in (fdens, fvel, fpres)] + [dma((4, 12)), dma((3,))],
        [info] + [pltpu.with_memory_space_constraint(x, pltpu.HBM) for x in (fdens, fvel, fpres)],
    )
    came = lax.all_to_all(sent, "wide", split_axis=0, concat_axis=0, tiled=True)

    edge = vm(8, 128)
    side = vm(5, 3, 8, 128)
    u0, plo, phi = call(
        prep_kernel,
        [HBM] * 3,
        [vm(*FIELD), edge, edge],
        [buf(8, 8, LIVE_Z), buf(3, 8, 8, LIVE_Z), buf(8, 8, LIVE_Z), dma((3,))],
        [pltpu.with_memory_space_constraint(x, pltpu.HBM) for x in (dens, vel, pres)],
    )
    zl0, zh0 = swap(plo, phi, "deep")
    (u0,) = call(halo_kernel, [VM] * 3, [vm(*FIELD)], [], (u0, zl0, zh0))
    ra, rb = trade(u0, u0)
    mid, plo, phi, fa, fza = call(
        coarse_one,
        [SM] + [VM] * 3,
        [vm(5, 18, 8, 128), edge, edge, vm(5, 2, 8, 128), vm(*FIELD)],
        WIDE_PASS,
        (info, u0, ra, rb),
    )
    zl1, zh1 = swap(plo, phi, "deep")
    new, mx, mz = call(
        coarse_two,
        [SM] + [VM] * 8,
        [vm(5, 12, 8, 128), vm(5, 2, 8, 128), vm(*FIELD)],
        WIDE_PASS,
        (info, u0, ra, rb, fa, fza, mid, zl1, zh1),
    )

    def rims(args, late):
        return call(
            lambda *refs: rim_kernel(*refs, late=late),
            [SM] + [VM] * len(args),
            [side, side],
            [],
            (info, *args),
        )

    old = rims((u0, ra, rb), False)
    late = rims((new,), True)

    strip = vm(5, 3, 4, 128)
    near = buf(5, 64, 128)
    s, near_side, far_side = call(
        take_kernel, [SM, ANY], [vm(*FIELD), strip, strip], [near, dma((4,))], (info, came)
    )
    rx = rz = base = None
    for stage in range(4):
        theta = THETA[stage]
        ga, gb = trade(near_side, far_side)
        gx = [old[0]] * (theta < 1.0) + [late[0]] * (theta > 0.0)
        gz = [old[1]] * (theta < 1.0) + [late[1]] * (theta > 0.0)
        args = [info, s] + gz + ([rz] if stage else [])
        pr, d, rz, inner = call(
            lambda *refs, stage=stage: yz_kernel(*refs, stage=stage),
            [SM] + [VM] * (len(args) - 1),
            [vm(*FIELD), vm(*FIELD), vm(5, 8, 128), vm(5, 5, 8, 128)],
            PASS,
            args,
        )
        args = [info, s, ga, gb, pr, d, inner] + gx
        args += ([base] if stage % 2 else []) + ([rx] if stage else [])
        if stage % 2 == 0:
            base = s
        got = call(
            lambda *refs, stage=stage: x_kernel(*refs, stage=stage),
            [SM] + [VM] * (len(args) - 1),
            [vm(*FIELD), vm(5, 8, 128)] + ([strip, strip] if stage < 3 else [(moved, f32, ANY)]),
            PASS + [buf(5, 3, 8, 128)] + ([] if stage < 3 else [near, dma((4,))]),
            args,
        )
        s, rx = got[:2]
        if stage < 3:
            near_side, far_side = got[2:]
    regs = (rx, rz)
    gone = got[2]
    home = lax.all_to_all(gone, "wide", split_axis=0, concat_axis=0, tiled=True)
    plane = vm(5, 8, 128)
    w, near_side, far_side = call(
        sync_kernel,
        [SM] + [VM] * 6,
        [vm(*FIELD), plane, plane],
        [],
        (info, s, regs[0], regs[1], new, mx, mz),
    )
    ra, rb = trade(near_side, far_side)
    initial = jnp.stack(
        cons_of([fdens, fvel[:, :, 0], fvel[:, :, 1], fvel[:, :, 2], fpres]), axis=2
    )
    (coarse_out,) = call(last_kernel, [SM] + [VM] * 3, [vm(5, 8, 8, LIVE_Z)], [], (info, w, ra, rb))
    (fine_out,) = call(
        home_kernel,
        [SM, ANY, ANY],
        [(initial.shape, f32, ANY)],
        [dma((4, 4))],
        (info, home, initial),
        alias={2: 0},
    )
    return coarse_out, fine_out


def solution(mesh):
    return jax.shard_map(
        local,
        mesh=mesh,
        in_specs=(
            P("wide", None, "deep"),
            P(None, "wide", None, "deep"),
            P("wide", None, "deep"),
            P("deep", "wide", None, None),
            P("deep", "wide", None, None, None),
            P("deep", "wide", None, None),
            P("deep", None),
            P("deep"),
        ),
        out_specs=(P(None, "wide", None, "deep"), P("deep", "wide", None, None, None)),
        check_vma=False,
    )
```
